128 devices in a mesh: heads: 16 (over z, y), model: 8 (over x, core).
Axes of the slice: x: 4, y: 4, z: 4, core: 2. Of those that a mesh axis runs over, the one named last changes fastest.
Arguments:
- hidden_in: bfloat16 [4096, 3072], P(None, 'model')
- seg_ids: int32 [4096], replicated
- positions: int32 [4096], replicated
- w_query: bfloat16 [2, 3072, 4096], P(None, 'model', 'heads')
- w_key: bfloat16 [2, 3072, 4096], P(None, 'model', 'heads')
- w_value: bfloat16 [2, 3072, 4096], P(None, 'model', 'heads')
- w_out: bfloat16 [2, 4096, 3072], P(None, 'heads', 'model')
- w_gate: bfloat16 [2, 3072, 24576], P(None, 'model', 'heads')
- w_up: bfloat16 [2, 3072, 24576], P(None, 'model', 'heads')
- w_down: bfloat16 [2, 24576, 3072], P(None, 'heads', 'model')
- norm_scales: float32 [2, 4, 3072], P(None, None, 'model')
- qk_scales: float32 [2, 2, 256], replicated
Outputs:
- output 1: bfloat16 [4096, 3072], P(None, 'model')
- output 2: bfloat16 [2, 4096, 16, 256], P(None, None, 'heads')
- output 3: bfloat16 [2, 4096, 16, 256], P(None, None, 'heads')
All inputs are finite; a program needn't handle non-finite values.
Results may differ from the reference program's by a relative error of at most 0.02.
Values are sent between devices in bfloat16 or wider.
A program may use at most 1 GiB of HBM per device.

```python
import jax
import jax.numpy as jnp
from jax import lax

TOKENS = 4096
D_MODEL = 3072
Q_HEADS = 16
KV_HEADS = 16
HEAD_DIM = 256
FFN_DIM = 24576
WINDOW = 1024
REQUESTS = 8
Q_BLOCK = 256
OUTLIERS = 8
NORM_EPS = 1e-6
GLOBAL_BASE = 1000000.0
GLOBAL_FACTOR = 8.0
LOCAL_BASE = 10000.0


def draw_requests(rng_key):
    cut_points = jnp.sort(jax.random.permutation(rng_key, TOKENS - 1)[:REQUESTS - 1] + 1).astype(jnp.int32)
    tok_index = jnp.arange(TOKENS, dtype=jnp.int32)
    seg_ids = jnp.sum((tok_index[:, None] >= cut_points[None, :]).astype(jnp.int32), axis=1)
    starts = jnp.concatenate([jnp.zeros((1,), jnp.int32), cut_points])
    positions = tok_index - starts[seg_ids]
    return seg_ids.astype(jnp.int32), positions.astype(jnp.int32)


def gauss_weight(rng_key, arr_shape, fan_in):
    return jax.random.normal(rng_key, arr_shape, jnp.float32) * (fan_in ** -0.5)


def setup_inputs(seed: int = 0) -> dict:
    rng_keys = jax.random.split(jax.random.key(seed), 16)
    seg_ids, positions = draw_requests(rng_keys[0])
    col_scale = jnp.exp(0.6 * jax.random.normal(rng_keys[1], (D_MODEL,), jnp.float32))
    hot_cols = jax.random.permutation(rng_keys[2], D_MODEL)[:OUTLIERS]
    col_scale = col_scale.at[hot_cols].set(20.0)
    hidden = jax.random.normal(rng_keys[3], (TOKENS, D_MODEL), jnp.float32) * col_scale[None, :]
    hidden = hidden * lax.rsqrt(jnp.mean(hidden * hidden))
    q_width = Q_HEADS * HEAD_DIM
    kv_width = KV_HEADS * HEAD_DIM
    out_cols = jnp.exp(0.5 * jax.random.normal(rng_keys[4], (2, 1, D_MODEL), jnp.float32))
    down_cols = jnp.exp(0.5 * jax.random.normal(rng_keys[5], (2, 1, D_MODEL), jnp.float32))
    return {
        'hidden_in': hidden.astype(jnp.bfloat16),
        'seg_ids': seg_ids,
        'positions': positions,
        'w_query': gauss_weight(rng_keys[6], (2, D_MODEL, q_width), D_MODEL).astype(jnp.bfloat16),
        'w_key': gauss_weight(rng_keys[7], (2, D_MODEL, kv_width), D_MODEL).astype(jnp.bfloat16),
        'w_value': gauss_weight(rng_keys[8], (2, D_MODEL, kv_width), D_MODEL).astype(jnp.bfloat16),
        'w_out': (gauss_weight(rng_keys[9], (2, q_width, D_MODEL), q_width) * out_cols).astype(jnp.bfloat16),
        'w_gate': gauss_weight(rng_keys[10], (2, D_MODEL, FFN_DIM), D_MODEL).astype(jnp.bfloat16),
        'w_up': gauss_weight(rng_keys[11], (2, D_MODEL, FFN_DIM), D_MODEL).astype(jnp.bfloat16),
        'w_down': (gauss_weight(rng_keys[12], (2, FFN_DIM, D_MODEL), FFN_DIM) * down_cols).astype(jnp.bfloat16),
        'norm_scales': 0.5 * jax.random.normal(rng_keys[13], (2, 4, D_MODEL), jnp.float32),
        'qk_scales': 0.5 * jax.random.normal(rng_keys[14], (2, 2, HEAD_DIM), jnp.float32),
    }


def gemma_norm(values, scale_row):
    mean_sq = jnp.mean(values * values, axis=-1, keepdims=True)
    return values * lax.rsqrt(mean_sq + NORM_EPS) * (1.0 + scale_row)


def rope_tables(positions, rope_base, pos_factor):
    exponents = jnp.arange(0, HEAD_DIM, 2).astype(jnp.float32) / HEAD_DIM
    inv_freq = rope_base ** (-exponents)
    angles = (positions.astype(jnp.float32) / pos_factor)[:, None] * inv_freq[None, :]
    return jnp.cos(angles), jnp.sin(angles)


def apply_rope(values, cos_tab, sin_tab):
    half_dim = values.shape[-1] // 2
    first_half = values[..., :half_dim]
    second_half = values[..., half_dim:]
    cos_bcast = cos_tab[:, None, :]
    sin_bcast = sin_tab[:, None, :]
    return jnp.concatenate([first_half * cos_bcast - second_half * sin_bcast, second_half * cos_bcast + first_half * sin_bcast], axis=-1)


def attend(query_heads, key_heads, value_heads, seg_ids, positions, window):
    group_size = Q_HEADS // KV_HEADS
    n_blocks = TOKENS // Q_BLOCK
    q_scale = HEAD_DIM ** -0.5
    key_f32 = key_heads.astype(jnp.float32)
    value_f32 = value_heads.astype(jnp.float32)
    q_blocks = query_heads.reshape(n_blocks, Q_BLOCK, KV_HEADS, group_size, HEAD_DIM)
    seg_blocks = seg_ids.reshape(n_blocks, Q_BLOCK)
    pos_blocks = positions.reshape(n_blocks, Q_BLOCK)

    def one_block(block_args):
        q_blk, seg_blk, pos_blk = block_args
        scores = jnp.einsum('qkgd,tkd->kgqt', q_blk.astype(jnp.float32), key_f32) * q_scale
        pos_gap = pos_blk[:, None] - positions[None, :]
        allowed = (seg_blk[:, None] == seg_ids[None, :]) & (pos_gap >= 0) & (pos_gap < window)
        scores = jnp.where(allowed[None, None], scores, -1e30)
        row_max = jnp.max(scores, axis=-1, keepdims=True)
        exp_scores = jnp.exp(scores - row_max)
        probs_bf = (exp_scores / jnp.sum(exp_scores, axis=-1, keepdims=True)).astype(jnp.bfloat16)
        blk_out = jnp.einsum('kgqt,tkd->qkgd', probs_bf.astype(jnp.float32), value_f32)
        return blk_out.astype(jnp.bfloat16)

    attn_out = lax.map(one_block, (q_blocks, seg_blocks, pos_blocks))
    return attn_out.reshape(TOKENS, Q_HEADS * HEAD_DIM)


def run_layer(hidden, seg_ids, positions, layer_w, norm_row, qk_row, rope_base, pos_factor, window):
    w_query, w_key, w_value, w_out, w_gate, w_up, w_down = layer_w
    resid_f32 = hidden.astype(jnp.float32)
    normed = gemma_norm(resid_f32, norm_row[0]).astype(jnp.bfloat16)
    query_bf = jnp.dot(normed, w_query, preferred_element_type=jnp.float32).astype(jnp.bfloat16)
    keys_bf = jnp.dot(normed, w_key, preferred_element_type=jnp.float32).astype(jnp.bfloat16)
    values_bf = jnp.dot(normed, w_value, preferred_element_type=jnp.float32).astype(jnp.bfloat16)
    cos_tab, sin_tab = rope_tables(positions, rope_base, pos_factor)
    query_heads = apply_rope(gemma_norm(query_bf.astype(jnp.float32).reshape(TOKENS, Q_HEADS, HEAD_DIM), qk_row[0]), cos_tab, sin_tab).astype(jnp.bfloat16)
    key_heads = apply_rope(gemma_norm(keys_bf.astype(jnp.float32).reshape(TOKENS, KV_HEADS, HEAD_DIM), qk_row[1]), cos_tab, sin_tab).astype(jnp.bfloat16)
    value_heads = values_bf.reshape(TOKENS, KV_HEADS, HEAD_DIM)
    attn_out = attend(query_heads, key_heads, value_heads, seg_ids, positions, window)
    attn_sum = jnp.dot(attn_out, w_out, preferred_element_type=jnp.float32).astype(jnp.bfloat16)
    hidden_mid = (resid_f32 + gemma_norm(attn_sum.astype(jnp.float32), norm_row[1])).astype(jnp.bfloat16)
    mid_f32 = hidden_mid.astype(jnp.float32)
    normed_ffn = gemma_norm(mid_f32, norm_row[2]).astype(jnp.bfloat16)
    gate_bf = jnp.dot(normed_ffn, w_gate, preferred_element_type=jnp.float32).astype(jnp.bfloat16)
    up_bf = jnp.dot(normed_ffn, w_up, preferred_element_type=jnp.float32).astype(jnp.bfloat16)
    ffn_in = (jax.nn.gelu(gate_bf.astype(jnp.float32), approximate=True) * up_bf.astype(jnp.float32)).astype(jnp.bfloat16)
    ffn_sum = jnp.dot(ffn_in, w_down, preferred_element_type=jnp.float32).astype(jnp.bfloat16)
    hidden_new = (mid_f32 + gemma_norm(ffn_sum.astype(jnp.float32), norm_row[3])).astype(jnp.bfloat16)
    return hidden_new, key_heads, value_heads


def reference(hidden_in, seg_ids, positions, w_query, w_key, w_value, w_out, w_gate, w_up, w_down, norm_scales, qk_scales):
    settings = ((GLOBAL_BASE, GLOBAL_FACTOR, TOKENS), (LOCAL_BASE, 1.0, WINDOW))
    hidden = hidden_in
    key_list = []
    value_list = []
    for layer_idx in range(2):
        rope_base, pos_factor, window = settings[layer_idx]
        layer_w = (w_query[layer_idx], w_key[layer_idx], w_value[layer_idx], w_out[layer_idx], w_gate[layer_idx], w_up[layer_idx], w_down[layer_idx])
        hidden, key_heads, value_heads = run_layer(hidden, seg_ids, positions, layer_w, norm_scales[layer_idx], qk_scales[layer_idx], rope_base, pos_factor, window)
        key_list.append(key_heads)
        value_list.append(value_heads)
    return hidden, jnp.stack(key_list), jnp.stack(value_list)
```

```python
import jax
import jax.numpy as jnp
from jax import lax
from jax.sharding import PartitionSpec as P

NORM_EPS = 1e-6
WINDOW = 1024
GLOBAL_BASE = 1000000.0
GLOBAL_FACTOR = 8.0
LOCAL_BASE = 10000.0


def norm(values, scale_row):
    mean_sq = jnp.mean(values * values, axis=-1, keepdims=True)
    return values * lax.rsqrt(mean_sq + NORM_EPS) * (1.0 + scale_row)


def rope_tables(positions, head_dim, rope_base, pos_factor):
    exponents = jnp.arange(0, head_dim, 2).astype(jnp.float32) / head_dim
    inv_freq = rope_base ** (-exponents)
    angles = (positions.astype(jnp.float32) / pos_factor)[:, None] * inv_freq[None, :]
    return jnp.cos(angles), jnp.sin(angles)


def apply_rope(values, cos_tab, sin_tab):
    half_dim = values.shape[-1] // 2
    first_half = values[..., :half_dim]
    second_half = values[..., half_dim:]
    return jnp.concatenate([first_half * cos_tab - second_half * sin_tab, second_half * cos_tab + first_half * sin_tab], axis=-1)


def attend(q, k, v, seg_q, pos_q, seg_ids, positions, window):
    scores = jnp.dot(q, k.T, preferred_element_type=jnp.float32) * (q.shape[-1] ** -0.5)
    gap = pos_q[:, None] - positions[None, :]
    allowed = (seg_q[:, None] == seg_ids[None, :]) & (gap >= 0) & (gap < window)
    scores = jnp.where(allowed, scores, -1e30)
    row_max = jnp.max(scores, axis=-1, keepdims=True)
    e = jnp.exp(scores - row_max)
    p = (e / jnp.sum(e, axis=-1, keepdims=True)).astype(jnp.bfloat16)
    return jnp.dot(p, v, preferred_element_type=jnp.float32).astype(jnp.bfloat16)


def solution(mesh):
    n_model = mesh.shape['model']
    n_heads = mesh.shape['heads']
    col_spec = P(None, 'model', 'heads')
    row_spec = P(None, 'heads', 'model')
    cache_spec = P(None, None, 'heads', None)

    def body(hidden_in, seg_ids, positions, w_query, w_key, w_value, w_out, w_gate, w_up, w_down, norm_scales, qk_scales):
        n_tok, width_loc = hidden_in.shape
        width = width_loc * n_model
        head_dim = qk_scales.shape[-1]
        tok_m = n_tok // n_model
        tok_own = tok_m // n_heads
        hd = lax.axis_index('heads')
        md = lax.axis_index('model')

        def gather_rows(w):
            return lax.all_gather(w, 'model', axis=0, tiled=True)

        def gather_cols(w):
            return lax.all_gather(w, 'model', axis=0)

        def dot_cols(a, w):
            parts = [jnp.dot(a, w[i], preferred_element_type=jnp.float32) for i in range(n_model)]
            return jnp.concatenate(parts, axis=1)

        scales = lax.all_gather(norm_scales, 'model', axis=2, tiled=True)
        mine = lax.dynamic_index_in_dim(hidden_in.reshape(n_model, n_heads, tok_own, width_loc), hd, 1, keepdims=False)
        mine = lax.all_to_all(mine, 'model', split_axis=0, concat_axis=0)
        resid = mine.transpose(1, 0, 2).reshape(tok_own, width)

        pos_m = lax.dynamic_slice_in_dim(positions, md * tok_m, tok_m)
        seg_m = lax.dynamic_slice_in_dim(seg_ids, md * tok_m, tok_m)

        settings = ((GLOBAL_BASE, GLOBAL_FACTOR, n_tok), (LOCAL_BASE, 1.0, WINDOW))
        keys, values = [], []
        for l in range(2):
            rope_base, pos_factor, window = settings[l]
            resid_f32 = resid.astype(jnp.float32)
            h_own = norm(resid_f32, scales[l, 0]).astype(jnp.bfloat16)
            h = lax.all_gather(h_own, 'heads', axis=0, tiled=True)
            wq, wk, wv = gather_rows(w_query[l]), gather_rows(w_key[l]), gather_rows(w_value[l])
            q = jnp.dot(h, wq, preferred_element_type=jnp.float32).astype(jnp.bfloat16)
            k = jnp.dot(h, wk, preferred_element_type=jnp.float32).astype(jnp.bfloat16)
            v = jnp.dot(h, wv, preferred_element_type=jnp.float32).astype(jnp.bfloat16)
            cos_tab, sin_tab = rope_tables(pos_m, head_dim, rope_base, pos_factor)
            q = apply_rope(norm(q.astype(jnp.float32), qk_scales[l, 0]), cos_tab, sin_tab).astype(jnp.bfloat16)
            k = apply_rope(norm(k.astype(jnp.float32), qk_scales[l, 1]), cos_tab, sin_tab).astype(jnp.bfloat16)
            k_all = lax.all_gather(k, 'model', axis=0, tiled=True)
            v_all = lax.all_gather(v, 'model', axis=0, tiled=True)
            keys.append(k_all[:, None, :])
            values.append(v_all[:, None, :])
            o = attend(q, k_all, v_all, seg_m, pos_m, seg_ids, positions, window)
            wo = gather_cols(w_out[l])
            a = lax.psum_scatter(dot_cols(o, wo), 'heads', scatter_dimension=0, tiled=True).astype(jnp.bfloat16)
            x1 = (resid_f32 + norm(a.astype(jnp.float32), scales[l, 1])).astype(jnp.bfloat16)
            x1_f32 = x1.astype(jnp.float32)
            h2_own = norm(x1_f32, scales[l, 2]).astype(jnp.bfloat16)
            h2 = lax.all_gather(h2_own, 'heads', axis=0, tiled=True)
            wg, wu = gather_rows(w_gate[l]), gather_rows(w_up[l])
            g = jnp.dot(h2, wg, preferred_element_type=jnp.float32).astype(jnp.bfloat16)
            u = jnp.dot(h2, wu, preferred_element_type=jnp.float32).astype(jnp.bfloat16)
            mid = (jax.nn.gelu(g.astype(jnp.float32), approximate=True) * u.astype(jnp.float32)).astype(jnp.bfloat16)
            wd = gather_cols(w_down[l])
            f = lax.psum_scatter(dot_cols(mid, wd), 'heads', scatter_dimension=0, tiled=True).astype(jnp.bfloat16)
            resid = (x1_f32 + norm(f.astype(jnp.float32), scales[l, 3])).astype(jnp.bfloat16)
        out = resid.reshape(tok_own, n_model, width_loc).transpose(1, 0, 2)
        out = lax.all_to_all(out, 'model', split_axis=0, concat_axis=0)
        out = lax.all_gather(out, 'heads', axis=1).reshape(n_tok, width_loc)
        return out, jnp.stack(keys), jnp.stack(values)

    return jax.shard_map(body, mesh=mesh,
                         in_specs=(P(None, 'model'), P(), P(), col_spec, col_spec, col_spec, row_spec, col_spec, col_spec, row_spec, P(None, None, 'model'), P()),
                         out_specs=(P(None, 'model'), cache_spec, cache_spec),
                         check_vma=False)
```

```python
import functools

import jax
import jax.numpy as jnp
from jax import lax
from jax.experimental import pallas as pl
from jax.experimental.pallas import tpu as pltpu
from jax.sharding import PartitionSpec as P

NORM_EPS = 1e-6
WINDOW = 1024
GLOBAL_BASE = 1000000.0
GLOBAL_FACTOR = 8.0
LOCAL_BASE = 10000.0
MESH = pl.DeviceIdType.MESH
SIDE = 4
COLORS = 4
VMEM_LIMIT = 60 * 1024 * 1024


def norm(values, scale_row):
    mean_sq = jnp.mean(values * values, axis=-1, keepdims=True)
    return values * lax.rsqrt(mean_sq + NORM_EPS) * (1.0 + scale_row)


def rope_tables(positions, head_dim, rope_base, pos_factor):
    exponents = jnp.arange(0, head_dim, 2).astype(jnp.float32) / head_dim
    inv_freq = rope_base ** (-exponents)
    angles = (positions.astype(jnp.float32) / pos_factor)[:, None] * inv_freq[None, :]
    return jnp.cos(angles), jnp.sin(angles)


def apply_rope(values, cos_tab, sin_tab):
    half_dim = values.shape[-1] // 2
    first_half = values[..., :half_dim]
    second_half = values[..., half_dim:]
    return jnp.concatenate([first_half * cos_tab - second_half * sin_tab, second_half * cos_tab + first_half * sin_tab], axis=-1)


def attend(q, k, v, seg_q, pos_q, seg_ids, positions, window):
    scores = jnp.dot(q, k.T, preferred_element_type=jnp.float32) * (q.shape[-1] ** -0.5)
    gap = pos_q[:, None] - positions[None, :]
    allowed = (seg_q[:, None] == seg_ids[None, :]) & (gap >= 0) & (gap < window)
    scores = jnp.where(allowed, scores, -1e30)
    row_max = jnp.max(scores, axis=-1, keepdims=True)
    e = jnp.exp(scores - row_max)
    p = (e / jnp.sum(e, axis=-1, keepdims=True)).astype(jnp.bfloat16)
    return jnp.dot(p, v, preferred_element_type=jnp.float32).astype(jnp.bfloat16)


def wrap(i):
    return lax.rem(i + 2 * SIDE, SIDE)


class Torus:
    def __init__(self):
        me = lax.axis_index('heads')
        self.z = me // SIDE
        self.y = lax.rem(me, SIDE)

    def own(self, axis):
        return self.y if axis == 0 else self.z

    def block(self, axis, along, across):
        return across * SIDE + along if axis == 0 else along * SIDE + across

    def peer(self, axis, step):
        moved = wrap(self.own(axis) + step)
        return self.block(axis, moved, self.own(1 - axis))

    def meet(self):
        barrier = pltpu.get_barrier_semaphore()
        for axis in (0, 1):
            for step in (1, -1):
                pl.semaphore_signal(barrier, inc=1, device_id={'heads': self.peer(axis, step)}, device_id_type=MESH)
        pl.semaphore_wait(barrier, 4)


def gather_blocks(torus, h_ref, send1, recv1, send2, recv2):
    rows = h_ref.shape[0] // (SIDE * SIDE)
    cols = h_ref.shape[1] // COLORS

    def view(q, axis, along, across):
        b = torus.block(axis, along, across)
        return h_ref.at[pl.ds(pl.multiple_of(b * rows, rows), rows), pl.ds(q * cols, cols)]

    def hop1(q, s):
        axis, d = q // 2, 1 - 2 * (q % 2)
        i, j = torus.own(axis), torus.own(1 - axis)
        v = view(q, axis, i, wrap(j - d * s))
        return pltpu.make_async_remote_copy(v, v, send1.at[q, s], recv1.at[q, s], device_id={'heads': torus.peer(1 - axis, d)}, device_id_type=MESH)

    def hop2(q, t, n):
        axis, d = q // 2, 1 - 2 * (q % 2)
        i, j = torus.own(axis), torus.own(1 - axis)
        v = view(q, axis, wrap(i - d * t), wrap(j - d * n))
        return pltpu.make_async_remote_copy(v, v, send2.at[q, t, n], recv2.at[q, t, n], device_id={'heads': torus.peer(axis, d)}, device_id_type=MESH)

    for q in range(COLORS):
        hop1(q, 0).start()
    for q in range(COLORS):
        hop2(q, 0, 0).start()
    for s in range(SIDE - 1):
        for q in range(COLORS):
            hop1(q, s).wait_recv()
            if s < SIDE - 2:
                hop1(q, s + 1).start()
            hop2(q, 0, s + 1).start()
    for t in range(SIDE - 1):
        for n in range(SIDE):
            for q in range(COLORS):
                hop2(q, t, n).wait_recv()
                if t < SIDE - 2:
                    hop2(q, t + 1, n).start()
    for q in range(COLORS):
        for s in range(SIDE - 1):
            hop1(q, s).wait_send()
            for n in range(SIDE):
                hop2(q, s, n).wait_send()


GATHER_SEMS = [pltpu.SemaphoreType.DMA((COLORS, SIDE - 1)), pltpu.SemaphoreType.DMA((COLORS, SIDE - 1)),
               pltpu.SemaphoreType.DMA((COLORS, SIDE - 1, SIDE)), pltpu.SemaphoreType.DMA((COLORS, SIDE - 1, SIDE))]


def gather_kernel(x_ref, h_ref, send1, recv1, send2, recv2):
    torus = Torus()
    rows = x_ref.shape[0]
    torus.meet()
    mine = torus.block(0, torus.y, torus.z)
    h_ref[pl.ds(pl.multiple_of(mine * rows, rows), rows), :] = x_ref[...]
    gather_blocks(torus, h_ref, send1, recv1, send2, recv2)


def all_gather_heads(x, cid):
    rows, width = x.shape
    vmem = pl.BlockSpec(memory_space=pltpu.VMEM)
    return pl.pallas_call(
        gather_kernel,
        out_shape=jax.ShapeDtypeStruct((rows * SIDE * SIDE, width), x.dtype),
        in_specs=[vmem], out_specs=vmem,
        scratch_shapes=list(GATHER_SEMS),
        compiler_params=pltpu.CompilerParams(collective_id=cid, has_side_effects=True, vmem_limit_bytes=VMEM_LIMIT),
        cost_estimate=pl.CostEstimate(flops=20_000_000_000, bytes_accessed=4_000_000, transcendentals=0),
        name='gather_heads',
    )(x)


def project_kernel(transposed, gather, a_ref, w_ref, res_ref, sa_ref, sb_ref, x_ref, h_ref,
                   first, slots1, slots2, s1, r1, s2, r2, gs1=None, gr1=None, gs2=None, gr2=None):
    torus = Torus()
    rows = res_ref.shape[0]
    cols = slots1.shape[-1]
    torus.meet()

    def ring1(q, s, n):
        axis, d = q // 2, 1 - 2 * (q % 2)
        src = first.at[q, n] if s == 0 else slots1.at[q, s - 1, n]
        return pltpu.make_async_remote_copy(src, slots1.at[q, s, n], s1.at[q, s, n], r1.at[q, s, n],
                                            device_id={'heads': torus.peer(axis, d)}, device_id_type=MESH)

    def ring2(q, t):
        axis, d = q // 2, 1 - 2 * (q % 2)
        src = slots1.at[q, SIDE - 2, 0] if t == 0 else slots2.at[q, t - 1]
        return pltpu.make_async_remote_copy(src, slots2.at[q, t], s2.at[q, t], r2.at[q, t],
                                            device_id={'heads': torus.peer(1 - axis, d)}, device_id_type=MESH)

    def product(q, s):
        axis, d = q // 2, 1 - 2 * (q % 2)
        along = wrap(torus.own(axis) - d * (1 + s))
        parts = []
        for n in range(SIDE):
            b = torus.block(axis, along, wrap(torus.own(1 - axis) - d * (1 + n)))
            parts.append(a_ref[pl.ds(pl.multiple_of(b * rows, rows), rows), :])
        lhs = jnp.concatenate(parts, axis=0)
        if transposed:
            return [lax.dot_general(lhs, w_ref[q * cols:(q + 1) * cols, :], (((1,), (1,)), ((), ())), preferred_element_type=jnp.float32)]
        per = cols // w_ref.shape[2]
        return [jnp.dot(lhs, w_ref[q * per + p], preferred_element_type=jnp.float32) for p in range(per)]

    for s in range(SIDE):
        for q in range(COLORS):
            pieces = product(q, s)
            for n in range(SIDE):
                if s > 0:
                    ring1(q, s - 1, n).wait_recv()
                at = 0
                for piece in pieces:
                    part = piece[n * rows:(n + 1) * rows]
                    span = slice(at, at + part.shape[1])
                    at += part.shape[1]
                    if s == 0:
                        first[q, n, :, span] = part
                    else:
                        slots1[q, s - 1, n, :, span] += part
                if s < SIDE - 1:
                    ring1(q, s, n).start()
                elif n == 0:
                    ring2(q, 0).start()
    for t in range(SIDE - 1):
        for q in range(COLORS):
            ring2(q, t).wait_recv()
            slots2[q, t] += slots1[q, SIDE - 2, t + 1]
            if t < SIDE - 2:
                ring2(q, t + 1).start()
    total = jnp.concatenate([slots2[q, SIDE - 2] for q in range(COLORS)], axis=1)
    out = total.astype(jnp.bfloat16).astype(jnp.float32)
    x_new = (res_ref[...].astype(jnp.float32) + norm(out, sa_ref[...])).astype(jnp.bfloat16)
    x_ref[...] = x_new
    if gather:
        mine = torus.block(0, torus.y, torus.z)
        h_ref[pl.ds(pl.multiple_of(mine * rows, rows), rows), :] = norm(x_new.astype(jnp.float32), sb_ref[...]).astype(jnp.bfloat16)
    for q in range(COLORS):
        for s in range(SIDE - 1):
            ring2(q, s).wait_send()
            for n in range(SIDE):
                ring1(q, s, n).wait_send()
    if gather:
        gather_blocks(torus, h_ref, gs1, gr1, gs2, gr2)


def project(a, w, resid, scale_a, scale_b, cid, transposed, gather):
    rows, width = resid.shape
    cols = width // COLORS
    vmem = pl.BlockSpec(memory_space=pltpu.VMEM)
    ring_sems = [pltpu.SemaphoreType.DMA((COLORS, SIDE - 1, SIDE)), pltpu.SemaphoreType.DMA((COLORS, SIDE - 1, SIDE)),
                 pltpu.SemaphoreType.DMA((COLORS, SIDE - 1)), pltpu.SemaphoreType.DMA((COLORS, SIDE - 1))]
    scratch = [pltpu.VMEM((COLORS, SIDE, rows, cols), jnp.float32),
               pltpu.VMEM((COLORS, SIDE - 1, SIDE, rows, cols), jnp.float32),
               pltpu.VMEM((COLORS, SIDE - 1, rows, cols), jnp.float32)] + ring_sems
    x_shape = jax.ShapeDtypeStruct((rows, width), jnp.bfloat16)
    h_shape = jax.ShapeDtypeStruct((rows * SIDE * SIDE, width), jnp.bfloat16)
    if gather:
        kernel = functools.partial(project_kernel, transposed, True)
        out_shape, out_specs, scratch = (x_shape, h_shape), (vmem, vmem), scratch + GATHER_SEMS
    else:
        def kernel(a_ref, w_ref, res_ref, sa_ref, sb_ref, x_ref, *rest):
            project_kernel(transposed, False, a_ref, w_ref, res_ref, sa_ref, sb_ref, x_ref, None, *rest)
        out_shape, out_specs = x_shape, vmem
    return pl.pallas_call(
        kernel, out_shape=out_shape, in_specs=[vmem] * 5, out_specs=out_specs, scratch_shapes=scratch,
        compiler_params=pltpu.CompilerParams(collective_id=cid, has_side_effects=True, vmem_limit_bytes=VMEM_LIMIT),
        cost_estimate=pl.CostEstimate(flops=50_000_000_000, bytes_accessed=20_000_000, transcendentals=0),
        name='project_reduce',
    )(a, w, resid, scale_a, scale_b)


def exchange_kernel(n_chips, k_ref, v_ref, ka_ref, va_ref, send, recv):
    md = lax.axis_index('model')
    chip, core = md // 2, lax.rem(md, 2)
    right = lax.rem(chip + 1, n_chips) * 2 + core
    left = lax.rem(chip + n_chips - 1, n_chips) * 2 + core
    mate = chip * 2 + 1 - core
    rows = k_ref.shape[0]
    half = rows // 2
    barrier = pltpu.get_barrier_semaphore()
    for other in (right, left, mate):
        pl.semaphore_signal(barrier, inc=1, device_id={'model': other}, device_id_type=MESH)
    pl.semaphore_wait(barrier, 3)
    refs = (ka_ref, va_ref)
    here = pl.ds(pl.multiple_of(md * rows, rows), rows)
    ka_ref[here, :] = k_ref[...]
    va_ref[here, :] = v_ref[...]

    def copy(a, slot, owner, to, part):
        start = owner * rows if part != 2 else owner * rows + half
        size = rows if part == 0 else half
        v = refs[a].at[pl.ds(pl.multiple_of(start, half), size), :]
        return pltpu.make_async_remote_copy(v, v, send.at[a, slot], recv.at[a, slot], device_id={'model': to}, device_id_type=MESH)

    far = lax.rem(chip + 2, n_chips) * 2 + core
    plan = [(0, md, right, 0), (1, md, left, 0), (2, md, mate, 0), (3, left, right, 1), (4, right, left, 2),
            (5, left, mate, 0), (6, right, mate, 0), (7, far, mate, 1), (8, far, mate, 2)]
    for slot in (0, 1, 2):
        for a in (0, 1):
            copy(a, *plan[slot]).start()
    for a in (0, 1):
        copy(a, *plan[0]).wait_recv()
        copy(a, *plan[3]).start()
        copy(a, *plan[1]).wait_recv()
        copy(a, *plan[4]).start()
        copy(a, *plan[5]).start()
        copy(a, *plan[6]).start()
    for a in (0, 1):
        copy(a, *plan[3]).wait_recv()
        copy(a, *plan[7]).start()
        copy(a, *plan[4]).wait_recv()
        copy(a, *plan[8]).start()
    for a in (0, 1):
        for slot in (2, 5, 6, 7, 8):
            copy(a, *plan[slot]).wait_recv()
        for slot in range(9):
            copy(a, *plan[slot]).wait_send()


def exchange(k, v, n_model, cid):
    rows, dim = k.shape
    vmem = pl.BlockSpec(memory_space=pltpu.VMEM)
    full = jax.ShapeDtypeStruct((rows * n_model, dim), k.dtype)
    return pl.pallas_call(
        functools.partial(exchange_kernel, n_model // 2),
        out_shape=(full, full), in_specs=[vmem] * 2, out_specs=(vmem, vmem),
        scratch_shapes=[pltpu.SemaphoreType.DMA((2, 9)), pltpu.SemaphoreType.DMA((2, 9))],
        compiler_params=pltpu.CompilerParams(collective_id=cid, has_side_effects=True, vmem_limit_bytes=VMEM_LIMIT),
        cost_estimate=pl.CostEstimate(flops=20_000_000_000, bytes_accessed=5_000_000, transcendentals=0),
        name='exchange_kv',
    )(k, v)


def solution(mesh):
    n_model = mesh.shape['model']
    n_heads = mesh.shape['heads']
    col_spec = P(None, 'model', 'heads')
    row_spec = P(None, 'heads', 'model')
    cache_spec = P(None, None, 'heads', None)

    def body(hidden_in, seg_ids, positions, w_query, w_key, w_value, w_out, w_gate, w_up, w_down, norm_scales, qk_scales):
        n_tok, width_loc = hidden_in.shape
        width = width_loc * n_model
        head_dim = qk_scales.shape[-1]
        tok_m = n_tok // n_model
        tok_own = tok_m // n_heads
        hd = lax.axis_index('heads')
        md = lax.axis_index('model')

        attn_w, gate_w, up_w, down_w = [], [], [], []
        for l in range(2):
            packed = jnp.concatenate([w_query[l], w_key[l], w_value[l], w_out[l].T], axis=1)
            attn_w.append(lax.all_gather(packed, 'model', axis=0, tiled=True))
            gate_w.append(lax.all_gather(w_gate[l], 'model', axis=0, tiled=True))
            up_w.append(lax.all_gather(w_up[l], 'model', axis=0, tiled=True))
            down_w.append(lax.all_gather(w_down[l], 'model', axis=0))

        scales = lax.all_gather(norm_scales, 'model', axis=2, tiled=True)
        mine = lax.dynamic_index_in_dim(hidden_in.reshape(n_model, n_heads, tok_own, width_loc), hd, 1, keepdims=False)
        mine = lax.all_to_all(mine, 'model', split_axis=0, concat_axis=0)
        resid = mine.transpose(1, 0, 2).reshape(tok_own, width)

        pos_m = lax.dynamic_slice_in_dim(positions, md * tok_m, tok_m)
        seg_m = lax.dynamic_slice_in_dim(seg_ids, md * tok_m, tok_m)

        settings = ((GLOBAL_BASE, GLOBAL_FACTOR, n_tok), (LOCAL_BASE, 1.0, WINDOW))
        keys, values = [], []
        h = all_gather_heads(norm(resid.astype(jnp.float32), scales[0, 0]).astype(jnp.bfloat16), 0)
        for l in range(2):
            rope_base, pos_factor, window = settings[l]
            wa = attn_w[l]
            qkv = jnp.dot(h, wa[:, :3 * head_dim], preferred_element_type=jnp.float32).astype(jnp.bfloat16)
            q, k, v = qkv[:, :head_dim], qkv[:, head_dim:2 * head_dim], qkv[:, 2 * head_dim:]
            cos_tab, sin_tab = rope_tables(pos_m, head_dim, rope_base, pos_factor)
            q = apply_rope(norm(q.astype(jnp.float32), qk_scales[l, 0]), cos_tab, sin_tab).astype(jnp.bfloat16)
            k = apply_rope(norm(k.astype(jnp.float32), qk_scales[l, 1]), cos_tab, sin_tab).astype(jnp.bfloat16)
            k_all, v_all = exchange(k, v, n_model, 1 + 3 * l)
            keys.append(k_all[:, None, :])
            values.append(v_all[:, None, :])
            o = attend(q, k_all, v_all, seg_m, pos_m, seg_ids, positions, window)
            x1, h2 = project(o, wa[:, 3 * head_dim:], resid, scales[l, 1:2], scales[l, 2:3], 2 + 3 * l, True, True)
            g = jnp.dot(h2, gate_w[l], preferred_element_type=jnp.float32).astype(jnp.bfloat16)
            u = jnp.dot(h2, up_w[l], preferred_element_type=jnp.float32).astype(jnp.bfloat16)
            mid = (jax.nn.gelu(g.astype(jnp.float32), approximate=True) * u.astype(jnp.float32)).astype(jnp.bfloat16)
            if l == 0:
                resid, h = project(mid, down_w[l], x1, scales[0, 3:4], scales[1, 0:1], 3 + 3 * l, False, True)
            else:
                resid = project(mid, down_w[l], x1, scales[1, 3:4], scales[1, 3:4], 3 + 3 * l, False, False)
        out = resid.reshape(tok_own, n_model, width_loc).transpose(1, 0, 2)
        out = lax.all_to_all(out, 'model', split_axis=0, concat_axis=0)
        out = all_gather_heads(out.transpose(1, 0, 2).reshape(tok_own, width), 7)
        out = out.reshape(tok_m, n_model, width_loc).transpose(1, 0, 2).reshape(n_tok, width_loc)
        return out, jnp.stack(keys), jnp.stack(values)

    return jax.shard_map(body, mesh=mesh,
                         in_specs=(P(None, 'model'), P(), P(), col_spec, col_spec, col_spec, row_spec, col_spec, col_spec, row_spec, P(None, None, 'model'), P()),
                         out_specs=(P(None, 'model'), cache_spec, cache_spec),
                         check_vma=False)
```

```python
import functools

import jax
import jax.numpy as jnp
from jax import lax
from jax.experimental import pallas as pl
from jax.experimental.pallas import tpu as pltpu
from jax.sharding import PartitionSpec as P

NORM_EPS = 1e-6
WINDOW = 1024
GLOBAL_BASE = 1000000.0
GLOBAL_FACTOR = 8.0
LOCAL_BASE = 10000.0
MESH = pl.DeviceIdType.MESH
SIDE = 4
VMEM_LIMIT = 60 * 1024 * 1024


def norm(values, scale_row):
    mean_sq = jnp.mean(values * values, axis=-1, keepdims=True)
    return values * lax.rsqrt(mean_sq + NORM_EPS) * (1.0 + scale_row)


def rope_tables(positions, head_dim, rope_base, pos_factor):
    exponents = jnp.arange(0, head_dim, 2).astype(jnp.float32) / head_dim
    inv_freq = rope_base ** (-exponents)
    angles = (positions.astype(jnp.float32) / pos_factor)[:, None] * inv_freq[None, :]
    return jnp.cos(angles), jnp.sin(angles)


def apply_rope(values, cos_tab, sin_tab):
    half_dim = values.shape[-1] // 2
    first_half = values[..., :half_dim]
    second_half = values[..., half_dim:]
    return jnp.concatenate([first_half * cos_tab - second_half * sin_tab, second_half * cos_tab + first_half * sin_tab], axis=-1)


def attend(q, k, v, seg_q, pos_q, seg_ids, positions, window):
    scores = jnp.dot(q, k.T, preferred_element_type=jnp.float32) * (q.shape[-1] ** -0.5)
    gap = pos_q[:, None] - positions[None, :]
    allowed = (seg_q[:, None] == seg_ids[None, :]) & (gap >= 0) & (gap < window)
    scores = jnp.where(allowed, scores, -1e30)
    row_max = jnp.max(scores, axis=-1, keepdims=True)
    e = jnp.exp(scores - row_max)
    p = (e / jnp.sum(e, axis=-1, keepdims=True)).astype(jnp.bfloat16)
    return jnp.dot(p, v, preferred_element_type=jnp.float32).astype(jnp.bfloat16)


def wrap(i):
    return lax.rem(i + 2 * SIDE, SIDE)


def remote(src, dst, send, recv, to):
    return pltpu.make_async_remote_copy(src, dst, send, recv, device_id=to, device_id_type=MESH)


def row_block(ref, start, size, align):
    return ref.at[pl.ds(pl.multiple_of(start, align), size), :]


class Torus:
    def __init__(self):
        me = lax.axis_index('heads')
        self.own = (lax.rem(me, SIDE), me // SIDE)

    def block(self, axis, along, across):
        return across * SIDE + along if axis == 0 else along * SIDE + across

    def at(self, axis, da, db):
        return self.block(axis, wrap(self.own[axis] + da), wrap(self.own[1 - axis] + db))

    def peer(self, axis, step):
        return {'heads': self.at(axis, step, 0)}


class Line:
    def __init__(self, n_model):
        self.n = n_model
        self.me = lax.axis_index('model')
        chips = n_model // 2
        chip, core = self.me // 2, lax.rem(self.me, 2)
        self.right = lax.rem(chip + 1, chips) * 2 + core
        self.left = lax.rem(chip + chips - 1, chips) * 2 + core
        self.far = lax.rem(chip + 2, chips) * 2 + core
        self.mate = chip * 2 + 1 - core


def meet(torus, models):
    barrier = pltpu.get_barrier_semaphore()
    count = len(models)
    for other in models:
        pl.semaphore_signal(barrier, inc=1, device_id={'model': other}, device_id_type=MESH)
    if torus is not None:
        for axis in (0, 1):
            for step in (1, -1):
                pl.semaphore_signal(barrier, inc=1, device_id=torus.peer(axis, step), device_id_type=MESH)
                count += 1
    pl.semaphore_wait(barrier, count)


def gather_blocks(torus, h_ref, send, recv):
    rows = h_ref.shape[0] // (SIDE * SIDE)
    cols = h_ref.shape[1] // 2
    half = rows // 2

    def view(q, da, db, part):
        start = torus.at(q, da, db) * rows + (half if part == 2 else 0)
        return h_ref.at[pl.ds(pl.multiple_of(start, half), rows if part == 0 else half), pl.ds(q * cols, cols)]

    def ring(q, axis, base, slot, offsets):
        def make(k, da, db, part, step):
            v = view(q, da, db, part)
            return remote(v, v, send.at[q, base, k], recv.at[q, base, k], torus.peer(axis, step))
        along = (lambda off: (off, offsets)) if axis == q else (lambda off: (offsets, off))
        return (make(0, *along(0), 0, 1), make(1, *along(0), 0, -1), make(2, *along(-1), 1, 1), make(3, *along(1), 2, -1))

    first = [ring(q, 1 - q, 0, 0, 0) for q in (0, 1)]
    second = [[ring(q, q, 1 + n, 0, off) for n, off in enumerate((0, -1, 1, 2))] for q in (0, 1)]

    def begin(copies):
        copies[0].start()
        copies[1].start()

    def onward(copies):
        copies[0].wait_recv()
        copies[2].start()
        copies[1].wait_recv()
        copies[3].start()

    for q in (0, 1):
        begin(first[q])
    for q in (0, 1):
        begin(second[q][0])
    for q in (0, 1):
        first[q][0].wait_recv()
        first[q][2].start()
        begin(second[q][1])
        first[q][1].wait_recv()
        first[q][3].start()
        begin(second[q][2])
    for q in (0, 1):
        onward(second[q][0])
    for q in (0, 1):
        first[q][2].wait_recv()
        first[q][3].wait_recv()
        begin(second[q][3])
    for n in (1, 2, 3):
        for q in (0, 1):
            onward(second[q][n])
    for q in (0, 1):
        for n in range(SIDE):
            second[q][n][2].wait_recv()
            second[q][n][3].wait_recv()
    for q in (0, 1):
        for copies in [first[q]] + second[q]:
            for c in copies:
                c.wait_send()


GATHER_SEMS = [pltpu.SemaphoreType.DMA((2, 1 + SIDE, 4)), pltpu.SemaphoreType.DMA((2, 1 + SIDE, 4))]


class Exchange:
    def __init__(self, line, refs, send, recv):
        self.refs = refs
        self.copies = []
        plan = [(line.me, line.right, 0), (line.me, line.left, 0), (line.me, line.mate, 0), (line.left, line.right, 1),
                (line.right, line.left, 2), (line.left, line.mate, 0), (line.right, line.mate, 0),
                (line.far, line.mate, 1), (line.far, line.mate, 2)]
        for a, ref in enumerate(refs):
            rows = ref.shape[0] // line.n
            half = rows // 2
            group = []
            for slot, (owner, to, part) in enumerate(plan):
                start = owner * rows + (half if part == 2 else 0)
                v = row_block(ref, start, rows if part == 0 else half, half)
                group.append(remote(v, v, send.at[a, slot], recv.at[a, slot], {'model': to}))
            self.copies.append(group)

    def begin(self):
        for c in self.copies:
            c[0].start()
            c[1].start()
            c[2].start()

    def onward(self):
        for c in self.copies:
            c[0].wait_recv()
            c[3].start()
            c[1].wait_recv()
            c[4].start()
            c[5].start()
            c[6].start()

    def finish(self):
        for c in self.copies:
            c[3].wait_recv()
            c[7].start()
            c[4].wait_recv()
            c[8].start()
        for c in self.copies:
            for slot in (2, 5, 6, 7, 8):
                c[slot].wait_recv()
            for one in c:
                one.wait_send()


def exchange_sems(count):
    return [pltpu.SemaphoreType.DMA((count, 9)), pltpu.SemaphoreType.DMA((count, 9))]


def exchange_kernel(n_model, k_ref, v_ref, ka_ref, va_ref, send, recv):
    line = Line(n_model)
    rows = k_ref.shape[0]
    meet(None, (line.right, line.left, line.mate))
    here = pl.ds(pl.multiple_of(line.me * rows, rows), rows)
    ka_ref[here, :] = k_ref[...]
    va_ref[here, :] = v_ref[...]
    ex = Exchange(line, (ka_ref, va_ref), send, recv)
    ex.begin()
    ex.onward()
    ex.finish()


VMEM = pl.BlockSpec(memory_space=pltpu.VMEM)


def params(cid):
    return pltpu.CompilerParams(collective_id=cid, has_side_effects=True, vmem_limit_bytes=VMEM_LIMIT)


def cost(flops):
    return pl.CostEstimate(flops=flops, bytes_accessed=10_000_000, transcendentals=0)


def exchange(k, v, n_model, cid):
    rows, dim = k.shape
    full = jax.ShapeDtypeStruct((rows * n_model, dim), k.dtype)
    return pl.pallas_call(
        functools.partial(exchange_kernel, n_model),
        out_shape=(full, full), in_specs=[VMEM] * 2, out_specs=(VMEM, VMEM),
        scratch_shapes=exchange_sems(2), compiler_params=params(cid), cost_estimate=cost(20_000_000_000), name='exchange_kv',
    )(k, v)


def load_attn_weights(line, layer, wq_ref, wk_ref, wv_ref, wo_ref, wqkv_ref, woa_ref):
    rows, dim = wq_ref.shape[1:]
    here = pl.ds(pl.multiple_of(line.me * rows, rows), rows)
    for at, ref in enumerate((wq_ref, wk_ref, wv_ref)):
        wqkv_ref[here, at * dim:(at + 1) * dim] = ref[layer]
    o_rows = wo_ref.shape[1]
    woa_ref[pl.ds(pl.multiple_of(line.me * o_rows, o_rows), o_rows), :] = wo_ref[layer]


def to_all(line, make):
    copies = []
    for step in range(1, line.n):
        peer = lax.rem(line.me + step, line.n)
        copies.append(make(step, peer))
    for c in copies:
        c.start()
    return copies


def others(line):
    return [lax.rem(line.me + step, line.n) for step in range(1, line.n)]


def start_kernel(n_model, hid_ref, sc_ref, wq_ref, wk_ref, wv_ref, wo_ref, x_ref, h_ref, sca_ref, wqkv_ref, woa_ref,
                 xin, scin, xs, xr, ss, sr, hs, hr, es, er):
    torus, line = Torus(), Line(n_model)
    rows = x_ref.shape[0]
    meet(torus, others(line))
    xin[line.me] = hid_ref[line.me]
    scin[line.me] = sc_ref[...]
    xc = to_all(line, lambda step, peer: remote(hid_ref.at[peer], xin.at[line.me], xs.at[step], xr.at[step], {'model': peer}))
    sc = to_all(line, lambda step, peer: remote(sc_ref, scin.at[line.me], ss.at[step], sr.at[step], {'model': peer}))
    load_attn_weights(line, 0, wq_ref, wk_ref, wv_ref, wo_ref, wqkv_ref, woa_ref)
    ex = Exchange(line, (wqkv_ref, woa_ref), es, er)
    ex.begin()
    for c in xc + sc:
        c.wait_recv()
    sca_ref[...] = jnp.concatenate([scin[m] for m in range(n_model)], axis=1)
    x = jnp.concatenate([xin[m] for m in range(n_model)], axis=1)
    x_ref[...] = x
    mine = torus.at(0, 0, 0)
    h_ref[pl.ds(pl.multiple_of(mine * rows, rows), rows), :] = norm(x.astype(jnp.float32), sca_ref[0:1]).astype(jnp.bfloat16)
    gather_blocks(torus, h_ref, hs, hr)
    ex.onward()
    ex.finish()
    for c in xc + sc:
        c.wait_send()


def attn_weight_shapes(wq, wo, n_model):
    _, rows, dim = wq.shape
    _, o_rows, o_cols = wo.shape
    return (jax.ShapeDtypeStruct((rows * n_model, 3 * dim), wq.dtype), jax.ShapeDtypeStruct((o_rows * n_model, o_cols), wo.dtype))


def start(hidden_mine, scales, wq, wk, wv, wo, cid):
    n_model, rows, width_loc = hidden_mine.shape
    width = n_model * width_loc
    peer_sems = [pltpu.SemaphoreType.DMA((n_model,))] * 4
    return pl.pallas_call(
        functools.partial(start_kernel, n_model),
        out_shape=(jax.ShapeDtypeStruct((rows, width), hidden_mine.dtype),
                   jax.ShapeDtypeStruct((rows * SIDE * SIDE, width), hidden_mine.dtype),
                   jax.ShapeDtypeStruct((scales.shape[0], width), scales.dtype)) + attn_weight_shapes(wq, wo, n_model),
        in_specs=[VMEM] * 6, out_specs=(VMEM,) * 5,
        scratch_shapes=[pltpu.VMEM(hidden_mine.shape, hidden_mine.dtype), pltpu.VMEM((n_model,) + scales.shape, scales.dtype)]
        + peer_sems + GATHER_SEMS + exchange_sems(2),
        compiler_params=params(cid), cost_estimate=cost(30_000_000_000), name='start',
    )(hidden_mine, scales, wq, wk, wv, wo)


def project_kernel(n_model, final, prefetch, a_ref, w_ref, res_ref, sa_ref, sb_ref, *rest):
    rest = list(rest)
    if prefetch:
        wq_ref, wk_ref, wv_ref, wo_ref = rest[:4]
        rest = rest[4:]
    if not final:
        x_ref = rest.pop(0)
    h_ref = rest.pop(0)
    if prefetch:
        wqkv_ref, woa_ref = rest[:2]
        rest = rest[2:]
    far, right, left, own, from_l1, from_r1, from_l, from_r, q_l1, q_r1, q_l, q_r, s1, r1, s2, r2, hs, hr = rest[:18]
    rest = rest[18:]
    torus, line = Torus(), Line(n_model)
    rows, width = res_ref.shape
    half = rows // 2
    cols = width // 2
    if final:
        meet(torus, others(line))
    elif prefetch:
        meet(torus, (line.right, line.left, line.mate))
    else:
        meet(torus, ())
    order = (2, 1, -1, 0)

    def product(q, off, dst):
        lhs = jnp.concatenate([a_ref[pl.ds(pl.multiple_of(torus.at(q, off, o) * rows, rows), rows), :] for o in order], axis=0)
        piece = w_ref.shape[2]
        per = cols // piece
        for p in range(per):
            res = jnp.dot(lhs, w_ref[q * per + p], preferred_element_type=jnp.float32)
            for n in range(SIDE):
                dst[q, n, :, p * piece:(p + 1) * piece] = res[n * rows:(n + 1) * rows]

    def ring1(q, n, k):
        src, dst, step = ((far.at[q, n, pl.ds(0, half)], from_l1.at[q, n], 1), (far.at[q, n, pl.ds(half, half)], from_r1.at[q, n], -1),
                          (right.at[q, n], from_l.at[q, n], 1), (left.at[q, n], from_r.at[q, n], -1))[k]
        return remote(src, dst, s1.at[q, n, k], r1.at[q, n, k], torus.peer(q, step))

    def ring2(q, k):
        src, dst, step = ((own.at[q, 0, pl.ds(0, half)], q_l1.at[q], 1), (own.at[q, 0, pl.ds(half, half)], q_r1.at[q], -1),
                          (own.at[q, 1], q_l.at[q], 1), (own.at[q, 2], q_r.at[q], -1))[k]
        return remote(src, dst, s2.at[q, k], r2.at[q, k], torus.peer(1 - q, step))

    for q in (0, 1):
        product(q, 2, far)
        for n in range(SIDE):
            ring1(q, n, 0).start()
            ring1(q, n, 1).start()
    if prefetch:
        load_attn_weights(line, 1, wq_ref, wk_ref, wv_ref, wo_ref, wqkv_ref, woa_ref)
        ex = Exchange(line, (wqkv_ref, woa_ref), rest[0], rest[1])
        ex.begin()
    for q in (0, 1):
        product(q, 1, right)
        product(q, -1, left)
        for n in range(SIDE):
            ring1(q, n, 0).wait_recv()
            right[q, n, 0:half] += from_l1[q, n]
            ring1(q, n, 2).start()
            ring1(q, n, 1).wait_recv()
            left[q, n, half:rows] += from_r1[q, n]
            ring1(q, n, 3).start()
    for q in (0, 1):
        product(q, 0, own)
    for n in range(SIDE):
        for q in (0, 1):
            ring1(q, n, 2).wait_recv()
            ring1(q, n, 3).wait_recv()
            own[q, n] += from_l[q, n] + from_r[q, n]
            if n == 0:
                ring2(q, 0).start()
                ring2(q, 1).start()
            if n == 1:
                ring2(q, 0).wait_recv()
                own[q, 1, 0:half] += q_l1[q]
                ring2(q, 2).start()
            if n == 2:
                ring2(q, 1).wait_recv()
                own[q, 2, half:rows] += q_r1[q]
                ring2(q, 3).start()
    if prefetch:
        ex.onward()
    total = []
    for q in (0, 1):
        ring2(q, 2).wait_recv()
        ring2(q, 3).wait_recv()
        total.append(own[q, 3] + q_l[q] + q_r[q])
    out = jnp.concatenate(total, axis=1).astype(jnp.bfloat16).astype(jnp.float32)
    x_new = (res_ref[...].astype(jnp.float32) + norm(out, sa_ref[...])).astype(jnp.bfloat16)
    here = pl.ds(pl.multiple_of(torus.at(0, 0, 0) * rows, rows), rows)
    if final:
        outgo, income, cs, cr = rest
        part = width // n_model
        for m in range(n_model):
            outgo[m] = x_new[:, m * part:(m + 1) * part]
        income[line.me] = outgo[line.me]
        copies = to_all(line, lambda step, peer: remote(outgo.at[peer], income.at[line.me], cs.at[step], cr.at[step], {'model': peer}))
        for c in copies:
            c.wait_recv()
        h_ref[here, :] = jnp.concatenate([income[m] for m in range(n_model)], axis=1)
    else:
        x_ref[...] = x_new
        h_ref[here, :] = norm(x_new.astype(jnp.float32), sb_ref[...]).astype(jnp.bfloat16)
    gather_blocks(torus, h_ref, hs, hr)
    if prefetch:
        ex.finish()
    if final:
        for c in copies:
            c.wait_send()
    for q in (0, 1):
        for k in range(4):
            ring2(q, k).wait_send()
            for n in range(SIDE):
                ring1(q, n, k).wait_send()


def project(a, w, resid, scale_a, scale_b, n_model, cid, final=False, prefetch=None):
    rows, width = resid.shape
    cols = width // 2
    half = rows // 2

    def f32(*shape):
        return pltpu.VMEM((2,) + shape + (cols,), jnp.float32)

    scratch = [f32(SIDE, rows)] * 4 + [f32(SIDE, half)] * 2 + [f32(SIDE, rows)] * 2 + [f32(half)] * 2 + [f32(rows)] * 2
    scratch += [pltpu.SemaphoreType.DMA((2, SIDE, 4))] * 2 + [pltpu.SemaphoreType.DMA((2, 4))] * 2 + GATHER_SEMS
    h_shape = jax.ShapeDtypeStruct((rows * SIDE * SIDE, width), jnp.bfloat16)
    out_shape = (h_shape,) if final else (jax.ShapeDtypeStruct((rows, width), jnp.bfloat16), h_shape)
    args = (a, w, resid, scale_a, scale_b)
    if prefetch is not None:
        args += tuple(prefetch)
        out_shape += attn_weight_shapes(prefetch[0], prefetch[3], n_model)
        scratch += exchange_sems(2)
    if final:
        part = (n_model, rows, width // n_model)
        scratch += [pltpu.VMEM(part, jnp.bfloat16)] * 2 + [pltpu.SemaphoreType.DMA((n_model,))] * 2
    return pl.pallas_call(
        functools.partial(project_kernel, n_model, final, prefetch is not None),
        out_shape=out_shape, in_specs=[VMEM] * len(args), out_specs=(VMEM,) * len(out_shape), scratch_shapes=scratch,
        compiler_params=params(cid), cost_estimate=cost(50_000_000_000), name='project_reduce',
    )(*args)


def solution(mesh):
    n_model = mesh.shape['model']
    n_heads = mesh.shape['heads']
    col_spec = P(None, 'model', 'heads')
    row_spec = P(None, 'heads', 'model')
    cache_spec = P(None, None, 'heads', None)

    def body(hidden_in, seg_ids, positions, w_query, w_key, w_value, w_out, w_gate, w_up, w_down, norm_scales, qk_scales):
        n_tok, width_loc = hidden_in.shape
        width = width_loc * n_model
        head_dim = qk_scales.shape[-1]
        tok_m = n_tok // n_model
        tok_own = tok_m // n_heads
        hd = lax.axis_index('heads')
        md = lax.axis_index('model')

        gate_w, up_w, down_w = [], [], []
        for l in range(2):
            gate_w.append(lax.all_gather(w_gate[l], 'model', axis=0, tiled=True))
            up_w.append(lax.all_gather(w_up[l], 'model', axis=0, tiled=True))
            down_w.append(lax.all_gather(w_down[l], 'model', axis=0))

        attn_shards = (w_query, w_key, w_value, w_out)
        mine = lax.dynamic_index_in_dim(hidden_in.reshape(n_model, n_heads, tok_own, width_loc), hd, 1, keepdims=False)
        resid, h, scales, wqkv, wo = start(mine, norm_scales.reshape(-1, width_loc), *attn_shards, 0)

        pos_m = lax.dynamic_slice_in_dim(positions, md * tok_m, tok_m)
        seg_m = lax.dynamic_slice_in_dim(seg_ids, md * tok_m, tok_m)

        settings = ((GLOBAL_BASE, GLOBAL_FACTOR, n_tok), (LOCAL_BASE, 1.0, WINDOW))
        keys, values = [], []
        for l in range(2):
            rope_base, pos_factor, window = settings[l]
            qkv = jnp.dot(h, wqkv, preferred_element_type=jnp.float32).astype(jnp.bfloat16)
            q, k, v = qkv[:, :head_dim], qkv[:, head_dim:2 * head_dim], qkv[:, 2 * head_dim:]
            cos_tab, sin_tab = rope_tables(pos_m, head_dim, rope_base, pos_factor)
            q = apply_rope(norm(q.astype(jnp.float32), qk_scales[l, 0]), cos_tab, sin_tab).astype(jnp.bfloat16)
            k = apply_rope(norm(k.astype(jnp.float32), qk_scales[l, 1]), cos_tab, sin_tab).astype(jnp.bfloat16)
            k_all, v_all = exchange(k, v, n_model, 1 + 3 * l)
            keys.append(k_all[:, None, :])
            values.append(v_all[:, None, :])
            o = attend(q, k_all, v_all, seg_m, pos_m, seg_ids, positions, window)
            wo = wo.reshape(n_model, head_dim, width_loc)
            row = 4 * l
            if l == 0:
                resid, h, wqkv, wo_next = project(o, wo, resid, scales[row + 1:row + 2], scales[row + 2:row + 3], n_model, 2, prefetch=attn_shards)
                wo = wo_next
            else:
                resid, h = project(o, wo, resid, scales[row + 1:row + 2], scales[row + 2:row + 3], n_model, 5)
            g = jnp.dot(h, gate_w[l], preferred_element_type=jnp.float32).astype(jnp.bfloat16)
            u = jnp.dot(h, up_w[l], preferred_element_type=jnp.float32).astype(jnp.bfloat16)
            mid = (jax.nn.gelu(g.astype(jnp.float32), approximate=True) * u.astype(jnp.float32)).astype(jnp.bfloat16)
            if l == 0:
                resid, h = project(mid, down_w[0], resid, scales[3:4], scales[4:5], n_model, 3)
            else:
                out, = project(mid, down_w[1], resid, scales[7:8], scales[7:8], n_model, 6, final=True)
        out = out.reshape(tok_m, n_model, width_loc).transpose(1, 0, 2).reshape(n_tok, width_loc)
        return out, jnp.stack(keys), jnp.stack(values)

    return jax.shard_map(body, mesh=mesh,
                         in_specs=(P(None, 'model'), P(), P(), col_spec, col_spec, col_spec, row_spec, col_spec, col_spec, row_spec, P(None, None, 'model'), P()),
                         out_specs=(P(None, 'model'), cache_spec, cache_spec),
                         check_vma=False)
```

```python
import functools

import jax
import jax.numpy as jnp
from jax import lax
from jax.experimental import pallas as pl
from jax.experimental.pallas import tpu as pltpu
from jax.sharding import PartitionSpec as P

NORM_EPS = 1e-6
WINDOW = 1024
GLOBAL_BASE = 1000000.0
GLOBAL_FACTOR = 8.0
LOCAL_BASE = 10000.0
MESH = pl.DeviceIdType.MESH
SIDE = 4
VMEM_LIMIT = 60 * 1024 * 1024


def norm(values, scale_row):
    mean_sq = jnp.mean(values * values, axis=-1, keepdims=True)
    return values * lax.rsqrt(mean_sq + NORM_EPS) * (1.0 + scale_row)


def rope_tables(positions, head_dim, rope_base, pos_factor):
    exponents = jnp.arange(0, head_dim, 2).astype(jnp.float32) / head_dim
    inv_freq = rope_base ** (-exponents)
    angles = (positions.astype(jnp.float32) / pos_factor)[:, None] * inv_freq[None, :]
    return jnp.cos(angles), jnp.sin(angles)


def apply_rope(values, cos_tab, sin_tab):
    half_dim = values.shape[-1] // 2
    first_half = values[..., :half_dim]
    second_half = values[..., half_dim:]
    return jnp.concatenate([first_half * cos_tab - second_half * sin_tab, second_half * cos_tab + first_half * sin_tab], axis=-1)


def attend(q, k, v, seg_q, pos_q, seg_ids, positions, window):
    scores = jnp.dot(q, k.T, preferred_element_type=jnp.float32) * (q.shape[-1] ** -0.5)
    gap = pos_q[:, None] - positions[None, :]
    allowed = (seg_q[:, None] == seg_ids[None, :]) & (gap >= 0) & (gap < window)
    scores = jnp.where(allowed, scores, -1e30)
    row_max = jnp.max(scores, axis=-1, keepdims=True)
    e = jnp.exp(scores - row_max)
    p = (e / jnp.sum(e, axis=-1, keepdims=True)).astype(jnp.bfloat16)
    return jnp.dot(p, v, preferred_element_type=jnp.float32).astype(jnp.bfloat16)


def wrap(i):
    return lax.rem(i + 2 * SIDE, SIDE)


def remote(src, dst, send, recv, to):
    return pltpu.make_async_remote_copy(src, dst, send, recv, device_id=to, device_id_type=MESH)


def row_block(ref, start, size, align):
    return ref.at[pl.ds(pl.multiple_of(start, align), size), :]


class Torus:
    def __init__(self):
        me = lax.axis_index('heads')
        self.own = (lax.rem(me, SIDE), me // SIDE)

    def block(self, axis, along, across):
        return across * SIDE + along if axis == 0 else along * SIDE + across

    def at(self, axis, da, db):
        return self.block(axis, wrap(self.own[axis] + da), wrap(self.own[1 - axis] + db))

    def peer(self, axis, step):
        return {'heads': self.at(axis, step, 0)}


class Line:
    def __init__(self, n_model):
        self.n = n_model
        self.me = lax.axis_index('model')
        chips = n_model // 2
        chip, core = self.me // 2, lax.rem(self.me, 2)
        self.right = lax.rem(chip + 1, chips) * 2 + core
        self.left = lax.rem(chip + chips - 1, chips) * 2 + core
        self.far = lax.rem(chip + 2, chips) * 2 + core
        self.mate = chip * 2 + 1 - core


def meet(torus, models):
    barrier = pltpu.get_barrier_semaphore()
    count = len(models)
    for other in models:
        pl.semaphore_signal(barrier, inc=1, device_id={'model': other}, device_id_type=MESH)
    if torus is not None:
        for axis in (0, 1):
            for step in (1, -1):
                pl.semaphore_signal(barrier, inc=1, device_id=torus.peer(axis, step), device_id_type=MESH)
                count += 1
    pl.semaphore_wait(barrier, count)


def gather_blocks(torus, h_ref, send, recv, between=lambda: None):
    rows = h_ref.shape[0] // (SIDE * SIDE)
    cols = h_ref.shape[1] // 2
    half = rows // 2

    def view(q, da, db, part):
        start = torus.at(q, da, db) * rows + (half if part == 2 else 0)
        return h_ref.at[pl.ds(pl.multiple_of(start, half), rows if part == 0 else half), pl.ds(q * cols, cols)]

    def ring(q, axis, base, slot, offsets):
        def make(k, da, db, part, step):
            v = view(q, da, db, part)
            return remote(v, v, send.at[q, base, k], recv.at[q, base, k], torus.peer(axis, step))
        along = (lambda off: (off, offsets)) if axis == q else (lambda off: (offsets, off))
        return (make(0, *along(0), 0, 1), make(1, *along(0), 0, -1), make(2, *along(-1), 1, 1), make(3, *along(1), 2, -1))

    first = [ring(q, 1 - q, 0, 0, 0) for q in (0, 1)]
    second = [[ring(q, q, 1 + n, 0, off) for n, off in enumerate((0, -1, 1, 2))] for q in (0, 1)]

    def begin(copies):
        copies[0].start()
        copies[1].start()

    def onward(copies):
        copies[0].wait_recv()
        copies[2].start()
        copies[1].wait_recv()
        copies[3].start()

    for q in (0, 1):
        begin(first[q])
    for q in (0, 1):
        begin(second[q][0])
    for q in (0, 1):
        first[q][0].wait_recv()
        first[q][2].start()
        begin(second[q][1])
        first[q][1].wait_recv()
        first[q][3].start()
        begin(second[q][2])
    for q in (0, 1):
        onward(second[q][0])
    for q in (0, 1):
        first[q][2].wait_recv()
        first[q][3].wait_recv()
        begin(second[q][3])
    between()
    for n in (1, 2, 3):
        for q in (0, 1):
            onward(second[q][n])
    for q in (0, 1):
        for n in range(SIDE):
            second[q][n][2].wait_recv()
            second[q][n][3].wait_recv()
    for q in (0, 1):
        for copies in [first[q]] + second[q]:
            for c in copies:
                c.wait_send()


GATHER_SEMS = [pltpu.SemaphoreType.DMA((2, 1 + SIDE, 4)), pltpu.SemaphoreType.DMA((2, 1 + SIDE, 4))]


class Exchange:
    def __init__(self, line, items, send, recv):
        self.copies = []
        plan = [(line.me, line.right, 0), (line.me, line.left, 0), (line.me, line.mate, 0), (line.left, line.right, 1),
                (line.right, line.left, 2), (line.left, line.mate, 0), (line.right, line.mate, 0),
                (line.far, line.mate, 1), (line.far, line.mate, 2)]
        for a, (ref, stride, row, rows, src) in enumerate(items):
            half = rows // 2
            group = []
            for slot, (owner, to, part) in enumerate(plan):
                first = owner * stride + (row + (half if part == 2 else 0))
                v = row_block(ref, first, rows if part == 0 else half, half)
                group.append(remote(src if src is not None and slot < 3 else v, v, send.at[a, slot], recv.at[a, slot], {'model': to}))
            self.copies.append(group)

    def begin(self):
        for c in self.copies:
            c[0].start()
            c[1].start()
            c[2].start()

    def onward(self, lo=0, hi=None):
        for c in self.copies[lo:hi]:
            c[0].wait_recv()
            c[3].start()
            c[1].wait_recv()
            c[4].start()
            c[5].start()
            c[6].start()

    def finish(self):
        for c in self.copies:
            c[3].wait_recv()
            c[7].start()
            c[4].wait_recv()
            c[8].start()
        for c in self.copies:
            for slot in (2, 5, 6, 7, 8):
                c[slot].wait_recv()
            for one in c:
                one.wait_send()


def exchange_sems(count):
    return [pltpu.SemaphoreType.DMA((count, 9)), pltpu.SemaphoreType.DMA((count, 9))]


def exchange_kernel(n_model, k_ref, v_ref, ka_ref, va_ref, send, recv):
    line = Line(n_model)
    rows = k_ref.shape[0]
    meet(None, (line.right, line.left, line.mate))
    here = pl.ds(pl.multiple_of(line.me * rows, rows), rows)
    ka_ref[here, :] = k_ref[...]
    va_ref[here, :] = v_ref[...]
    ex = Exchange(line, [(ka_ref, rows, 0, rows, None), (va_ref, rows, 0, rows, None)], send, recv)
    ex.begin()
    ex.onward()
    ex.finish()


VMEM = pl.BlockSpec(memory_space=pltpu.VMEM)
ANY = pl.BlockSpec(memory_space=pl.ANY)
PIECES = 4


def params(cid):
    return pltpu.CompilerParams(collective_id=cid, has_side_effects=True, vmem_limit_bytes=VMEM_LIMIT)


def cost(flops):
    return pl.CostEstimate(flops=flops, bytes_accessed=10_000_000, transcendentals=0)


def exchange(k, v, n_model, cid):
    rows, dim = k.shape
    full = jax.ShapeDtypeStruct((rows * n_model, dim), k.dtype)
    return pl.pallas_call(
        functools.partial(exchange_kernel, n_model),
        out_shape=(full, full), in_specs=[VMEM] * 2, out_specs=(VMEM, VMEM),
        scratch_shapes=exchange_sems(2), compiler_params=params(cid), cost_estimate=cost(20_000_000_000), name='exchange_kv',
    )(k, v)


def load_attn_weights(line, layer, wq_ref, wk_ref, wv_ref, wo_ref, wqkv_ref, woa_ref):
    rows, dim = wq_ref.shape[1:]
    here = pl.ds(pl.multiple_of(line.me * rows, rows), rows)
    for at, ref in enumerate((wq_ref, wk_ref, wv_ref)):
        wqkv_ref[here, at * dim:(at + 1) * dim] = ref[layer]
    o_rows = wo_ref.shape[1]
    woa_ref[pl.ds(pl.multiple_of(line.me * o_rows, o_rows), o_rows), :] = wo_ref[layer]
    return [(wqkv_ref, rows, 0, rows, None), (woa_ref, o_rows, 0, o_rows, None)]


def to_all(line, make):
    copies = []
    for step in range(1, line.n):
        peer = lax.rem(line.me + step, line.n)
        copies.append(make(step, peer))
    for c in copies:
        c.start()
    return copies


def others(line):
    return [lax.rem(line.me + step, line.n) for step in range(1, line.n)]


def start_kernel(n_model, hid_ref, sc_ref, wq_ref, wk_ref, wv_ref, wo_ref, wg_ref, wu_ref,
                 x_ref, h_ref, sca_ref, wqkv_ref, woa_ref, g0_ref, u0_ref, g1_ref, u1_ref,
                 xin, scin, stage, xs, xr, ss, sr, ls, hs, hr, es, er):
    torus, line = Torus(), Line(n_model)
    rows = x_ref.shape[0]
    shards = ((wg_ref, 0, g0_ref), (wu_ref, 0, u0_ref), (wg_ref, 1, g1_ref), (wu_ref, 1, u1_ref))
    loads = [pltpu.make_async_copy(ref.at[layer], stage.at[k], ls.at[k]) for k, (ref, layer, _) in enumerate(shards)]
    stores = [pltpu.make_async_copy(stage.at[k], dst, ls.at[k]) for k, (_, _, dst) in enumerate(shards)]
    for c in loads:
        c.start()
    meet(torus, others(line))
    xin[line.me] = hid_ref[line.me]
    scin[line.me] = sc_ref[...]
    xc = to_all(line, lambda step, peer: remote(hid_ref.at[peer], xin.at[line.me], xs.at[step], xr.at[step], {'model': peer}))
    sc = to_all(line, lambda step, peer: remote(sc_ref, scin.at[line.me], ss.at[step], sr.at[step], {'model': peer}))
    ex = Exchange(line, load_attn_weights(line, 0, wq_ref, wk_ref, wv_ref, wo_ref, wqkv_ref, woa_ref), es, er)
    ex.begin()
    for load, store in zip(loads, stores):
        load.wait()
        store.start()
    for c in xc + sc:
        c.wait_recv()
    sca_ref[...] = jnp.concatenate([scin[m] for m in range(n_model)], axis=1)
    x = jnp.concatenate([xin[m] for m in range(n_model)], axis=1)
    x_ref[...] = x
    mine = torus.at(0, 0, 0)
    h_ref[pl.ds(pl.multiple_of(mine * rows, rows), rows), :] = norm(x.astype(jnp.float32), sca_ref[0:1]).astype(jnp.bfloat16)
    gather_blocks(torus, h_ref, hs, hr, ex.onward)
    ex.finish()
    for c in stores:
        c.wait()
    for c in xc + sc:
        c.wait_send()


def attn_weight_shapes(wq, wo, n_model):
    _, rows, dim = wq.shape
    _, o_rows, o_cols = wo.shape
    return (jax.ShapeDtypeStruct((rows * n_model, 3 * dim), wq.dtype), jax.ShapeDtypeStruct((o_rows * n_model, o_cols), wo.dtype))


def start(hidden_mine, scales, wq, wk, wv, wo, wg, wu, cid):
    n_model, rows, width_loc = hidden_mine.shape
    width = n_model * width_loc
    peer_sems = [pltpu.SemaphoreType.DMA((n_model,))] * 4
    return pl.pallas_call(
        functools.partial(start_kernel, n_model),
        out_shape=(jax.ShapeDtypeStruct((rows, width), hidden_mine.dtype),
                   jax.ShapeDtypeStruct((rows * SIDE * SIDE, width), hidden_mine.dtype),
                   jax.ShapeDtypeStruct((scales.shape[0], width), scales.dtype)) + attn_weight_shapes(wq, wo, n_model)
        + (jax.ShapeDtypeStruct(wg.shape[1:], wg.dtype),) * 4,
        in_specs=[VMEM] * 6 + [ANY] * 2, out_specs=(VMEM,) * 5 + (ANY,) * 4,
        scratch_shapes=[pltpu.VMEM(hidden_mine.shape, hidden_mine.dtype), pltpu.VMEM((n_model,) + scales.shape, scales.dtype),
                        pltpu.VMEM((4,) + wg.shape[1:], wg.dtype)]
        + peer_sems + [pltpu.SemaphoreType.DMA((4,))] + GATHER_SEMS + exchange_sems(2),
        compiler_params=params(cid), cost_estimate=cost(30_000_000_000), name='start',
    )(hidden_mine, scales, wq, wk, wv, wo, wg, wu)


def project_kernel(n_model, final, attn, down, a_ref, w_ref, res_ref, sa_ref, sb_ref, *rest):
    rest = list(rest)
    fetch = attn or down is not None
    if attn:
        wq_ref, wk_ref, wv_ref, wo_ref = rest[:4]
        rest = rest[4:]
    if down is not None:
        wd_ref = rest.pop(0)
    if not final:
        x_ref = rest.pop(0)
    h_ref = rest.pop(0)
    if attn:
        wqkv_ref, woa_ref = rest[:2]
        rest = rest[2:]
    if down is not None:
        wda_ref = rest.pop(0)
    far, right, left, own, from_l1, from_r1, from_l, from_r, q_l1, q_r1, q_l, q_r, s1, r1, s2, r2, hs, hr = rest[:18]
    rest = rest[18:]
    torus, line = Torus(), Line(n_model)
    rows, width = res_ref.shape
    half = rows // 2
    cols = width // 2
    if final:
        meet(torus, others(line))
    elif fetch:
        meet(torus, (line.right, line.left, line.mate))
    else:
        meet(torus, ())
    order = (2, 1, -1, 0)

    def product(q, off, dst):
        lhs = jnp.concatenate([a_ref[pl.ds(pl.multiple_of(torus.at(q, off, o) * rows, rows), rows), :] for o in order], axis=0)
        piece = w_ref.shape[2]
        per = cols // piece
        for p in range(per):
            res = jnp.dot(lhs, w_ref[q * per + p], preferred_element_type=jnp.float32)
            for n in range(SIDE):
                dst[q, n, :, p * piece:(p + 1) * piece] = res[n * rows:(n + 1) * rows]

    def ring1(q, n, k):
        src, dst, step = ((far.at[q, n, pl.ds(0, half)], from_l1.at[q, n], 1), (far.at[q, n, pl.ds(half, half)], from_r1.at[q, n], -1),
                          (right.at[q, n], from_l.at[q, n], 1), (left.at[q, n], from_r.at[q, n], -1))[k]
        return remote(src, dst, s1.at[q, n, k], r1.at[q, n, k], torus.peer(q, step))

    def ring2(q, k):
        src, dst, step = ((own.at[q, 0, pl.ds(0, half)], q_l1.at[q], 1), (own.at[q, 0, pl.ds(half, half)], q_r1.at[q], -1),
                          (own.at[q, 1], q_l.at[q], 1), (own.at[q, 2], q_r.at[q], -1))[k]
        return remote(src, dst, s2.at[q, k], r2.at[q, k], torus.peer(1 - q, step))

    if down is not None:
        mine, ls = rest[2:]
        load = pltpu.make_async_copy(wd_ref.at[down], mine, ls.at[0])
        load.start()
    for q in (0, 1):
        product(q, 2, far)
        for n in range(SIDE):
            ring1(q, n, 0).start()
            ring1(q, n, 1).start()
    if attn:
        ex = Exchange(line, load_attn_weights(line, 1, wq_ref, wk_ref, wv_ref, wo_ref, wqkv_ref, woa_ref), rest[0], rest[1])
        ex.begin()
    if down is not None:
        load.wait()
        stride = mine.shape[0]
        piece = stride // PIECES
        keep = pltpu.make_async_copy(mine, row_block(wda_ref, line.me * stride, stride, stride), ls.at[0])
        keep.start()
        ex = Exchange(line, [(wda_ref, stride, k * piece, piece, mine.at[pl.ds(k * piece, piece)]) for k in range(PIECES)], rest[0], rest[1])
        ex.begin()
    for q in (0, 1):
        product(q, 1, right)
        product(q, -1, left)
        for n in range(SIDE):
            ring1(q, n, 0).wait_recv()
            right[q, n, 0:half] += from_l1[q, n]
            ring1(q, n, 2).start()
            ring1(q, n, 1).wait_recv()
            left[q, n, half:rows] += from_r1[q, n]
            ring1(q, n, 3).start()
    for q in (0, 1):
        product(q, 0, own)
    if down is not None:
        ex.onward(0, 2)
    for n in range(SIDE):
        for q in (0, 1):
            ring1(q, n, 2).wait_recv()
            ring1(q, n, 3).wait_recv()
            own[q, n] += from_l[q, n] + from_r[q, n]
            if n == 0:
                ring2(q, 0).start()
                ring2(q, 1).start()
            if n == 1:
                ring2(q, 0).wait_recv()
                own[q, 1, 0:half] += q_l1[q]
                ring2(q, 2).start()
            if n == 2:
                ring2(q, 1).wait_recv()
                own[q, 2, half:rows] += q_r1[q]
                ring2(q, 3).start()
    total = []
    for q in (0, 1):
        ring2(q, 2).wait_recv()
        ring2(q, 3).wait_recv()
        total.append(own[q, 3] + q_l[q] + q_r[q])
    out = jnp.concatenate(total, axis=1).astype(jnp.bfloat16).astype(jnp.float32)
    x_new = (res_ref[...].astype(jnp.float32) + norm(out, sa_ref[...])).astype(jnp.bfloat16)
    here = pl.ds(pl.multiple_of(torus.at(0, 0, 0) * rows, rows), rows)
    if final:
        outgo, income, cs, cr = rest
        part = width // n_model
        for m in range(n_model):
            outgo[m] = x_new[:, m * part:(m + 1) * part]
        income[line.me] = outgo[line.me]
        copies = to_all(line, lambda step, peer: remote(outgo.at[peer], income.at[line.me], cs.at[step], cr.at[step], {'model': peer}))
        for c in copies:
            c.wait_recv()
        h_ref[here, :] = jnp.concatenate([income[m] for m in range(n_model)], axis=1)
    else:
        x_ref[...] = x_new
        h_ref[here, :] = norm(x_new.astype(jnp.float32), sb_ref[...]).astype(jnp.bfloat16)
    if attn:
        gather_blocks(torus, h_ref, hs, hr, ex.onward)
        ex.finish()
    elif down is not None:
        gather_blocks(torus, h_ref, hs, hr, lambda: ex.onward(2))
        ex.finish()
        keep.wait()
    else:
        gather_blocks(torus, h_ref, hs, hr)
    if final:
        for c in copies:
            c.wait_send()
    for q in (0, 1):
        for k in range(4):
            ring2(q, k).wait_send()
            for n in range(SIDE):
                ring1(q, n, k).wait_send()


def project(a, w, resid, scale_a, scale_b, n_model, cid, final=False, attn=None, down=None, layer=None):
    rows, width = resid.shape
    cols = width // 2
    half = rows // 2

    def f32(*shape):
        return pltpu.VMEM((2,) + shape + (cols,), jnp.float32)

    scratch = [f32(SIDE, rows)] * 4 + [f32(SIDE, half)] * 2 + [f32(SIDE, rows)] * 2 + [f32(half)] * 2 + [f32(rows)] * 2
    scratch += [pltpu.SemaphoreType.DMA((2, SIDE, 4))] * 2 + [pltpu.SemaphoreType.DMA((2, 4))] * 2 + GATHER_SEMS
    h_shape = jax.ShapeDtypeStruct((rows * SIDE * SIDE, width), jnp.bfloat16)
    out_shape = (h_shape,) if final else (jax.ShapeDtypeStruct((rows, width), jnp.bfloat16), h_shape)
    args = (a, w, resid, scale_a, scale_b)
    in_specs, out_specs = [VMEM] * 5, (VMEM,) * len(out_shape)
    if attn is not None:
        args += tuple(attn)
        in_specs += [VMEM] * 4
        out_shape += attn_weight_shapes(attn[0], attn[3], n_model)
        out_specs += (VMEM,) * 2
        scratch += exchange_sems(2)
    if down is not None:
        args += (down,)
        in_specs += [ANY]
        _, d_rows, d_cols = down.shape
        out_shape += (jax.ShapeDtypeStruct((d_rows * n_model, d_cols), down.dtype),)
        out_specs += (ANY,)
        scratch += exchange_sems(PIECES) + [pltpu.VMEM((d_rows, d_cols), down.dtype), pltpu.SemaphoreType.DMA((1,))]
    if final:
        part = (n_model, rows, width // n_model)
        scratch += [pltpu.VMEM(part, jnp.bfloat16)] * 2 + [pltpu.SemaphoreType.DMA((n_model,))] * 2
    return pl.pallas_call(
        functools.partial(project_kernel, n_model, final, attn is not None, layer),
        out_shape=out_shape, in_specs=in_specs, out_specs=out_specs, scratch_shapes=scratch,
        compiler_params=params(cid), cost_estimate=cost(50_000_000_000), name='project_reduce',
    )(*args)


def solution(mesh):
    n_model = mesh.shape['model']
    n_heads = mesh.shape['heads']
    col_spec = P(None, 'model', 'heads')
    row_spec = P(None, 'heads', 'model')
    cache_spec = P(None, None, 'heads', None)

    def body(hidden_in, seg_ids, positions, w_query, w_key, w_value, w_out, w_gate, w_up, w_down, norm_scales, qk_scales):
        n_tok, width_loc = hidden_in.shape
        width = width_loc * n_model
        head_dim = qk_scales.shape[-1]
        tok_m = n_tok // n_model
        tok_own = tok_m // n_heads
        hd = lax.axis_index('heads')
        md = lax.axis_index('model')

        attn_shards = (w_query, w_key, w_value, w_out)
        mine = lax.dynamic_index_in_dim(hidden_in.reshape(n_model, n_heads, tok_own, width_loc), hd, 1, keepdims=False)
        resid, h, scales, wqkv, wo, *shards = start(mine, norm_scales.reshape(-1, width_loc), *attn_shards, w_gate, w_up, 0)
        wide = [lax.all_gather(w, 'model', axis=0, tiled=True) for w in shards]

        pos_m = lax.dynamic_slice_in_dim(positions, md * tok_m, tok_m)
        seg_m = lax.dynamic_slice_in_dim(seg_ids, md * tok_m, tok_m)

        settings = ((GLOBAL_BASE, GLOBAL_FACTOR, n_tok), (LOCAL_BASE, 1.0, WINDOW))
        keys, values = [], []
        for l in range(2):
            rope_base, pos_factor, window = settings[l]
            qkv = jnp.dot(h, wqkv, preferred_element_type=jnp.float32).astype(jnp.bfloat16)
            q, k, v = qkv[:, :head_dim], qkv[:, head_dim:2 * head_dim], qkv[:, 2 * head_dim:]
            cos_tab, sin_tab = rope_tables(pos_m, head_dim, rope_base, pos_factor)
            q = apply_rope(norm(q.astype(jnp.float32), qk_scales[l, 0]), cos_tab, sin_tab).astype(jnp.bfloat16)
            k = apply_rope(norm(k.astype(jnp.float32), qk_scales[l, 1]), cos_tab, sin_tab).astype(jnp.bfloat16)
            k_all, v_all = exchange(k, v, n_model, 1 + 3 * l)
            keys.append(k_all[:, None, :])
            values.append(v_all[:, None, :])
            o = attend(q, k_all, v_all, seg_m, pos_m, seg_ids, positions, window)
            wo = wo.reshape(n_model, head_dim, width_loc)
            row = 4 * l
            resid, h, wd = project(o, wo, resid, scales[row + 1:row + 2], scales[row + 2:row + 3], n_model, 2 + 3 * l, down=w_down, layer=l)
            wd = wd.reshape(n_model, w_down.shape[1], width_loc)
            g = jnp.dot(h, wide[2 * l], preferred_element_type=jnp.float32).astype(jnp.bfloat16)
            u = jnp.dot(h, wide[2 * l + 1], preferred_element_type=jnp.float32).astype(jnp.bfloat16)
            mid = (jax.nn.gelu(g.astype(jnp.float32), approximate=True) * u.astype(jnp.float32)).astype(jnp.bfloat16)
            if l == 0:
                resid, h, wqkv, wo = project(mid, wd, resid, scales[3:4], scales[4:5], n_model, 3, attn=attn_shards)
            else:
                out, = project(mid, wd, resid, scales[7:8], scales[7:8], n_model, 6, final=True)
        out = out.reshape(tok_m, n_model, width_loc).transpose(1, 0, 2).reshape(n_tok, width_loc)
        return out, jnp.stack(keys), jnp.stack(values)

    return jax.shard_map(body, mesh=mesh,
                         in_specs=(P(None, 'model'), P(), P(), col_spec, col_spec, col_spec, row_spec, col_spec, col_spec, row_spec, P(None, None, 'model'), P()),
                         out_specs=(P(None, 'model'), cache_spec, cache_spec),
                         check_vma=False)
```

```python
import functools

import jax
import jax.numpy as jnp
from jax import lax
from jax.experimental import pallas as pl
from jax.experimental.pallas import tpu as pltpu
from jax.sharding import PartitionSpec as P

NORM_EPS = 1e-6
WINDOW = 1024
GLOBAL_BASE = 1000000.0
GLOBAL_FACTOR = 8.0
LOCAL_BASE = 10000.0
MESH = pl.DeviceIdType.MESH
SIDE = 4
VMEM_LIMIT = 63 * 1024 * 1024


def norm(values, scale_row):
    mean_sq = jnp.mean(values * values, axis=-1, keepdims=True)
    return values * lax.rsqrt(mean_sq + NORM_EPS) * (1.0 + scale_row)


def rope_tables(positions, head_dim, rope_base, pos_factor):
    exponents = jnp.arange(0, head_dim, 2).astype(jnp.float32) / head_dim
    inv_freq = rope_base ** (-exponents)
    angles = (positions.astype(jnp.float32) / pos_factor)[:, None] * inv_freq[None, :]
    return jnp.cos(angles), jnp.sin(angles)


def apply_rope(values, cos_tab, sin_tab):
    half_dim = values.shape[-1] // 2
    first_half = values[..., :half_dim]
    second_half = values[..., half_dim:]
    return jnp.concatenate([first_half * cos_tab - second_half * sin_tab, second_half * cos_tab + first_half * sin_tab], axis=-1)


def attend(q, k, v, seg_q, pos_q, seg_ids, positions, window):
    scores = jnp.dot(q, k.T, preferred_element_type=jnp.float32) * (q.shape[-1] ** -0.5)
    gap = pos_q[:, None] - positions[None, :]
    allowed = (seg_q[:, None] == seg_ids[None, :]) & (gap >= 0) & (gap < window)
    scores = jnp.where(allowed, scores, -1e30)
    row_max = jnp.max(scores, axis=-1, keepdims=True)
    e = jnp.exp(scores - row_max)
    p = (e / jnp.sum(e, axis=-1, keepdims=True)).astype(jnp.bfloat16)
    return jnp.dot(p, v, preferred_element_type=jnp.float32).astype(jnp.bfloat16)


def wrap(i):
    return lax.rem(i + 2 * SIDE, SIDE)


def remote(src, dst, send, recv, to):
    return pltpu.make_async_remote_copy(src, dst, send, recv, device_id=to, device_id_type=MESH)


def row_block(ref, start, size, align):
    return ref.at[pl.ds(pl.multiple_of(start, align), size), :]


class Torus:
    def __init__(self):
        me = lax.axis_index('heads')
        self.own = (lax.rem(me, SIDE), me // SIDE)

    def block(self, axis, along, across):
        return across * SIDE + along if axis == 0 else along * SIDE + across

    def at(self, axis, da, db):
        return self.block(axis, wrap(self.own[axis] + da), wrap(self.own[1 - axis] + db))

    def peer(self, axis, step):
        return {'heads': self.at(axis, step, 0)}


class Line:
    def __init__(self, n_model):
        self.n = n_model
        self.me = lax.axis_index('model')
        chips = n_model // 2
        chip, core = self.me // 2, lax.rem(self.me, 2)
        self.right = lax.rem(chip + 1, chips) * 2 + core
        self.left = lax.rem(chip + chips - 1, chips) * 2 + core
        self.far = lax.rem(chip + 2, chips) * 2 + core
        self.mate = chip * 2 + 1 - core


def meet(torus, models):
    barrier = pltpu.get_barrier_semaphore()
    count = len(models)
    for other in models:
        pl.semaphore_signal(barrier, inc=1, device_id={'model': other}, device_id_type=MESH)
    if torus is not None:
        for axis in (0, 1):
            for step in (1, -1):
                pl.semaphore_signal(barrier, inc=1, device_id=torus.peer(axis, step), device_id_type=MESH)
                count += 1
    pl.semaphore_wait(barrier, count)


def gather_blocks(torus, h_ref, send, recv, between=lambda: None):
    rows = h_ref.shape[0] // (SIDE * SIDE)
    cols = h_ref.shape[1] // 2
    half = rows // 2

    def view(q, da, db, part):
        start = torus.at(q, da, db) * rows + (half if part == 2 else 0)
        return h_ref.at[pl.ds(pl.multiple_of(start, half), rows if part == 0 else half), pl.ds(q * cols, cols)]

    def ring(q, axis, base, offsets):
        def make(k, da, db, part, step):
            v = view(q, da, db, part)
            return remote(v, v, send.at[q, base, k], recv.at[q, base, k], torus.peer(axis, step))

        along = (lambda off: (off, offsets)) if axis == q else (lambda off: (offsets, off))
        return (make(0, *along(0), 0, 1), make(1, *along(0), 0, -1), make(2, *along(-1), 1, 1), make(3, *along(1), 2, -1))

    first = [ring(q, 1 - q, 0, 0) for q in (0, 1)]
    second = [[ring(q, q, 1 + n, off) for n, off in enumerate((0, -1, 1, 2))] for q in (0, 1)]

    def begin(copies):
        copies[0].start()
        copies[1].start()

    def onward(copies):
        copies[0].wait_recv()
        copies[2].start()
        copies[1].wait_recv()
        copies[3].start()

    for q in (0, 1):
        begin(first[q])
    for q in (0, 1):
        begin(second[q][0])
    for q in (0, 1):
        first[q][0].wait_recv()
        first[q][2].start()
        begin(second[q][1])
        first[q][1].wait_recv()
        first[q][3].start()
        begin(second[q][2])
    for q in (0, 1):
        onward(second[q][0])
    for q in (0, 1):
        first[q][2].wait_recv()
        first[q][3].wait_recv()
        begin(second[q][3])
    between()
    for n in (1, 2, 3):
        for q in (0, 1):
            onward(second[q][n])
    for q in (0, 1):
        for n in range(SIDE):
            second[q][n][2].wait_recv()
            second[q][n][3].wait_recv()
    for q in (0, 1):
        for copies in [first[q]] + second[q]:
            for c in copies:
                c.wait_send()


GATHER_SEMS = [pltpu.SemaphoreType.DMA((2, 1 + SIDE, 4)), pltpu.SemaphoreType.DMA((2, 1 + SIDE, 4))]


class Exchange:
    def __init__(self, line, items, send, recv):
        self.copies = []
        plan = [(line.me, line.right, 0), (line.me, line.left, 0), (line.me, line.mate, 0), (line.left, line.right, 1),
                (line.right, line.left, 2), (line.left, line.mate, 0), (line.right, line.mate, 0),
                (line.far, line.mate, 1), (line.far, line.mate, 2)]
        for a, (ref, stride, row, rows, src) in enumerate(items):
            half = rows // 2
            group = []
            for slot, (owner, to, part) in enumerate(plan):
                first = owner * stride + (row + (half if part == 2 else 0))
                v = row_block(ref, first, rows if part == 0 else half, half)
                group.append(remote(src if src is not None and slot < 3 else v, v, send.at[a, slot], recv.at[a, slot], {'model': to}))
            self.copies.append(group)

    def begin(self):
        for c in self.copies:
            c[0].start()
            c[1].start()
            c[2].start()

    def onward(self, lo=0, hi=None):
        for c in self.copies[lo:hi]:
            c[0].wait_recv()
            c[3].start()
            c[1].wait_recv()
            c[4].start()
            c[5].start()
            c[6].start()

    def finish(self):
        for c in self.copies:
            c[3].wait_recv()
            c[7].start()
            c[4].wait_recv()
            c[8].start()
        for c in self.copies:
            for slot in (2, 5, 6, 7, 8):
                c[slot].wait_recv()
            for one in c:
                one.wait_send()


def exchange_sems(count):
    return [pltpu.SemaphoreType.DMA((count, 9)), pltpu.SemaphoreType.DMA((count, 9))]


def exchange_kernel(n_model, k_ref, v_ref, ka_ref, va_ref, send, recv):
    line = Line(n_model)
    rows = k_ref.shape[0]
    meet(None, (line.right, line.left, line.mate))
    here = pl.ds(pl.multiple_of(line.me * rows, rows), rows)
    ka_ref[here, :] = k_ref[...]
    va_ref[here, :] = v_ref[...]
    ex = Exchange(line, [(ka_ref, rows, 0, rows, None), (va_ref, rows, 0, rows, None)], send, recv)
    ex.begin()
    ex.onward()
    ex.finish()


VMEM = pl.BlockSpec(memory_space=pltpu.VMEM)
ANY = pl.BlockSpec(memory_space=pl.ANY)
PIECES = 4
WIDE = 3
NEED = ((2, 2), (2, 1), (2, -1), (2, 0), (1, 2), (-1, 2), (0, 2), (1, 1),
        (1, -1), (1, 0), (-1, 1), (-1, -1), (-1, 0), (0, 1), (0, -1), (0, 0))


def params(cid):
    return pltpu.CompilerParams(collective_id=cid, has_side_effects=True, vmem_limit_bytes=VMEM_LIMIT)


def cost(flops):
    return pl.CostEstimate(flops=flops, bytes_accessed=10_000_000, transcendentals=0)


def exchange(k, v, n_model, cid):
    rows, dim = k.shape
    full = jax.ShapeDtypeStruct((rows * n_model, dim), k.dtype)
    return pl.pallas_call(
        functools.partial(exchange_kernel, n_model),
        out_shape=(full, full), in_specs=[VMEM] * 2, out_specs=(VMEM, VMEM),
        scratch_shapes=exchange_sems(2), compiler_params=params(cid), cost_estimate=cost(100_000_000), name='exchange_kv',
    )(k, v)


def load_attn_weights(line, layer, wq_ref, wk_ref, wv_ref, wo_ref, wqkv_ref, woa_ref):
    rows, dim = wq_ref.shape[1:]
    here = pl.ds(pl.multiple_of(line.me * rows, rows), rows)
    for at, ref in enumerate((wq_ref, wk_ref, wv_ref)):
        wqkv_ref[here, at * dim:(at + 1) * dim] = ref[layer]
    o_rows = wo_ref.shape[1]
    woa_ref[pl.ds(pl.multiple_of(line.me * o_rows, o_rows), o_rows), :] = wo_ref[layer]
    return [(wqkv_ref, rows, 0, rows, None), (woa_ref, o_rows, 0, o_rows, None)]


def to_all(line, make):
    copies = []
    for step in range(1, line.n):
        peer = lax.rem(line.me + step, line.n)
        copies.append(make(step, peer))
    for c in copies:
        c.start()
    return copies


def others(line):
    return [lax.rem(line.me + step, line.n) for step in range(1, line.n)]


def start_kernel(n_model, hid_ref, sc_ref, wq_ref, wk_ref, wv_ref, wo_ref, wg_ref, wu_ref,
                 x_ref, h_ref, sca_ref, wqkv_ref, woa_ref, u0_ref, g1_ref, u1_ref,
                 xin, scin, stage, xs, xr, ss, sr, ls, hs, hr, es, er):
    torus, line = Torus(), Line(n_model)
    rows = x_ref.shape[0]
    shards = ((wu_ref, 0, u0_ref), (wg_ref, 1, g1_ref), (wu_ref, 1, u1_ref))
    loads = [pltpu.make_async_copy(ref.at[layer], stage.at[k], ls.at[k]) for k, (ref, layer, _) in enumerate(shards)]
    stores = [pltpu.make_async_copy(stage.at[k], dst, ls.at[k]) for k, (_, _, dst) in enumerate(shards)]
    for c in loads:
        c.start()
    meet(torus, others(line))
    xin[line.me] = hid_ref[line.me]
    scin[line.me] = sc_ref[...]
    xc = to_all(line, lambda step, peer: remote(hid_ref.at[peer], xin.at[line.me], xs.at[step], xr.at[step], {'model': peer}))
    sc = to_all(line, lambda step, peer: remote(sc_ref, scin.at[line.me], ss.at[step], sr.at[step], {'model': peer}))
    ex = Exchange(line, load_attn_weights(line, 0, wq_ref, wk_ref, wv_ref, wo_ref, wqkv_ref, woa_ref), es, er)
    ex.begin()
    for load, store in zip(loads, stores):
        load.wait()
        store.start()
    for c in xc + sc:
        c.wait_recv()
    sca_ref[...] = jnp.concatenate([scin[m] for m in range(n_model)], axis=1)
    x = jnp.concatenate([xin[m] for m in range(n_model)], axis=1)
    x_ref[...] = x
    mine = torus.at(0, 0, 0)
    h_ref[pl.ds(pl.multiple_of(mine * rows, rows), rows), :] = norm(x.astype(jnp.float32), sca_ref[0:1]).astype(jnp.bfloat16)
    gather_blocks(torus, h_ref, hs, hr, ex.onward)
    ex.finish()
    for c in stores:
        c.wait()
    for c in xc + sc:
        c.wait_send()


def attn_weight_shapes(wq, wo, n_model):
    _, rows, dim = wq.shape
    _, o_rows, o_cols = wo.shape
    return (jax.ShapeDtypeStruct((rows * n_model, 3 * dim), wq.dtype), jax.ShapeDtypeStruct((o_rows * n_model, o_cols), wo.dtype))


def start(hidden_mine, scales, wq, wk, wv, wo, wg, wu, cid):
    n_model, rows, width_loc = hidden_mine.shape
    width = n_model * width_loc
    peer_sems = [pltpu.SemaphoreType.DMA((n_model,))] * 4
    return pl.pallas_call(
        functools.partial(start_kernel, n_model),
        out_shape=(jax.ShapeDtypeStruct((rows, width), hidden_mine.dtype),
                   jax.ShapeDtypeStruct((rows * SIDE * SIDE, width), hidden_mine.dtype),
                   jax.ShapeDtypeStruct((scales.shape[0], width), scales.dtype)) + attn_weight_shapes(wq, wo, n_model)
        + (jax.ShapeDtypeStruct(wg.shape[1:], wg.dtype),) * 3,
        in_specs=[VMEM] * 6 + [ANY] * 2, out_specs=(VMEM,) * 5 + (ANY,) * 3,
        scratch_shapes=[pltpu.VMEM(hidden_mine.shape, hidden_mine.dtype), pltpu.VMEM((n_model,) + scales.shape, scales.dtype),
                        pltpu.VMEM((3,) + wg.shape[1:], wg.dtype)]
        + peer_sems + [pltpu.SemaphoreType.DMA((3,))] + GATHER_SEMS + exchange_sems(2),
        compiler_params=params(cid), cost_estimate=cost(100_000_000), name='start',
    )(hidden_mine, scales, wq, wk, wv, wo, wg, wu)


def project_kernel(n_model, ffn, final, attn, down, a_ref, w_ref, res_ref, sa_ref, sb_ref, *rest):
    rest = list(rest)
    if ffn:
        wg_any, wu_any = rest[:2]
        rest = rest[2:]
    fetch = attn or down is not None
    if attn:
        wq_ref, wk_ref, wv_ref, wo_ref = rest[:4]
        rest = rest[4:]
    if down is not None:
        wd_ref = rest.pop(0)
    if not final:
        x_ref = rest.pop(0)
    h_ref = rest.pop(0)
    if attn:
        wqkv_ref, woa_ref = rest[:2]
        rest = rest[2:]
    if down is not None:
        wda_ref = rest.pop(0)
    far, right, left, own, from_l1, from_r1, from_l, from_r, q_l1, q_r1, q_l, q_r, s1, r1, s2, r2, hs, hr = rest[:18]
    rest = rest[18:]
    if ffn:
        hp, mid, wg_ref, wu_ref, wd_ref2, fs = rest[:6]
        rest = rest[6:]
    torus, line = Torus(), Line(n_model)
    rows, width = res_ref.shape
    half = rows // 2
    cols = width // 2
    if ffn:
        span = wg_any.shape[1] // WIDE

        def wide_load(k, n):
            src, dst = ((wg_any, wg_ref), (wu_any, wu_ref))[k]
            at = pl.ds(pl.multiple_of(n * span, span), span)
            return pltpu.make_async_copy(src.at[:, at], dst.at[:, at], fs.at[k, n])

        for n in range(WIDE):
            wide_load(0, n).start()
            wide_load(1, n).start()
        down_load = pltpu.make_async_copy(w_ref, wd_ref2, fs.at[2, 0])
        down_load.start()
        w_ref = wd_ref2
    if final:
        meet(torus, others(line))
    elif fetch:
        meet(torus, (line.right, line.left, line.mate))
    else:
        meet(torus, ())
    order = (2, 1, -1, 0)

    def feed(group):
        these = slice(group * SIDE * rows, (group + 1) * SIDE * rows)

        def step(n, carry):
            if group == 0:
                wide_load(0, n).wait()
                wide_load(1, n).wait()
            at = pl.ds(pl.multiple_of(n * span, span), span)
            lhs = hp[these, :]
            g = jnp.dot(lhs, wg_ref[:, at], preferred_element_type=jnp.float32).astype(jnp.bfloat16)
            u = jnp.dot(lhs, wu_ref[:, at], preferred_element_type=jnp.float32).astype(jnp.bfloat16)
            act = jax.nn.gelu(g.astype(jnp.float32), approximate=True)
            mid[these, at] = (act * u.astype(jnp.float32)).astype(jnp.bfloat16)
            return carry

        lax.fori_loop(0, WIDE, step, 0)

    def operand(q, off, o):
        if ffn:
            at = NEED.index((off, o) if q == 0 else (o, off)) * rows
            return mid[at:at + rows, :]
        return a_ref[pl.ds(pl.multiple_of(torus.at(q, off, o) * rows, rows), rows), :]

    def product(q, off, dst):
        lhs = jnp.concatenate([operand(q, off, o) for o in order], axis=0)
        piece = w_ref.shape[2]
        per = cols // piece
        for p in range(per):
            res = jnp.dot(lhs, w_ref[q * per + p], preferred_element_type=jnp.float32)
            for n in range(SIDE):
                dst[q, n, :, p * piece:(p + 1) * piece] = res[n * rows:(n + 1) * rows]

    def ring1(q, n, k):
        src, dst, step = ((far.at[q, n, pl.ds(0, half)], from_l1.at[q, n], 1), (far.at[q, n, pl.ds(half, half)], from_r1.at[q, n], -1),
                          (right.at[q, n], from_l.at[q, n], 1), (left.at[q, n], from_r.at[q, n], -1))[k]
        return remote(src, dst, s1.at[q, n, k], r1.at[q, n, k], torus.peer(q, step))

    def ring2(q, k):
        src, dst, step = ((own.at[q, 0, pl.ds(0, half)], q_l1.at[q], 1), (own.at[q, 0, pl.ds(half, half)], q_r1.at[q], -1),
                          (own.at[q, 1], q_l.at[q], 1), (own.at[q, 2], q_r.at[q], -1))[k]
        return remote(src, dst, s2.at[q, k], r2.at[q, k], torus.peer(1 - q, step))

    if down is not None:
        mine, ls = rest[2:]
        load = pltpu.make_async_copy(wd_ref.at[down], mine, ls.at[0])
        load.start()
    if ffn:
        for k, (dy, dz) in enumerate(NEED):
            hp[k * rows:(k + 1) * rows, :] = a_ref[pl.ds(pl.multiple_of(torus.at(0, dy, dz) * rows, rows), rows), :]
    for q in (0, 1):
        if ffn:
            feed(q)
            if q == 0:
                down_load.wait()
        product(q, 2, far)
        for n in range(SIDE):
            ring1(q, n, 0).start()
            ring1(q, n, 1).start()
    if attn:
        ex = Exchange(line, load_attn_weights(line, 1, wq_ref, wk_ref, wv_ref, wo_ref, wqkv_ref, woa_ref), rest[0], rest[1])
        ex.begin()
    if down is not None:
        load.wait()
        stride = mine.shape[0]
        piece = stride // PIECES
        keep = pltpu.make_async_copy(mine, row_block(wda_ref, line.me * stride, stride, stride), ls.at[0])
        keep.start()
        ex = Exchange(line, [(wda_ref, stride, k * piece, piece, mine.at[pl.ds(k * piece, piece)]) for k in range(PIECES)], rest[0], rest[1])
        ex.begin()
    for q in (0, 1):
        if ffn and q == 0:
            feed(2)
        product(q, 1, right)
        for n in range(SIDE):
            ring1(q, n, 0).wait_recv()
            right[q, n, 0:half] += from_l1[q, n]
            ring1(q, n, 2).start()
        if ffn and q == 0:
            feed(3)
        product(q, -1, left)
        for n in range(SIDE):
            ring1(q, n, 1).wait_recv()
            left[q, n, half:rows] += from_r1[q, n]
            ring1(q, n, 3).start()
    for q in (0, 1):
        product(q, 0, own)
    if down is not None:
        ex.onward(0, 2)
    for n in range(SIDE):
        for q in (0, 1):
            ring1(q, n, 2).wait_recv()
            ring1(q, n, 3).wait_recv()
            own[q, n] += from_l[q, n] + from_r[q, n]
            if n == 0:
                ring2(q, 0).start()
                ring2(q, 1).start()
            if n == 1:
                ring2(q, 0).wait_recv()
                own[q, 1, 0:half] += q_l1[q]
                ring2(q, 2).start()
            if n == 2:
                ring2(q, 1).wait_recv()
                own[q, 2, half:rows] += q_r1[q]
                ring2(q, 3).start()
    total = []
    for q in (0, 1):
        ring2(q, 2).wait_recv()
        ring2(q, 3).wait_recv()
        total.append(own[q, 3] + q_l[q] + q_r[q])
    out = jnp.concatenate(total, axis=1).astype(jnp.bfloat16).astype(jnp.float32)
    x_new = (res_ref[...].astype(jnp.float32) + norm(out, sa_ref[...])).astype(jnp.bfloat16)
    here = pl.ds(pl.multiple_of(torus.at(0, 0, 0) * rows, rows), rows)
    if final:
        outgo, income, cs, cr = rest
        part = width // n_model
        for m in range(n_model):
            outgo[m] = x_new[:, m * part:(m + 1) * part]
        income[line.me] = outgo[line.me]
        copies = to_all(line, lambda step, peer: remote(outgo.at[peer], income.at[line.me], cs.at[step], cr.at[step], {'model': peer}))
        for c in copies:
            c.wait_recv()
        h_ref[here, :] = jnp.concatenate([income[m] for m in range(n_model)], axis=1)
    else:
        x_ref[...] = x_new
        h_ref[here, :] = norm(x_new.astype(jnp.float32), sb_ref[...]).astype(jnp.bfloat16)
    if attn:
        gather_blocks(torus, h_ref, hs, hr, ex.onward)
        ex.finish()
    elif down is not None:
        gather_blocks(torus, h_ref, hs, hr, lambda: ex.onward(2))
        ex.finish()
        keep.wait()
    else:
        gather_blocks(torus, h_ref, hs, hr)
    if final:
        for c in copies:
            c.wait_send()
    for q in (0, 1):
        for k in range(4):
            ring2(q, k).wait_send()
            for n in range(SIDE):
                ring1(q, n, k).wait_send()


def project(a, w, resid, scale_a, scale_b, n_model, cid, wide=None, final=False, attn=None, down=None, layer=None):
    rows, width = resid.shape
    cols = width // 2
    half = rows // 2

    def f32(*shape):
        return pltpu.VMEM((2,) + shape + (cols,), jnp.float32)

    scratch = [f32(SIDE, rows)] * 4 + [f32(SIDE, half)] * 2 + [f32(SIDE, rows)] * 2 + [f32(half)] * 2 + [f32(rows)] * 2
    scratch += [pltpu.SemaphoreType.DMA((2, SIDE, 4))] * 2 + [pltpu.SemaphoreType.DMA((2, 4))] * 2 + GATHER_SEMS
    h_shape = jax.ShapeDtypeStruct((rows * SIDE * SIDE, width), jnp.bfloat16)
    out_shape = (h_shape,) if final else (jax.ShapeDtypeStruct((rows, width), jnp.bfloat16), h_shape)
    args = (a, w, resid, scale_a, scale_b)
    in_specs, out_specs = [VMEM] * 5, (VMEM,) * len(out_shape)
    if wide is not None:
        args += tuple(wide)
        in_specs[1] = ANY
        in_specs += [ANY] * 2
        gate = wide[0]
        scratch += [pltpu.VMEM(a.shape, a.dtype), pltpu.VMEM((a.shape[0], gate.shape[1]), a.dtype), pltpu.VMEM(gate.shape, gate.dtype),
                    pltpu.VMEM(gate.shape, gate.dtype), pltpu.VMEM(w.shape, w.dtype), pltpu.SemaphoreType.DMA((3, WIDE))]
    if attn is not None:
        args += tuple(attn)
        in_specs += [VMEM] * 4
        out_shape += attn_weight_shapes(attn[0], attn[3], n_model)
        out_specs += (VMEM,) * 2
        scratch += exchange_sems(2)
    if down is not None:
        args += (down,)
        in_specs += [ANY]
        _, d_rows, d_cols = down.shape
        out_shape += (jax.ShapeDtypeStruct((d_rows * n_model, d_cols), down.dtype),)
        out_specs += (ANY,)
        scratch += exchange_sems(PIECES) + [pltpu.VMEM((d_rows, d_cols), down.dtype), pltpu.SemaphoreType.DMA((1,))]
    if final:
        part = (n_model, rows, width // n_model)
        scratch += [pltpu.VMEM(part, jnp.bfloat16)] * 2 + [pltpu.SemaphoreType.DMA((n_model,))] * 2
    return pl.pallas_call(
        functools.partial(project_kernel, n_model, wide is not None, final, attn is not None, layer),
        out_shape=out_shape, in_specs=in_specs, out_specs=out_specs, scratch_shapes=scratch,
        compiler_params=params(cid), cost_estimate=cost(100_000_000), name='project_reduce',
    )(*args)


def solution(mesh):
    n_model = mesh.shape['model']
    n_heads = mesh.shape['heads']
    col_spec = P(None, 'model', 'heads')
    row_spec = P(None, 'heads', 'model')
    cache_spec = P(None, None, 'heads', None)

    def body(hidden_in, seg_ids, positions, w_query, w_key, w_value, w_out, w_gate, w_up, w_down, norm_scales, qk_scales):
        n_tok, width_loc = hidden_in.shape
        head_dim = qk_scales.shape[-1]
        tok_m = n_tok // n_model
        tok_own = tok_m // n_heads
        hd = lax.axis_index('heads')
        md = lax.axis_index('model')

        attn_shards = (w_query, w_key, w_value, w_out)
        mine = lax.dynamic_index_in_dim(hidden_in.reshape(n_model, n_heads, tok_own, width_loc), hd, 1, keepdims=False)
        gate_0 = lax.all_gather(w_gate[0], 'model', axis=0, tiled=True)
        resid, h, scales, wqkv, wo, *shards = start(mine, norm_scales.reshape(-1, width_loc), *attn_shards, w_gate, w_up, 0)
        wide = [gate_0, lax.all_gather(shards[0], 'model', axis=0, tiled=True)]

        pos_m = lax.dynamic_slice_in_dim(positions, md * tok_m, tok_m)
        seg_m = lax.dynamic_slice_in_dim(seg_ids, md * tok_m, tok_m)

        settings = ((GLOBAL_BASE, GLOBAL_FACTOR, n_tok), (LOCAL_BASE, 1.0, WINDOW))
        keys, values = [], []
        for l in range(2):
            rope_base, pos_factor, window = settings[l]
            qkv = jnp.dot(h, wqkv, preferred_element_type=jnp.float32).astype(jnp.bfloat16)
            q, k, v = qkv[:, :head_dim], qkv[:, head_dim:2 * head_dim], qkv[:, 2 * head_dim:]
            cos_tab, sin_tab = rope_tables(pos_m, head_dim, rope_base, pos_factor)
            q = apply_rope(norm(q.astype(jnp.float32), qk_scales[l, 0]), cos_tab, sin_tab).astype(jnp.bfloat16)
            k = apply_rope(norm(k.astype(jnp.float32), qk_scales[l, 1]), cos_tab, sin_tab).astype(jnp.bfloat16)
            k_all, v_all = exchange(k, v, n_model, 1 + 3 * l)
            keys.append(k_all[:, None, :])
            values.append(v_all[:, None, :])
            o = attend(q, k_all, v_all, seg_m, pos_m, seg_ids, positions, window)
            wo = wo.reshape(n_model, head_dim, width_loc)
            row = 4 * l
            resid, h, wd = project(o, wo, resid, scales[row + 1:row + 2], scales[row + 2:row + 3], n_model, 2 + 3 * l, down=w_down, layer=l)
            wd = wd.reshape(n_model, w_down.shape[1], width_loc)
            if l == 0:
                h, *late = lax.optimization_barrier((h, *shards[1:]))
                wide_next = [lax.all_gather(w, 'model', axis=0, tiled=True) for w in late]
                resid, h, wqkv, wo = project(h, wd, resid, scales[3:4], scales[4:5], n_model, 3, wide=wide, attn=attn_shards)
            else:
                out, = project(h, wd, resid, scales[7:8], scales[7:8], n_model, 6, wide=wide_next, final=True)
        out = out.reshape(tok_m, n_model, width_loc).transpose(1, 0, 2).reshape(n_tok, width_loc)
        return out, jnp.stack(keys), jnp.stack(values)

    return jax.shard_map(body, mesh=mesh,
                         in_specs=(P(None, 'model'), P(), P(), col_spec, col_spec, col_spec, row_spec, col_spec, col_spec, row_spec, P(None, None, 'model'), P()),
                         out_specs=(P(None, 'model'), cache_spec, cache_spec),
                         check_vma=False)
```

```python
import functools

import jax
import jax.numpy as jnp
from jax import lax
from jax.experimental import pallas as pl
from jax.experimental.pallas import tpu as pltpu
from jax.sharding import PartitionSpec as P

NORM_EPS = 1e-6
WINDOW = 1024
GLOBAL_BASE = 1000000.0
GLOBAL_FACTOR = 8.0
LOCAL_BASE = 10000.0
MESH = pl.DeviceIdType.MESH
SIDE = 4
VMEM_LIMIT = 63 * 1024 * 1024


def norm(values, scale_row):
    mean_sq = jnp.mean(values * values, axis=-1, keepdims=True)
    return values * lax.rsqrt(mean_sq + NORM_EPS) * (1.0 + scale_row)


def rope_tables(positions, head_dim, rope_base, pos_factor):
    exponents = jnp.arange(0, head_dim, 2).astype(jnp.float32) / head_dim
    inv_freq = rope_base ** (-exponents)
    angles = (positions.astype(jnp.float32) / pos_factor)[:, None] * inv_freq[None, :]
    return jnp.cos(angles), jnp.sin(angles)


def apply_rope(values, cos_tab, sin_tab):
    half_dim = values.shape[-1] // 2
    first_half = values[..., :half_dim]
    second_half = values[..., half_dim:]
    return jnp.concatenate([first_half * cos_tab - second_half * sin_tab, second_half * cos_tab + first_half * sin_tab], axis=-1)


def attend(q, k, v, seg_q, pos_q, seg_ids, positions, window):
    scores = jnp.dot(q, k.T, preferred_element_type=jnp.float32) * (q.shape[-1] ** -0.5)
    gap = pos_q[:, None] - positions[None, :]
    allowed = (seg_q[:, None] == seg_ids[None, :]) & (gap >= 0) & (gap < window)
    scores = jnp.where(allowed, scores, -1e30)
    row_max = jnp.max(scores, axis=-1, keepdims=True)
    e = jnp.exp(scores - row_max)
    p = (e / jnp.sum(e, axis=-1, keepdims=True)).astype(jnp.bfloat16)
    return jnp.dot(p, v, preferred_element_type=jnp.float32).astype(jnp.bfloat16)


def wrap(i):
    return lax.rem(i + 2 * SIDE, SIDE)


def remote(src, dst, send, recv, to):
    return pltpu.make_async_remote_copy(src, dst, send, recv, device_id=to, device_id_type=MESH)


def row_block(ref, start, size, align):
    return ref.at[pl.ds(pl.multiple_of(start, align), size), :]


class Torus:
    def __init__(self):
        me = lax.axis_index('heads')
        self.own = (lax.rem(me, SIDE), me // SIDE)

    def block(self, axis, along, across):
        return across * SIDE + along if axis == 0 else along * SIDE + across

    def at(self, axis, da, db):
        return self.block(axis, wrap(self.own[axis] + da), wrap(self.own[1 - axis] + db))

    def peer(self, axis, step):
        return {'heads': self.at(axis, step, 0)}


class Line:
    def __init__(self, n_model):
        self.n = n_model
        self.me = lax.axis_index('model')
        chips = n_model // 2
        chip, core = self.me // 2, lax.rem(self.me, 2)
        self.right = lax.rem(chip + 1, chips) * 2 + core
        self.left = lax.rem(chip + chips - 1, chips) * 2 + core
        self.far = lax.rem(chip + 2, chips) * 2 + core
        self.mate = chip * 2 + 1 - core


def meet(torus, models):
    barrier = pltpu.get_barrier_semaphore()
    count = len(models)
    for other in models:
        pl.semaphore_signal(barrier, inc=1, device_id={'model': other}, device_id_type=MESH)
    if torus is not None:
        for axis in (0, 1):
            for step in (1, -1):
                pl.semaphore_signal(barrier, inc=1, device_id=torus.peer(axis, step), device_id_type=MESH)
                count += 1
    pl.semaphore_wait(barrier, count)


def gather_blocks(torus, h_ref, send, recv, between=lambda: None):
    apart = len(h_ref.shape) == 3
    rows = h_ref.shape[-2] // (SIDE * SIDE)
    cols = h_ref.shape[0 if apart else 1] // 2
    half = rows // 2

    def view(q, da, db, part):
        start = torus.at(q, da, db) * rows + (half if part == 2 else 0)
        if apart:
            return h_ref.at[pl.ds(q * cols, cols), pl.ds(pl.multiple_of(start, half), rows if part == 0 else half), :]
        return h_ref.at[pl.ds(pl.multiple_of(start, half), rows if part == 0 else half), pl.ds(q * cols, cols)]

    def ring(q, axis, base, offsets):
        def make(k, da, db, part, step):
            v = view(q, da, db, part)
            return remote(v, v, send.at[q, base, k], recv.at[q, base, k], torus.peer(axis, step))

        along = (lambda off: (off, offsets)) if axis == q else (lambda off: (offsets, off))
        return (make(0, *along(0), 0, 1), make(1, *along(0), 0, -1), make(2, *along(-1), 1, 1), make(3, *along(1), 2, -1))

    first = [ring(q, 1 - q, 0, 0) for q in (0, 1)]
    second = [[ring(q, q, 1 + n, off) for n, off in enumerate((0, -1, 1, 2))] for q in (0, 1)]

    def begin(copies):
        copies[0].start()
        copies[1].start()

    def onward(copies):
        copies[0].wait_recv()
        copies[2].start()
        copies[1].wait_recv()
        copies[3].start()

    for q in (0, 1):
        begin(first[q])
    for q in (0, 1):
        begin(second[q][0])
    for q in (0, 1):
        first[q][0].wait_recv()
        first[q][2].start()
        begin(second[q][1])
        first[q][1].wait_recv()
        first[q][3].start()
        begin(second[q][2])
    for q in (0, 1):
        onward(second[q][0])
    for q in (0, 1):
        first[q][2].wait_recv()
        first[q][3].wait_recv()
        begin(second[q][3])
    between()
    for n in (1, 2, 3):
        for q in (0, 1):
            onward(second[q][n])
    for q in (0, 1):
        for n in range(SIDE):
            second[q][n][2].wait_recv()
            second[q][n][3].wait_recv()
    for q in (0, 1):
        for copies in [first[q]] + second[q]:
            for c in copies:
                c.wait_send()


GATHER_SEMS = [pltpu.SemaphoreType.DMA((2, 1 + SIDE, 4)), pltpu.SemaphoreType.DMA((2, 1 + SIDE, 4))]


class Exchange:
    def __init__(self, line, items, send, recv):
        self.copies = []
        plan = [(line.me, line.right, 0), (line.me, line.left, 0), (line.me, line.mate, 0), (line.left, line.right, 1),
                (line.right, line.left, 2), (line.left, line.mate, 0), (line.right, line.mate, 0),
                (line.far, line.mate, 1), (line.far, line.mate, 2)]
        for a, (ref, stride, row, rows, src) in enumerate(items):
            half = rows // 2
            group = []
            for slot, (owner, to, part) in enumerate(plan):
                first = owner * stride + (row + (half if part == 2 else 0))
                v = row_block(ref, first, rows if part == 0 else half, half)
                group.append(remote(src if src is not None and slot < 3 else v, v, send.at[a, slot], recv.at[a, slot], {'model': to}))
            self.copies.append(group)

    def begin(self):
        for c in self.copies:
            c[0].start()
            c[1].start()
            c[2].start()

    def onward(self, lo=0, hi=None):
        for c in self.copies[lo:hi]:
            c[0].wait_recv()
            c[3].start()
            c[1].wait_recv()
            c[4].start()
            c[5].start()
            c[6].start()

    def finish(self):
        for c in self.copies:
            c[3].wait_recv()
            c[7].start()
            c[4].wait_recv()
            c[8].start()
        for c in self.copies:
            for slot in (2, 5, 6, 7, 8):
                c[slot].wait_recv()
            for one in c:
                one.wait_send()


def exchange_sems(count):
    return [pltpu.SemaphoreType.DMA((count, 9)), pltpu.SemaphoreType.DMA((count, 9))]


def exchange_kernel(n_model, k_ref, v_ref, ka_ref, va_ref, send, recv):
    line = Line(n_model)
    rows = k_ref.shape[0]
    meet(None, (line.right, line.left, line.mate))
    here = pl.ds(pl.multiple_of(line.me * rows, rows), rows)
    ka_ref[here, :] = k_ref[...]
    va_ref[here, :] = v_ref[...]
    piece = rows // 2
    ex = Exchange(line, [(ref, rows, at, piece, None) for at in (0, piece) for ref in (ka_ref, va_ref)], send, recv)
    ex.begin()
    ex.onward()
    ex.finish()


VMEM = pl.BlockSpec(memory_space=pltpu.VMEM)
ANY = pl.BlockSpec(memory_space=pl.ANY)
PIECES = 4
WIDE = 6
NEED = ((2, 2), (2, 1), (2, -1), (2, 0), (1, 2), (-1, 2), (0, 2), (1, 1),
        (1, -1), (1, 0), (-1, 1), (-1, -1), (-1, 0), (0, 1), (0, -1), (0, 0))


def params(cid):
    return pltpu.CompilerParams(collective_id=cid, has_side_effects=True, vmem_limit_bytes=VMEM_LIMIT)


def cost(flops):
    return pl.CostEstimate(flops=flops, bytes_accessed=10_000_000, transcendentals=0)


def exchange(k, v, n_model, cid):
    rows, dim = k.shape
    full = jax.ShapeDtypeStruct((rows * n_model, dim), k.dtype)
    return pl.pallas_call(
        functools.partial(exchange_kernel, n_model),
        out_shape=(full, full), in_specs=[VMEM] * 2, out_specs=(VMEM, VMEM),
        scratch_shapes=exchange_sems(4), compiler_params=params(cid), cost_estimate=cost(100_000_000), name='exchange_kv',
    )(k, v)


def load_attn_weights(line, layer, wq_ref, wk_ref, wv_ref, wo_ref, wqkv_ref, woa_ref):
    rows, dim = wq_ref.shape[1:]
    here = pl.ds(pl.multiple_of(line.me * rows, rows), rows)
    for at, ref in enumerate((wq_ref, wk_ref, wv_ref)):
        wqkv_ref[here, at * dim:(at + 1) * dim] = ref[layer]
    o_rows = wo_ref.shape[1]
    woa_ref[pl.ds(pl.multiple_of(line.me * o_rows, o_rows), o_rows), :] = wo_ref[layer]
    return [(wqkv_ref, rows, 0, rows, None), (woa_ref, o_rows, 0, o_rows, None)]


def to_all(line, make):
    copies = []
    for step in range(1, line.n):
        peer = lax.rem(line.me + step, line.n)
        copies.append(make(step, peer))
    for c in copies:
        c.start()
    return copies


def others(line):
    return [lax.rem(line.me + step, line.n) for step in range(1, line.n)]


def start_kernel(n_model, hid_ref, sc_ref, wq_ref, wk_ref, wv_ref, wo_ref, wg_ref, wu_ref,
                 x_ref, h_ref, sca_ref, wqkv_ref, woa_ref, u0_ref, g1_ref, u1_ref,
                 xin, scin, stage, xs, xr, ss, sr, ls, hs, hr, es, er):
    torus, line = Torus(), Line(n_model)
    rows = x_ref.shape[0]
    shards = ((wu_ref, 0, u0_ref), (wg_ref, 1, g1_ref), (wu_ref, 1, u1_ref))
    loads = [pltpu.make_async_copy(ref.at[layer], stage.at[k], ls.at[k]) for k, (ref, layer, _) in enumerate(shards)]
    stores = [pltpu.make_async_copy(stage.at[k], dst, ls.at[k]) for k, (_, _, dst) in enumerate(shards)]
    for c in loads:
        c.start()
    meet(torus, others(line))
    xin[line.me] = hid_ref[line.me]
    scin[line.me] = sc_ref[...]
    xc = to_all(line, lambda step, peer: remote(hid_ref.at[peer], xin.at[line.me], xs.at[step], xr.at[step], {'model': peer}))
    sc = to_all(line, lambda step, peer: remote(sc_ref, scin.at[line.me], ss.at[step], sr.at[step], {'model': peer}))
    ex = Exchange(line, load_attn_weights(line, 0, wq_ref, wk_ref, wv_ref, wo_ref, wqkv_ref, woa_ref), es, er)
    ex.begin()
    for load, store in zip(loads, stores):
        load.wait()
        store.start()
    for c in xc + sc:
        c.wait_recv()
    sca_ref[...] = jnp.concatenate([scin[m] for m in range(n_model)], axis=1)
    x = jnp.concatenate([xin[m] for m in range(n_model)], axis=1)
    x_ref[...] = x
    mine = torus.at(0, 0, 0)
    h_ref[pl.ds(pl.multiple_of(mine * rows, rows), rows), :] = norm(x.astype(jnp.float32), sca_ref[0:1]).astype(jnp.bfloat16)
    gather_blocks(torus, h_ref, hs, hr, ex.onward)
    ex.finish()
    for c in stores:
        c.wait()
    for c in xc + sc:
        c.wait_send()


def attn_weight_shapes(wq, wo, n_model):
    _, rows, dim = wq.shape
    _, o_rows, o_cols = wo.shape
    return (jax.ShapeDtypeStruct((rows * n_model, 3 * dim), wq.dtype), jax.ShapeDtypeStruct((o_rows * n_model, o_cols), wo.dtype))


def start(hidden_mine, scales, wq, wk, wv, wo, wg, wu, cid):
    n_model, rows, width_loc = hidden_mine.shape
    width = n_model * width_loc
    peer_sems = [pltpu.SemaphoreType.DMA((n_model,))] * 4
    return pl.pallas_call(
        functools.partial(start_kernel, n_model),
        out_shape=(jax.ShapeDtypeStruct((rows, width), hidden_mine.dtype),
                   jax.ShapeDtypeStruct((rows * SIDE * SIDE, width), hidden_mine.dtype),
                   jax.ShapeDtypeStruct((scales.shape[0], width), scales.dtype)) + attn_weight_shapes(wq, wo, n_model)
        + (jax.ShapeDtypeStruct(wg.shape[1:], wg.dtype),) * 3,
        in_specs=[VMEM] * 6 + [ANY] * 2, out_specs=(VMEM,) * 5 + (ANY,) * 3,
        scratch_shapes=[pltpu.VMEM(hidden_mine.shape, hidden_mine.dtype), pltpu.VMEM((n_model,) + scales.shape, scales.dtype),
                        pltpu.VMEM((3,) + wg.shape[1:], wg.dtype)]
        + peer_sems + [pltpu.SemaphoreType.DMA((3,))] + GATHER_SEMS + exchange_sems(2),
        compiler_params=params(cid), cost_estimate=cost(100_000_000), name='start',
    )(hidden_mine, scales, wq, wk, wv, wo, wg, wu)


def project_kernel(n_model, ffn, final, attn, down, a_ref, w_ref, res_ref, sa_ref, sb_ref, *rest):
    rest = list(rest)
    if ffn:
        wg_any, wu_any = rest[:2]
        rest = rest[2:]
    fetch = attn or down is not None
    if attn:
        wq_ref, wk_ref, wv_ref, wo_ref = rest[:4]
        rest = rest[4:]
    if down is not None:
        wd_ref = rest.pop(0)
    if not final:
        x_ref = rest.pop(0)
    h_ref = rest.pop(0)
    if attn:
        wqkv_ref, woa_ref = rest[:2]
        rest = rest[2:]
    if down is not None:
        wda_ref = rest.pop(0)
    far, right, left, own, from_l1, from_r1, from_l, from_r, q_l1, q_r1, q_l, q_r, s1, r1, s2, r2, hs, hr = rest[:18]
    rest = rest[18:]
    if ffn:
        hp, mid, wg_ref, wu_ref, wd_ref2, lhs_ref, fs = rest[:7]
        rest = rest[7:]
    torus, line = Torus(), Line(n_model)
    rows, width = res_ref.shape
    half = rows // 2
    cols = width // 2
    if ffn:
        span = wg_any.shape[1] // WIDE

        def wide_load(k, n):
            src, dst = ((wg_any, wg_ref), (wu_any, wu_ref))[k]
            at = pl.ds(pl.multiple_of(n * span, span), span)
            return pltpu.make_async_copy(src.at[:, at], dst.at[:, at], fs.at[k, n])

        for n in range(WIDE):
            wide_load(0, n).start()
            wide_load(1, n).start()
        down_load = pltpu.make_async_copy(w_ref, wd_ref2, fs.at[2, 0])
        down_load.start()
        w_ref = wd_ref2
    if final:
        meet(torus, others(line))
    elif fetch:
        meet(torus, (line.right, line.left, line.mate))
    else:
        meet(torus, ())
    order = (2, 1, -1, 0)

    def feed(group):
        these = slice(group * SIDE * rows, (group + 1) * SIDE * rows)

        def step(n, carry):
            if group == 0:
                wide_load(0, n).wait()
                wide_load(1, n).wait()
            at = pl.ds(pl.multiple_of(n * span, span), span)
            lhs = hp[these, :]
            g = jnp.dot(lhs, wg_ref[:, at], preferred_element_type=jnp.float32).astype(jnp.bfloat16)
            u = jnp.dot(lhs, wu_ref[:, at], preferred_element_type=jnp.float32).astype(jnp.bfloat16)
            act = jax.nn.gelu(g.astype(jnp.float32), approximate=True)
            mid[these, at] = (act * u.astype(jnp.float32)).astype(jnp.bfloat16)
            return carry

        lax.fori_loop(0, WIDE, step, 0)

    def operand(q, off, o):
        if ffn:
            at = NEED.index((off, o) if q == 0 else (o, off)) * rows
            return mid[at:at + rows, :]
        return a_ref[pl.ds(pl.multiple_of(torus.at(q, off, o) * rows, rows), rows), :]

    def product(q, off, dst):
        lhs = jnp.concatenate([operand(q, off, o) for o in order], axis=0)
        piece = w_ref.shape[2]
        per = cols // piece
        if ffn:
            lhs_ref[...] = lhs

            def step(p, carry):
                res = jnp.dot(lhs_ref[...], w_ref[q * per + p], preferred_element_type=jnp.float32)
                at = pl.ds(pl.multiple_of(p * piece, piece), piece)
                for n in range(SIDE):
                    dst[q, n, :, at] = res[n * rows:(n + 1) * rows]
                return carry

            lax.fori_loop(0, per, step, 0)
            return
        for p in range(per):
            res = jnp.dot(lhs, w_ref[q * per + p], preferred_element_type=jnp.float32)
            for n in range(SIDE):
                dst[q, n, :, p * piece:(p + 1) * piece] = res[n * rows:(n + 1) * rows]

    def held(q):
        return q == 1 or not ffn

    def ring1(q, n, k):
        src, dst, step = ((far.at[q, n, pl.ds(0, half)], from_l1.at[q, n], 1), (far.at[q, n, pl.ds(half, half)], from_r1.at[q, n], -1),
                          (right.at[q, n], from_l.at[q, n], 1), (left.at[q, n], from_r.at[q, n], -1))[k]
        return remote(src, dst, s1.at[q, n, k], r1.at[q, n, k], torus.peer(q, step))

    def ring2(q, k):
        src, dst, step = ((own.at[q, 0, pl.ds(0, half)], q_l1.at[q], 1), (own.at[q, 0, pl.ds(half, half)], q_r1.at[q], -1),
                          (own.at[q, 1], q_l.at[q], 1), (own.at[q, 2], q_r.at[q], -1))[k]
        return remote(src, dst, s2.at[q, k], r2.at[q, k], torus.peer(1 - q, step))

    if down is not None:
        mine, ls = rest[2:]
        load = pltpu.make_async_copy(wd_ref.at[down], mine, ls.at[0])
        load.start()
    if ffn:
        for k, (dy, dz) in enumerate(NEED):
            hp[k * rows:(k + 1) * rows, :] = a_ref[pl.ds(pl.multiple_of(torus.at(0, dy, dz) * rows, rows), rows), :]
    for q in (0, 1):
        if ffn:
            feed(q)
            if q == 0:
                down_load.wait()
        product(q, 2, far)
        for n in range(SIDE):
            ring1(q, n, 0).start()
            ring1(q, n, 1).start()
    if attn:
        ex = Exchange(line, load_attn_weights(line, 1, wq_ref, wk_ref, wv_ref, wo_ref, wqkv_ref, woa_ref), rest[0], rest[1])
        ex.begin()
    if down is not None:
        load.wait()
        stride = mine.shape[0]
        piece = stride // PIECES
        keep = pltpu.make_async_copy(mine, row_block(wda_ref, line.me * stride, stride, stride), ls.at[0])
        keep.start()
        ex = Exchange(line, [(wda_ref, stride, k * piece, piece, mine.at[pl.ds(k * piece, piece)]) for k in range(PIECES)], rest[0], rest[1])
        ex.begin()
    for q in (0, 1):
        if ffn and q == 0:
            feed(2)
        product(q, 1, right)
        for n in range(SIDE):
            ring1(q, n, 0).wait_recv()
            right[q, n, 0:half] += from_l1[q, n]
            if n < 2 or not held(q):
                ring1(q, n, 2).start()
        if ffn and q == 0:
            feed(3)
        product(q, -1, left)
        for n in range(SIDE):
            ring1(q, n, 1).wait_recv()
            left[q, n, half:rows] += from_r1[q, n]
            if n < 2 or not held(q):
                ring1(q, n, 3).start()
    for q in (0, 1):
        product(q, 0, own)
    if down is not None:
        ex.onward(0, 2)
    for n in range(SIDE):
        for q in (0, 1):
            ring1(q, n, 2).wait_recv()
            ring1(q, n, 3).wait_recv()
            own[q, n] += from_l[q, n] + from_r[q, n]
            if n == 0:
                ring2(q, 0).start()
                ring2(q, 1).start()
            if n == 1:
                ring2(q, 0).wait_recv()
                own[q, 1, 0:half] += q_l1[q]
                ring2(q, 2).start()
            if n == 2:
                ring2(q, 1).wait_recv()
                own[q, 2, half:rows] += q_r1[q]
                ring2(q, 3).start()
        for q in (0, 1):
            if n < 2 and held(q):
                ring1(q, n + 2, 2).start()
                ring1(q, n + 2, 3).start()
    total = []
    for q in (0, 1):
        ring2(q, 2).wait_recv()
        ring2(q, 3).wait_recv()
        total.append(own[q, 3] + q_l[q] + q_r[q])
    out = jnp.concatenate(total, axis=1).astype(jnp.bfloat16).astype(jnp.float32)
    x_new = (res_ref[...].astype(jnp.float32) + norm(out, sa_ref[...])).astype(jnp.bfloat16)
    here = pl.ds(pl.multiple_of(torus.at(0, 0, 0) * rows, rows), rows)
    if final:
        outgo, income, cs, cr = rest
        part = width // n_model
        for m in range(n_model):
            outgo[m] = x_new[:, m * part:(m + 1) * part]
        income[line.me] = outgo[line.me]
        copies = to_all(line, lambda step, peer: remote(outgo.at[peer], income.at[line.me], cs.at[step], cr.at[step], {'model': peer}))
        for c in copies:
            c.wait_recv()
        for m in range(n_model):
            h_ref[m, here, :] = income[m]
    else:
        x_ref[...] = x_new
        h_ref[here, :] = norm(x_new.astype(jnp.float32), sb_ref[...]).astype(jnp.bfloat16)
    if attn:
        gather_blocks(torus, h_ref, hs, hr, ex.onward)
        ex.finish()
    elif down is not None:
        gather_blocks(torus, h_ref, hs, hr, lambda: ex.onward(2))
        ex.finish()
        keep.wait()
    else:
        gather_blocks(torus, h_ref, hs, hr)
    if final:
        for c in copies:
            c.wait_send()
    for q in (0, 1):
        for k in range(4):
            ring2(q, k).wait_send()
            for n in range(SIDE):
                ring1(q, n, k).wait_send()


def project(a, w, resid, scale_a, scale_b, n_model, cid, wide=None, final=False, attn=None, down=None, layer=None):
    rows, width = resid.shape
    cols = width // 2
    half = rows // 2

    def f32(*shape):
        return pltpu.VMEM((2,) + shape + (cols,), jnp.float32)

    scratch = [f32(SIDE, rows)] * 4 + [f32(SIDE, half)] * 2 + [f32(SIDE, rows)] * 2 + [f32(half)] * 2 + [f32(rows)] * 2
    scratch += [pltpu.SemaphoreType.DMA((2, SIDE, 4))] * 2 + [pltpu.SemaphoreType.DMA((2, 4))] * 2 + GATHER_SEMS
    h_dims = (n_model, rows * SIDE * SIDE, width // n_model) if final else (rows * SIDE * SIDE, width)
    h_shape = jax.ShapeDtypeStruct(h_dims, jnp.bfloat16)
    out_shape = (h_shape,) if final else (jax.ShapeDtypeStruct((rows, width), jnp.bfloat16), h_shape)
    args = (a, w, resid, scale_a, scale_b)
    in_specs, out_specs = [VMEM] * 5, (VMEM,) * len(out_shape)
    if wide is not None:
        args += tuple(wide)
        in_specs[1] = ANY
        in_specs += [ANY] * 2
        gate = wide[0]
        scratch += [pltpu.VMEM(a.shape, a.dtype), pltpu.VMEM((a.shape[0], gate.shape[1]), a.dtype), pltpu.VMEM(gate.shape, gate.dtype),
                    pltpu.VMEM(gate.shape, gate.dtype), pltpu.VMEM(w.shape, w.dtype),
                    pltpu.VMEM((SIDE * rows, w.shape[1]), w.dtype), pltpu.SemaphoreType.DMA((3, WIDE))]
    if attn is not None:
        args += tuple(attn)
        in_specs += [VMEM] * 4
        out_shape += attn_weight_shapes(attn[0], attn[3], n_model)
        out_specs += (VMEM,) * 2
        scratch += exchange_sems(2)
    if down is not None:
        args += (down,)
        in_specs += [ANY]
        _, d_rows, d_cols = down.shape
        out_shape += (jax.ShapeDtypeStruct((d_rows * n_model, d_cols), down.dtype),)
        out_specs += (ANY,)
        scratch += exchange_sems(PIECES) + [pltpu.VMEM((d_rows, d_cols), down.dtype), pltpu.SemaphoreType.DMA((1,))]
    if final:
        part = (n_model, rows, width // n_model)
        scratch += [pltpu.VMEM(part, jnp.bfloat16)] * 2 + [pltpu.SemaphoreType.DMA((n_model,))] * 2
    return pl.pallas_call(
        functools.partial(project_kernel, n_model, wide is not None, final, attn is not None, layer),
        out_shape=out_shape, in_specs=in_specs, out_specs=out_specs, scratch_shapes=scratch,
        compiler_params=params(cid), cost_estimate=cost(100_000_000), name='project_reduce',
    )(*args)


def solution(mesh):
    n_model = mesh.shape['model']
    n_heads = mesh.shape['heads']
    col_spec = P(None, 'model', 'heads')
    row_spec = P(None, 'heads', 'model')
    cache_spec = P(None, None, 'heads', None)

    def body(hidden_in, seg_ids, positions, w_query, w_key, w_value, w_out, w_gate, w_up, w_down, norm_scales, qk_scales):
        n_tok, width_loc = hidden_in.shape
        head_dim = qk_scales.shape[-1]
        tok_m = n_tok // n_model
        tok_own = tok_m // n_heads
        hd = lax.axis_index('heads')
        md = lax.axis_index('model')

        attn_shards = (w_query, w_key, w_value, w_out)
        mine = lax.dynamic_index_in_dim(hidden_in.reshape(n_model, n_heads, tok_own, width_loc), hd, 1, keepdims=False)
        gate_0 = lax.all_gather(w_gate[0], 'model', axis=0, tiled=True)
        resid, h, scales, wqkv, wo, *shards = start(mine, norm_scales.reshape(-1, width_loc), *attn_shards, w_gate, w_up, 0)
        wide = [gate_0, lax.all_gather(shards[0], 'model', axis=0, tiled=True)]

        pos_m = lax.dynamic_slice_in_dim(positions, md * tok_m, tok_m)
        seg_m = lax.dynamic_slice_in_dim(seg_ids, md * tok_m, tok_m)

        settings = ((GLOBAL_BASE, GLOBAL_FACTOR, n_tok), (LOCAL_BASE, 1.0, WINDOW))
        keys, values = [], []
        for l in range(2):
            rope_base, pos_factor, window = settings[l]
            qkv = jnp.dot(h, wqkv, preferred_element_type=jnp.float32).astype(jnp.bfloat16)
            q, k, v = qkv[:, :head_dim], qkv[:, head_dim:2 * head_dim], qkv[:, 2 * head_dim:]
            cos_tab, sin_tab = rope_tables(pos_m, head_dim, rope_base, pos_factor)
            q = apply_rope(norm(q.astype(jnp.float32), qk_scales[l, 0]), cos_tab, sin_tab).astype(jnp.bfloat16)
            k = apply_rope(norm(k.astype(jnp.float32), qk_scales[l, 1]), cos_tab, sin_tab).astype(jnp.bfloat16)
            k_all, v_all = exchange(k, v, n_model, 1 + 3 * l)
            if l == 1:
                k_all, up_last = lax.optimization_barrier((k_all, late[1]))
                wide_next.append(lax.all_gather(up_last, 'model', axis=0, tiled=True))
            keys.append(k_all[:, None, :])
            values.append(v_all[:, None, :])
            o = attend(q, k_all, v_all, seg_m, pos_m, seg_ids, positions, window)
            wo = wo.reshape(n_model, head_dim, width_loc)
            row = 4 * l
            resid, h, wd = project(o, wo, resid, scales[row + 1:row + 2], scales[row + 2:row + 3], n_model, 2 + 3 * l, down=w_down, layer=l)
            wd = wd.reshape(n_model, w_down.shape[1], width_loc)
            if l == 0:
                h, *late = lax.optimization_barrier((h, *shards[1:]))
                wide_next = [lax.all_gather(late[0], 'model', axis=0, tiled=True)]
                resid, h, wqkv, wo = project(h, wd, resid, scales[3:4], scales[4:5], n_model, 3, wide=wide, attn=attn_shards)
            else:
                out, = project(h, wd, resid, scales[7:8], scales[7:8], n_model, 6, wide=wide_next, final=True)
        out = out.reshape(n_tok, width_loc)
        return out, jnp.stack(keys), jnp.stack(values)

    return jax.shard_map(body, mesh=mesh,
                         in_specs=(P(None, 'model'), P(), P(), col_spec, col_spec, col_spec, row_spec, col_spec, col_spec, row_spec, P(None, None, 'model'), P()),
                         out_specs=(P(None, 'model'), cache_spec, cache_spec),
                         check_vma=False)
```

```python
import functools

import jax
import jax.numpy as jnp
from jax import lax
from jax.experimental import pallas as pl
from jax.experimental.pallas import tpu as pltpu
from jax.sharding import PartitionSpec as P

NORM_EPS = 1e-6
WINDOW = 1024
GLOBAL_BASE = 1000000.0
GLOBAL_FACTOR = 8.0
LOCAL_BASE = 10000.0
MESH = pl.DeviceIdType.MESH
SIDE = 4
VMEM_LIMIT = 63 * 1024 * 1024


def norm(values, scale_row):
    mean_sq = jnp.mean(values * values, axis=-1, keepdims=True)
    return values * lax.rsqrt(mean_sq + NORM_EPS) * (1.0 + scale_row)


def rope_tables(positions, head_dim, rope_base, pos_factor):
    exponents = jnp.arange(0, head_dim, 2).astype(jnp.float32) / head_dim
    inv_freq = rope_base ** (-exponents)
    angles = (positions.astype(jnp.float32) / pos_factor)[:, None] * inv_freq[None, :]
    return jnp.cos(angles), jnp.sin(angles)


def apply_rope(values, cos_tab, sin_tab):
    half_dim = values.shape[-1] // 2
    first_half = values[..., :half_dim]
    second_half = values[..., half_dim:]
    return jnp.concatenate([first_half * cos_tab - second_half * sin_tab, second_half * cos_tab + first_half * sin_tab], axis=-1)


def attend(q, k, v, seg_q, pos_q, seg_ids, positions, window):
    scores = jnp.dot(q, k.T, preferred_element_type=jnp.float32) * (q.shape[-1] ** -0.5)
    gap = pos_q[:, None] - positions[None, :]
    allowed = (seg_q[:, None] == seg_ids[None, :]) & (gap >= 0) & (gap < window)
    scores = jnp.where(allowed, scores, -1e30)
    row_max = jnp.max(scores, axis=-1, keepdims=True)
    e = jnp.exp(scores - row_max)
    p = (e / jnp.sum(e, axis=-1, keepdims=True)).astype(jnp.bfloat16)
    return jnp.dot(p, v, preferred_element_type=jnp.float32).astype(jnp.bfloat16)


def wrap(i):
    return lax.rem(i + 2 * SIDE, SIDE)


def remote(src, dst, send, recv, to):
    return pltpu.make_async_remote_copy(src, dst, send, recv, device_id=to, device_id_type=MESH)


def row_block(ref, start, size, align):
    return ref.at[pl.ds(pl.multiple_of(start, align), size), :]


class Torus:
    def __init__(self):
        me = lax.axis_index('heads')
        self.own = (lax.rem(me, SIDE), me // SIDE)

    def block(self, axis, along, across):
        return across * SIDE + along if axis == 0 else along * SIDE + across

    def at(self, axis, da, db):
        return self.block(axis, wrap(self.own[axis] + da), wrap(self.own[1 - axis] + db))

    def peer(self, axis, step):
        return {'heads': self.at(axis, step, 0)}


class Line:
    def __init__(self, n_model):
        self.n = n_model
        self.me = lax.axis_index('model')
        chips = n_model // 2
        chip, core = self.me // 2, lax.rem(self.me, 2)
        self.right = lax.rem(chip + 1, chips) * 2 + core
        self.left = lax.rem(chip + chips - 1, chips) * 2 + core
        self.far = lax.rem(chip + 2, chips) * 2 + core
        self.mate = chip * 2 + 1 - core


def meet(torus, models):
    barrier = pltpu.get_barrier_semaphore()
    count = len(models)
    for other in models:
        pl.semaphore_signal(barrier, inc=1, device_id={'model': other}, device_id_type=MESH)
    if torus is not None:
        for axis in (0, 1):
            for step in (1, -1):
                pl.semaphore_signal(barrier, inc=1, device_id=torus.peer(axis, step), device_id_type=MESH)
                count += 1
    pl.semaphore_wait(barrier, count)


def gather_blocks(torus, h_ref, send, recv, between=lambda: None):
    apart = len(h_ref.shape) == 3
    rows = h_ref.shape[-2] // (SIDE * SIDE)
    cols = h_ref.shape[0 if apart else 1] // 2
    half = rows // 2

    def view(q, da, db, part):
        start = torus.at(q, da, db) * rows + (half if part == 2 else 0)
        if apart:
            return h_ref.at[pl.ds(q * cols, cols), pl.ds(pl.multiple_of(start, half), rows if part == 0 else half), :]
        return h_ref.at[pl.ds(pl.multiple_of(start, half), rows if part == 0 else half), pl.ds(q * cols, cols)]

    def ring(q, axis, base, offsets):
        def make(k, da, db, part, step):
            v = view(q, da, db, part)
            return remote(v, v, send.at[q, base, k], recv.at[q, base, k], torus.peer(axis, step))

        along = (lambda off: (off, offsets)) if axis == q else (lambda off: (offsets, off))
        return (make(0, *along(0), 0, 1), make(1, *along(0), 0, -1), make(2, *along(-1), 1, 1), make(3, *along(1), 2, -1))

    first = [ring(q, 1 - q, 0, 0) for q in (0, 1)]
    second = [[ring(q, q, 1 + n, off) for n, off in enumerate((0, -1, 1, 2))] for q in (0, 1)]

    def begin(copies):
        copies[0].start()
        copies[1].start()

    def onward(copies):
        copies[0].wait_recv()
        copies[2].start()
        copies[1].wait_recv()
        copies[3].start()

    for q in (0, 1):
        begin(first[q])
    for q in (0, 1):
        begin(second[q][0])
    for q in (0, 1):
        first[q][0].wait_recv()
        first[q][2].start()
        begin(second[q][1])
        first[q][1].wait_recv()
        first[q][3].start()
        begin(second[q][2])
    for q in (0, 1):
        onward(second[q][0])
    for q in (0, 1):
        first[q][2].wait_recv()
        first[q][3].wait_recv()
        begin(second[q][3])
    between()
    for n in (1, 2, 3):
        for q in (0, 1):
            onward(second[q][n])
    for q in (0, 1):
        for n in range(SIDE):
            second[q][n][2].wait_recv()
            second[q][n][3].wait_recv()
    for q in (0, 1):
        for copies in [first[q]] + second[q]:
            for c in copies:
                c.wait_send()


GATHER_SEMS = [pltpu.SemaphoreType.DMA((2, 1 + SIDE, 4)), pltpu.SemaphoreType.DMA((2, 1 + SIDE, 4))]


class Exchange:
    def __init__(self, line, items, send, recv):
        self.copies = []
        plan = [(line.me, line.right, 0), (line.me, line.left, 0), (line.me, line.mate, 0), (line.left, line.right, 1),
                (line.right, line.left, 2), (line.left, line.mate, 0), (line.right, line.mate, 0),
                (line.far, line.mate, 1), (line.far, line.mate, 2)]
        for a, (ref, stride, row, rows, src) in enumerate(items):
            half = rows // 2
            group = []
            for slot, (owner, to, part) in enumerate(plan):
                first = owner * stride + (row + (half if part == 2 else 0))
                v = row_block(ref, first, rows if part == 0 else half, half)
                group.append(remote(src if src is not None and slot < 3 else v, v, send.at[a, slot], recv.at[a, slot], {'model': to}))
            self.copies.append(group)

    def begin(self, lo=0, hi=None):
        for c in self.copies[lo:hi]:
            c[0].start()
            c[1].start()
            c[2].start()

    def onward(self, lo=0, hi=None):
        for c in self.copies[lo:hi]:
            c[0].wait_recv()
            c[3].start()
            c[1].wait_recv()
            c[4].start()
            c[5].start()
            c[6].start()

    def finish(self):
        for c in self.copies:
            c[3].wait_recv()
            c[7].start()
            c[4].wait_recv()
            c[8].start()
        for c in self.copies:
            for slot in (2, 5, 6, 7, 8):
                c[slot].wait_recv()
            for one in c:
                one.wait_send()


def exchange_sems(count):
    return [pltpu.SemaphoreType.DMA((count, 9)), pltpu.SemaphoreType.DMA((count, 9))]


def qkv_kernel(n_model, h_ref, w_any, cos_ref, sin_ref, qk_ref, q_ref, ka_ref, va_ref, w_ref, ls, send, recv):
    line = Line(n_model)
    rows, dim = q_ref.shape
    parts = [pl.ds(at * dim, dim) for at in range(3)]
    loads = [pltpu.make_async_copy(w_any.at[:, p], w_ref.at[:, p], ls.at[k]) for k, p in enumerate(parts)]
    for k in (1, 2, 0):
        loads[k].start()
    meet(None, (line.right, line.left, line.mate))
    here = pl.ds(pl.multiple_of(line.me * rows, rows), rows)
    piece = rows // 2
    ex = Exchange(line, [(ref, rows, at, piece, None) for ref in (ka_ref, va_ref) for at in (0, piece)], send, recv)

    def made(k):
        loads[k].wait()
        return jnp.dot(h_ref[...], w_ref[:, k * dim:(k + 1) * dim], preferred_element_type=jnp.float32).astype(jnp.bfloat16)

    def turned(values, row):
        return apply_rope(norm(values.astype(jnp.float32), qk_ref[row:row + 1]), cos_ref[...], sin_ref[...]).astype(jnp.bfloat16)

    ka_ref[here, :] = turned(made(1), 1)
    ex.begin(0, 2)
    va_ref[here, :] = made(2)
    ex.begin(2)
    q_ref[...] = turned(made(0), 0)
    ex.onward()
    ex.finish()


VMEM = pl.BlockSpec(memory_space=pltpu.VMEM)
ANY = pl.BlockSpec(memory_space=pl.ANY)
PIECES = 4
WIDE = 4
NEED = ((2, 2), (2, 1), (2, -1), (2, 0), (1, 2), (-1, 2), (0, 2), (1, 1),
        (1, -1), (1, 0), (-1, 1), (-1, -1), (-1, 0), (0, 1), (0, -1), (0, 0))


def params(cid):
    return pltpu.CompilerParams(collective_id=cid, has_side_effects=True, vmem_limit_bytes=VMEM_LIMIT)


def cost(flops):
    return pl.CostEstimate(flops=flops, bytes_accessed=10_000_000, transcendentals=0)


def make_qkv(h, w, cos_tab, sin_tab, qk_rows, n_model, cid):
    rows, dim = h.shape[0], qk_rows.shape[1]
    full = jax.ShapeDtypeStruct((rows * n_model, dim), h.dtype)
    return pl.pallas_call(
        functools.partial(qkv_kernel, n_model),
        out_shape=(jax.ShapeDtypeStruct((rows, dim), h.dtype), full, full), in_specs=[VMEM, ANY, VMEM, VMEM, VMEM], out_specs=(VMEM,) * 3,
        scratch_shapes=[pltpu.VMEM(w.shape, w.dtype), pltpu.SemaphoreType.DMA((3,))] + exchange_sems(4),
        compiler_params=params(cid), cost_estimate=cost(100_000_000), name='make_qkv',
    )(h, w, cos_tab, sin_tab, qk_rows)


def load_attn_weights(line, layer, wq_ref, wk_ref, wv_ref, wo_ref, wqkv_ref, woa_ref):
    rows, dim = wq_ref.shape[1:]
    here = pl.ds(pl.multiple_of(line.me * rows, rows), rows)
    for at, ref in enumerate((wq_ref, wk_ref, wv_ref)):
        wqkv_ref[here, at * dim:(at + 1) * dim] = ref[layer]
    o_rows = wo_ref.shape[1]
    woa_ref[pl.ds(pl.multiple_of(line.me * o_rows, o_rows), o_rows), :] = wo_ref[layer]
    return [(wqkv_ref, rows, 0, rows, None), (woa_ref, o_rows, 0, o_rows, None)]


def to_all(line, make):
    copies = []
    for step in range(1, line.n):
        peer = lax.rem(line.me + step, line.n)
        copies.append(make(step, peer))
    for c in copies:
        c.start()
    return copies


def others(line):
    return [lax.rem(line.me + step, line.n) for step in range(1, line.n)]


def start_kernel(n_model, hid_ref, sc_ref, wq_ref, wk_ref, wv_ref, wo_ref, wg_ref, wu_ref,
                 x_ref, h_ref, sca_ref, wqkv_ref, woa_ref, u0a_ref, u0b_ref, g1_ref, u1a_ref, u1b_ref,
                 xin, scin, stage, xs, xr, ss, sr, ls, hs, hr, es, er):
    torus, line = Torus(), Line(n_model)
    rows = x_ref.shape[0]
    part = wg_ref.shape[2] // 2
    shards = ((wu_ref, 0, (u0a_ref, u0b_ref)), (wg_ref, 1, (g1_ref,)), (wu_ref, 1, (u1a_ref, u1b_ref)))
    loads = [pltpu.make_async_copy(ref.at[layer], stage.at[k], ls.at[k]) for k, (ref, layer, _) in enumerate(shards)]
    stores = []
    for k, (_, _, dsts) in enumerate(shards):
        if len(dsts) == 1:
            stores.append([pltpu.make_async_copy(stage.at[k], dsts[0], ls.at[k])])
        else:
            stores.append([pltpu.make_async_copy(stage.at[k, :, pl.ds(i * part, part)], dst, ls.at[k + 3 * i]) for i, dst in enumerate(dsts)])
    for c in loads:
        c.start()
    meet(torus, others(line))
    xin[line.me] = hid_ref[line.me]
    scin[line.me] = sc_ref[...]
    xc = to_all(line, lambda step, peer: remote(hid_ref.at[peer], xin.at[line.me], xs.at[step], xr.at[step], {'model': peer}))
    sc = to_all(line, lambda step, peer: remote(sc_ref, scin.at[line.me], ss.at[step], sr.at[step], {'model': peer}))
    ex = Exchange(line, load_attn_weights(line, 0, wq_ref, wk_ref, wv_ref, wo_ref, wqkv_ref, woa_ref), es, er)
    ex.begin()
    for load, store in zip(loads, stores):
        load.wait()
        for c in store:
            c.start()
    for c in xc + sc:
        c.wait_recv()
    sca_ref[...] = jnp.concatenate([scin[m] for m in range(n_model)], axis=1)
    x = jnp.concatenate([xin[m] for m in range(n_model)], axis=1)
    x_ref[...] = x
    mine = torus.at(0, 0, 0)
    h_ref[pl.ds(pl.multiple_of(mine * rows, rows), rows), :] = norm(x.astype(jnp.float32), sca_ref[0:1]).astype(jnp.bfloat16)
    gather_blocks(torus, h_ref, hs, hr, ex.onward)
    ex.finish()
    for c in sum(stores, []):
        c.wait()
    for c in xc + sc:
        c.wait_send()


def attn_weight_shapes(wq, wo, n_model):
    _, rows, dim = wq.shape
    _, o_rows, o_cols = wo.shape
    return (jax.ShapeDtypeStruct((rows * n_model, 3 * dim), wq.dtype), jax.ShapeDtypeStruct((o_rows * n_model, o_cols), wo.dtype))


def start(hidden_mine, scales, wq, wk, wv, wo, wg, wu, cid):
    n_model, rows, width_loc = hidden_mine.shape
    width = n_model * width_loc
    peer_sems = [pltpu.SemaphoreType.DMA((n_model,))] * 4
    return pl.pallas_call(
        functools.partial(start_kernel, n_model),
        out_shape=(jax.ShapeDtypeStruct((rows, width), hidden_mine.dtype),
                   jax.ShapeDtypeStruct((rows * SIDE * SIDE, width), hidden_mine.dtype),
                   jax.ShapeDtypeStruct((scales.shape[0], width), scales.dtype)) + attn_weight_shapes(wq, wo, n_model)
        + tuple(jax.ShapeDtypeStruct((wg.shape[1], wg.shape[2] // cut), wg.dtype) for cut in (2, 2, 1, 2, 2)),
        in_specs=[VMEM] * 6 + [ANY] * 2, out_specs=(VMEM,) * 5 + (ANY,) * 5,
        scratch_shapes=[pltpu.VMEM(hidden_mine.shape, hidden_mine.dtype), pltpu.VMEM((n_model,) + scales.shape, scales.dtype),
                        pltpu.VMEM((3,) + wg.shape[1:], wg.dtype)]
        + peer_sems + [pltpu.SemaphoreType.DMA((6,))] + GATHER_SEMS + exchange_sems(2),
        compiler_params=params(cid), cost_estimate=cost(100_000_000), name='start',
    )(hidden_mine, scales, wq, wk, wv, wo, wg, wu)


def project_kernel(n_model, ffn, final, attn, down, a_ref, w_ref, res_ref, sa_ref, sb_ref, *rest):
    rest = list(rest)
    if ffn:
        wg_any, wu_lo, wu_hi = rest[:3]
        rest = rest[3:]
    fetch = attn or down is not None
    if attn:
        wq_ref, wk_ref, wv_ref, wo_ref = rest[:4]
        rest = rest[4:]
    if down is not None:
        wd_ref = rest.pop(0)
    if not final:
        x_ref = rest.pop(0)
    h_ref = rest.pop(0)
    if attn:
        wqkv_ref, woa_ref = rest[:2]
        rest = rest[2:]
    if down is not None:
        wda_ref = rest.pop(0)
    far, right, left, own, from_l1, from_r1, from_l, from_r, q_l1, q_r1, q_l, q_r, s1, r1, s2, r2, hs, hr = rest[:18]
    rest = rest[18:]
    if ffn:
        hp, mid, wg_ref, wu_ref, wd_ref2, fs = rest[:6]
        rest = rest[6:]
    torus, line = Torus(), Line(n_model)
    rows, width = res_ref.shape
    half = rows // 2
    cols = width // 2
    if ffn:
        span = wg_any.shape[1] // WIDE

        def wide_load(k, n):
            at = pl.ds(pl.multiple_of(n * span, span), span)
            dst = (wg_ref, wu_ref)[k]
            return pltpu.make_async_copy(wg_any.at[:, at], dst.at[:, at], fs.at[k, n])

        for n in range(WIDE):
            wide_load(0, n).start()
            part = wu_lo if n < WIDE // 2 else wu_hi
            pltpu.make_async_copy(part.at[:, pl.ds(n % (WIDE // 2) * span, span)], wu_ref.at[:, pl.ds(n * span, span)], fs.at[1, n]).start()
        down_load = pltpu.make_async_copy(w_ref, wd_ref2, fs.at[2, 0])
        down_load.start()
        w_ref = wd_ref2
    if final:
        meet(torus, others(line))
    elif fetch:
        meet(torus, (line.right, line.left, line.mate))
    else:
        meet(torus, ())
    order = (2, 1, -1, 0)

    def feed(group):
        these = slice(group * SIDE * rows, (group + 1) * SIDE * rows)

        def step(n, carry):
            if group == 0:
                wide_load(0, n).wait()
                wide_load(1, n).wait()
            at = pl.ds(pl.multiple_of(n * span, span), span)
            lhs = hp[these, :]
            g = jnp.dot(lhs, wg_ref[:, at], preferred_element_type=jnp.float32).astype(jnp.bfloat16)
            u = jnp.dot(lhs, wu_ref[:, at], preferred_element_type=jnp.float32).astype(jnp.bfloat16)
            act = jax.nn.gelu(g.astype(jnp.float32), approximate=True)
            mid[these, at] = (act * u.astype(jnp.float32)).astype(jnp.bfloat16)
            return carry

        lax.fori_loop(0, WIDE, step, 0)

    def operand(q, off, o):
        if ffn:
            at = NEED.index((off, o) if q == 0 else (o, off)) * rows
            return mid[at:at + rows, :]
        return a_ref[pl.ds(pl.multiple_of(torus.at(q, off, o) * rows, rows), rows), :]

    def product(q, off, dst):
        lhs = jnp.concatenate([operand(q, off, o) for o in order], axis=0)
        piece = w_ref.shape[2]
        per = cols // piece
        for p in range(per):
            res = jnp.dot(lhs, w_ref[q * per + p], preferred_element_type=jnp.float32)
            for n in range(SIDE):
                dst[q, n, :, p * piece:(p + 1) * piece] = res[n * rows:(n + 1) * rows]

    def ring1(q, n, k):
        src, dst, step = ((far.at[q, n, pl.ds(0, half)], from_l1.at[q, n], 1), (far.at[q, n, pl.ds(half, half)], from_r1.at[q, n], -1),
                          (right.at[q, n], from_l.at[q, n], 1), (left.at[q, n], from_r.at[q, n], -1))[k]
        return remote(src, dst, s1.at[q, n, k], r1.at[q, n, k], torus.peer(q, step))

    def ring2(q, k):
        src, dst, step = ((own.at[q, 0, pl.ds(0, half)], q_l1.at[q], 1), (own.at[q, 0, pl.ds(half, half)], q_r1.at[q], -1),
                          (own.at[q, 1], q_l.at[q], 1), (own.at[q, 2], q_r.at[q], -1))[k]
        return remote(src, dst, s2.at[q, k], r2.at[q, k], torus.peer(1 - q, step))

    if down is not None:
        mine, ls = rest[2:]
        load = pltpu.make_async_copy(wd_ref.at[down], mine, ls.at[0])
        load.start()
    if ffn:
        for k, (dy, dz) in enumerate(NEED):
            hp[k * rows:(k + 1) * rows, :] = a_ref[pl.ds(pl.multiple_of(torus.at(0, dy, dz) * rows, rows), rows), :]
    for q in (0, 1):
        if ffn:
            feed(q)
            if q == 0:
                down_load.wait()
        product(q, 2, far)
        for n in range(SIDE):
            ring1(q, n, 0).start()
            ring1(q, n, 1).start()
    if attn:
        ex = Exchange(line, load_attn_weights(line, 1, wq_ref, wk_ref, wv_ref, wo_ref, wqkv_ref, woa_ref), rest[0], rest[1])
        ex.begin()
    if down is not None:
        load.wait()
        stride = mine.shape[0]
        piece = stride // PIECES
        keep = pltpu.make_async_copy(mine, row_block(wda_ref, line.me * stride, stride, stride), ls.at[0])
        keep.start()
        ex = Exchange(line, [(wda_ref, stride, k * piece, piece, mine.at[pl.ds(k * piece, piece)]) for k in range(PIECES)], rest[0], rest[1])
        ex.begin()
    for q in (0, 1):
        if ffn and q == 0:
            feed(2)
        product(q, 1, right)
        for n in range(SIDE):
            ring1(q, n, 0).wait_recv()
            right[q, n, 0:half] += from_l1[q, n]
            ring1(q, n, 2).start()
        if ffn and q == 0:
            feed(3)
        product(q, -1, left)
        for n in range(SIDE):
            ring1(q, n, 1).wait_recv()
            left[q, n, half:rows] += from_r1[q, n]
            ring1(q, n, 3).start()
    for q in (0, 1):
        product(q, 0, own)
    if down is not None:
        ex.onward(0, 2)
    for n in range(SIDE):
        for q in (0, 1):
            ring1(q, n, 2).wait_recv()
            ring1(q, n, 3).wait_recv()
            own[q, n] += from_l[q, n] + from_r[q, n]
            if n == 0:
                ring2(q, 0).start()
                ring2(q, 1).start()
            if n == 1:
                ring2(q, 0).wait_recv()
                own[q, 1, 0:half] += q_l1[q]
                ring2(q, 2).start()
            if n == 2:
                ring2(q, 1).wait_recv()
                own[q, 2, half:rows] += q_r1[q]
                ring2(q, 3).start()
    total = []
    for q in (0, 1):
        ring2(q, 2).wait_recv()
        ring2(q, 3).wait_recv()
        total.append(own[q, 3] + q_l[q] + q_r[q])
    out = jnp.concatenate(total, axis=1).astype(jnp.bfloat16).astype(jnp.float32)
    x_new = (res_ref[...].astype(jnp.float32) + norm(out, sa_ref[...])).astype(jnp.bfloat16)
    here = pl.ds(pl.multiple_of(torus.at(0, 0, 0) * rows, rows), rows)
    if final:
        outgo, income, cs, cr = rest
        part = width // n_model
        for m in range(n_model):
            outgo[m] = x_new[:, m * part:(m + 1) * part]
        income[line.me] = outgo[line.me]
        copies = to_all(line, lambda step, peer: remote(outgo.at[peer], income.at[line.me], cs.at[step], cr.at[step], {'model': peer}))
        for c in copies:
            c.wait_recv()
        for m in range(n_model):
            h_ref[m, here, :] = income[m]
    else:
        x_ref[...] = x_new
        h_ref[here, :] = norm(x_new.astype(jnp.float32), sb_ref[...]).astype(jnp.bfloat16)
    if attn:
        gather_blocks(torus, h_ref, hs, hr, ex.onward)
        ex.finish()
    elif down is not None:
        gather_blocks(torus, h_ref, hs, hr, lambda: ex.onward(2))
        ex.finish()
        keep.wait()
    else:
        gather_blocks(torus, h_ref, hs, hr)
    if final:
        for c in copies:
            c.wait_send()
    for q in (0, 1):
        for k in range(4):
            ring2(q, k).wait_send()
            for n in range(SIDE):
                ring1(q, n, k).wait_send()


def project(a, w, resid, scale_a, scale_b, n_model, cid, wide=None, final=False, attn=None, down=None, layer=None):
    rows, width = resid.shape
    cols = width // 2
    half = rows // 2

    def f32(*shape):
        return pltpu.VMEM((2,) + shape + (cols,), jnp.float32)

    scratch = [f32(SIDE, rows)] * 4 + [f32(SIDE, half)] * 2 + [f32(SIDE, rows)] * 2 + [f32(half)] * 2 + [f32(rows)] * 2
    scratch += [pltpu.SemaphoreType.DMA((2, SIDE, 4))] * 2 + [pltpu.SemaphoreType.DMA((2, 4))] * 2 + GATHER_SEMS
    h_dims = (n_model, rows * SIDE * SIDE, width // n_model) if final else (rows * SIDE * SIDE, width)
    h_shape = jax.ShapeDtypeStruct(h_dims, jnp.bfloat16)
    out_shape = (h_shape,) if final else (jax.ShapeDtypeStruct((rows, width), jnp.bfloat16), h_shape)
    args = (a, w, resid, scale_a, scale_b)
    in_specs, out_specs = [VMEM] * 5, (VMEM,) * len(out_shape)
    if wide is not None:
        args += tuple(wide)
        in_specs[1] = ANY
        in_specs += [ANY] * 3
        gate = wide[0]
        scratch += [pltpu.VMEM(a.shape, a.dtype), pltpu.VMEM((a.shape[0], gate.shape[1]), a.dtype), pltpu.VMEM(gate.shape, gate.dtype),
                    pltpu.VMEM(gate.shape, gate.dtype), pltpu.VMEM(w.shape, w.dtype), pltpu.SemaphoreType.DMA((3, WIDE))]
    if attn is not None:
        args += tuple(attn)
        in_specs += [VMEM] * 4
        out_shape += attn_weight_shapes(attn[0], attn[3], n_model)
        out_specs += (VMEM,) * 2
        scratch += exchange_sems(2)
    if down is not None:
        args += (down,)
        in_specs += [ANY]
        _, d_rows, d_cols = down.shape
        out_shape += (jax.ShapeDtypeStruct((d_rows * n_model, d_cols), down.dtype),)
        out_specs += (ANY,)
        scratch += exchange_sems(PIECES) + [pltpu.VMEM((d_rows, d_cols), down.dtype), pltpu.SemaphoreType.DMA((1,))]
    if final:
        part = (n_model, rows, width // n_model)
        scratch += [pltpu.VMEM(part, jnp.bfloat16)] * 2 + [pltpu.SemaphoreType.DMA((n_model,))] * 2
    return pl.pallas_call(
        functools.partial(project_kernel, n_model, wide is not None, final, attn is not None, layer),
        out_shape=out_shape, in_specs=in_specs, out_specs=out_specs, scratch_shapes=scratch,
        compiler_params=params(cid), cost_estimate=cost(100_000_000), name='project_reduce',
    )(*args)


def solution(mesh):
    n_model = mesh.shape['model']
    n_heads = mesh.shape['heads']
    col_spec = P(None, 'model', 'heads')
    row_spec = P(None, 'heads', 'model')
    cache_spec = P(None, None, 'heads', None)

    def body(hidden_in, seg_ids, positions, w_query, w_key, w_value, w_out, w_gate, w_up, w_down, norm_scales, qk_scales):
        n_tok, width_loc = hidden_in.shape
        head_dim = qk_scales.shape[-1]
        tok_m = n_tok // n_model
        tok_own = tok_m // n_heads
        hd = lax.axis_index('heads')
        md = lax.axis_index('model')

        attn_shards = (w_query, w_key, w_value, w_out)
        mine = lax.dynamic_index_in_dim(hidden_in.reshape(n_model, n_heads, tok_own, width_loc), hd, 1, keepdims=False)
        gate_0 = lax.all_gather(w_gate[0], 'model', axis=0, tiled=True)
        resid, h, scales, wqkv, wo, *shards = start(mine, norm_scales.reshape(-1, width_loc), *attn_shards, w_gate, w_up, 0)
        wide = [gate_0] + [lax.all_gather(w, 'model', axis=0, tiled=True) for w in shards[:2]]

        pos_m = lax.dynamic_slice_in_dim(positions, md * tok_m, tok_m)
        seg_m = lax.dynamic_slice_in_dim(seg_ids, md * tok_m, tok_m)

        settings = ((GLOBAL_BASE, GLOBAL_FACTOR, n_tok), (LOCAL_BASE, 1.0, WINDOW))
        keys, values = [], []
        for l in range(2):
            rope_base, pos_factor, window = settings[l]
            cos_tab, sin_tab = rope_tables(pos_m, head_dim, rope_base, pos_factor)
            q, k_all, v_all = make_qkv(h, wqkv, cos_tab, sin_tab, qk_scales[l], n_model, 1 + 3 * l)
            if l == 1:
                k_all, up_last = lax.optimization_barrier((k_all, late[2]))
                wide_next.append(lax.all_gather(up_last, 'model', axis=0, tiled=True))
            keys.append(k_all[:, None, :])
            values.append(v_all[:, None, :])
            o = attend(q, k_all, v_all, seg_m, pos_m, seg_ids, positions, window)
            wo = wo.reshape(n_model, head_dim, width_loc)
            row = 4 * l
            resid, h, wd = project(o, wo, resid, scales[row + 1:row + 2], scales[row + 2:row + 3], n_model, 2 + 3 * l, down=w_down, layer=l)
            wd = wd.reshape(n_model, w_down.shape[1], width_loc)
            if l == 0:
                h, *late = lax.optimization_barrier((h, *shards[2:]))
                wide_next = [lax.all_gather(w, 'model', axis=0, tiled=True) for w in late[:2]]
                resid, h, wqkv, wo = project(h, wd, resid, scales[3:4], scales[4:5], n_model, 3, wide=wide, attn=attn_shards)
            else:
                out, = project(h, wd, resid, scales[7:8], scales[7:8], n_model, 6, wide=wide_next, final=True)
        out = out.reshape(n_tok, width_loc)
        return out, jnp.stack(keys), jnp.stack(values)

    return jax.shard_map(body, mesh=mesh,
                         in_specs=(P(None, 'model'), P(), P(), col_spec, col_spec, col_spec, row_spec, col_spec, col_spec, row_spec, P(None, None, 'model'), P()),
                         out_specs=(P(None, 'model'), cache_spec, cache_spec),
                         check_vma=False)
```

```python
import functools

import jax
import jax.numpy as jnp
from jax import lax
from jax.experimental import pallas as pl
from jax.experimental.pallas import tpu as pltpu
from jax.sharding import PartitionSpec as P

NORM_EPS = 1e-6
WINDOW = 1024
GLOBAL_BASE = 1000000.0
GLOBAL_FACTOR = 8.0
LOCAL_BASE = 10000.0
MESH = pl.DeviceIdType.MESH
SIDE = 4
VMEM_LIMIT = 63 * 1024 * 1024


def norm(values, scale_row):
    mean_sq = jnp.mean(values * values, axis=-1, keepdims=True)
    return values * lax.rsqrt(mean_sq + NORM_EPS) * (1.0 + scale_row)


def rope_tables(positions, head_dim, rope_base, pos_factor):
    exponents = jnp.arange(0, head_dim, 2).astype(jnp.float32) / head_dim
    inv_freq = rope_base ** (-exponents)
    angles = (positions.astype(jnp.float32) / pos_factor)[:, None] * inv_freq[None, :]
    return jnp.cos(angles), jnp.sin(angles)


def apply_rope(values, cos_tab, sin_tab):
    half_dim = values.shape[-1] // 2
    first_half = values[..., :half_dim]
    second_half = values[..., half_dim:]
    return jnp.concatenate([first_half * cos_tab - second_half * sin_tab, second_half * cos_tab + first_half * sin_tab], axis=-1)


def attend(q, k, v, seg_q, pos_q, seg_ids, positions, window):
    scores = jnp.dot(q, k.T, preferred_element_type=jnp.float32) * (q.shape[-1] ** -0.5)
    gap = pos_q[:, None] - positions[None, :]
    allowed = (seg_q[:, None] == seg_ids[None, :]) & (gap >= 0) & (gap < window)
    scores = jnp.where(allowed, scores, -1e30)
    row_max = jnp.max(scores, axis=-1, keepdims=True)
    e = jnp.exp(scores - row_max)
    p = (e / jnp.sum(e, axis=-1, keepdims=True)).astype(jnp.bfloat16)
    return jnp.dot(p, v, preferred_element_type=jnp.float32).astype(jnp.bfloat16)


def wrap(i):
    return lax.rem(i + 2 * SIDE, SIDE)


def remote(src, dst, send, recv, to):
    return pltpu.make_async_remote_copy(src, dst, send, recv, device_id=to, device_id_type=MESH)


def row_block(ref, start, size, align):
    return ref.at[pl.ds(pl.multiple_of(start, align), size), :]


class Torus:
    def __init__(self):
        me = lax.axis_index('heads')
        self.own = (lax.rem(me, SIDE), me // SIDE)

    def block(self, axis, along, across):
        return across * SIDE + along if axis == 0 else along * SIDE + across

    def at(self, axis, da, db):
        return self.block(axis, wrap(self.own[axis] + da), wrap(self.own[1 - axis] + db))

    def peer(self, axis, step):
        return {'heads': self.at(axis, step, 0)}


class Line:
    def __init__(self, n_model):
        self.n = n_model
        self.me = lax.axis_index('model')
        chips = n_model // 2
        chip, core = self.me // 2, lax.rem(self.me, 2)
        self.right = lax.rem(chip + 1, chips) * 2 + core
        self.left = lax.rem(chip + chips - 1, chips) * 2 + core
        self.far = lax.rem(chip + 2, chips) * 2 + core
        self.mate = chip * 2 + 1 - core


def meet(torus, models):
    barrier = pltpu.get_barrier_semaphore()
    count = len(models)
    for other in models:
        pl.semaphore_signal(barrier, inc=1, device_id={'model': other}, device_id_type=MESH)
    if torus is not None:
        for axis in (0, 1):
            for step in (1, -1):
                pl.semaphore_signal(barrier, inc=1, device_id=torus.peer(axis, step), device_id_type=MESH)
                count += 1
    pl.semaphore_wait(barrier, count)


def gather_blocks(torus, h_ref, send, recv, between=lambda: None):
    apart = len(h_ref.shape) == 3
    rows = h_ref.shape[-2] // (SIDE * SIDE)
    cols = h_ref.shape[0 if apart else 1] // 2
    half = rows // 2

    def view(q, da, db, part):
        start = torus.at(q, da, db) * rows + (half if part == 2 else 0)
        if apart:
            return h_ref.at[pl.ds(q * cols, cols), pl.ds(pl.multiple_of(start, half), rows if part == 0 else half), :]
        return h_ref.at[pl.ds(pl.multiple_of(start, half), rows if part == 0 else half), pl.ds(q * cols, cols)]

    def ring(q, axis, base, offsets):
        def make(k, da, db, part, step):
            v = view(q, da, db, part)
            return remote(v, v, send.at[q, base, k], recv.at[q, base, k], torus.peer(axis, step))

        along = (lambda off: (off, offsets)) if axis == q else (lambda off: (offsets, off))
        return (make(0, *along(0), 0, 1), make(1, *along(0), 0, -1), make(2, *along(-1), 1, 1), make(3, *along(1), 2, -1))

    first = [ring(q, 1 - q, 0, 0) for q in (0, 1)]
    second = [[ring(q, q, 1 + n, off) for n, off in enumerate((0, -1, 1, 2))] for q in (0, 1)]

    def begin(copies):
        copies[0].start()
        copies[1].start()

    def onward(copies):
        copies[0].wait_recv()
        copies[2].start()
        copies[1].wait_recv()
        copies[3].start()

    for q in (0, 1):
        begin(first[q])
    for q in (0, 1):
        begin(second[q][0])
    for q in (0, 1):
        first[q][0].wait_recv()
        first[q][2].start()
        begin(second[q][1])
        first[q][1].wait_recv()
        first[q][3].start()
        begin(second[q][2])
    for q in (0, 1):
        onward(second[q][0])
    for q in (0, 1):
        first[q][2].wait_recv()
        first[q][3].wait_recv()
        begin(second[q][3])
    between()
    for n in (1, 2, 3):
        for q in (0, 1):
            onward(second[q][n])
    for q in (0, 1):
        for n in range(SIDE):
            second[q][n][2].wait_recv()
            second[q][n][3].wait_recv()
    for q in (0, 1):
        for copies in [first[q]] + second[q]:
            for c in copies:
                c.wait_send()


GATHER_SEMS = [pltpu.SemaphoreType.DMA((2, 1 + SIDE, 4)), pltpu.SemaphoreType.DMA((2, 1 + SIDE, 4))]


class Exchange:
    def __init__(self, line, items, send, recv):
        self.copies = []
        plan = [(line.me, line.right, 0), (line.me, line.left, 0), (line.me, line.mate, 0), (line.left, line.right, 1),
                (line.right, line.left, 2), (line.left, line.mate, 0), (line.right, line.mate, 0),
                (line.far, line.mate, 1), (line.far, line.mate, 2)]
        for a, (ref, stride, row, rows, src) in enumerate(items):
            half = rows // 2
            group = []
            for slot, (owner, to, part) in enumerate(plan):
                first = owner * stride + (row + (half if part == 2 else 0))
                v = row_block(ref, first, rows if part == 0 else half, half)
                group.append(remote(src if src is not None and slot < 3 else v, v, send.at[a, slot], recv.at[a, slot], {'model': to}))
            self.copies.append(group)

    def begin(self, lo=0, hi=None):
        for c in self.copies[lo:hi]:
            c[0].start()
            c[1].start()
            c[2].start()

    def onward(self, lo=0, hi=None):
        for c in self.copies[lo:hi]:
            c[0].wait_recv()
            c[3].start()
            c[1].wait_recv()
            c[4].start()
            c[5].start()
            c[6].start()

    def finish(self):
        for c in self.copies:
            c[3].wait_recv()
            c[7].start()
            c[4].wait_recv()
            c[8].start()
        for c in self.copies:
            for slot in (2, 5, 6, 7, 8):
                c[slot].wait_recv()
            for one in c:
                one.wait_send()


def exchange_sems(count):
    return [pltpu.SemaphoreType.DMA((count, 9)), pltpu.SemaphoreType.DMA((count, 9))]


def qkv_kernel(n_model, h_ref, w_any, cos_ref, sin_ref, qk_ref, q_ref, ka_ref, va_ref, w_ref, ls, send, recv):
    line = Line(n_model)
    rows, dim = q_ref.shape
    parts = [pl.ds(at * dim, dim) for at in range(3)]
    loads = [pltpu.make_async_copy(w_any.at[:, p], w_ref.at[:, p], ls.at[k]) for k, p in enumerate(parts)]
    for k in (1, 2, 0):
        loads[k].start()
    meet(None, (line.right, line.left, line.mate))
    here = pl.ds(pl.multiple_of(line.me * rows, rows), rows)
    piece = rows // 2
    ex = Exchange(line, [(ref, rows, at, piece, None) for ref in (ka_ref, va_ref) for at in (0, piece)], send, recv)

    def made(k):
        loads[k].wait()
        return jnp.dot(h_ref[...], w_ref[:, k * dim:(k + 1) * dim], preferred_element_type=jnp.float32).astype(jnp.bfloat16)

    def turned(values, row):
        return apply_rope(norm(values.astype(jnp.float32), qk_ref[row:row + 1]), cos_ref[...], sin_ref[...]).astype(jnp.bfloat16)

    ka_ref[here, :] = turned(made(1), 1)
    ex.begin(0, 2)
    va_ref[here, :] = made(2)
    ex.begin(2)
    q_ref[...] = turned(made(0), 0)
    ex.onward()
    ex.finish()


VMEM = pl.BlockSpec(memory_space=pltpu.VMEM)
ANY = pl.BlockSpec(memory_space=pl.ANY)
PIECES = 4
WIDE = 2
NEED = ((2, 2), (2, 1), (2, -1), (2, 0), (1, 2), (-1, 2), (0, 2), (1, 1),
        (1, -1), (1, 0), (-1, 1), (-1, -1), (-1, 0), (0, 1), (0, -1), (0, 0))


def params(cid):
    return pltpu.CompilerParams(collective_id=cid, has_side_effects=True, vmem_limit_bytes=VMEM_LIMIT)


def cost(flops):
    return pl.CostEstimate(flops=flops, bytes_accessed=10_000_000, transcendentals=0)


def make_qkv(h, w, cos_tab, sin_tab, qk_rows, n_model, cid):
    rows, dim = h.shape[0], qk_rows.shape[1]
    full = jax.ShapeDtypeStruct((rows * n_model, dim), h.dtype)
    return pl.pallas_call(
        functools.partial(qkv_kernel, n_model),
        out_shape=(jax.ShapeDtypeStruct((rows, dim), h.dtype), full, full), in_specs=[VMEM, ANY, VMEM, VMEM, VMEM], out_specs=(VMEM,) * 3,
        scratch_shapes=[pltpu.VMEM(w.shape, w.dtype), pltpu.SemaphoreType.DMA((3,))] + exchange_sems(4),
        compiler_params=params(cid), cost_estimate=cost(100_000_000), name='make_qkv',
    )(h, w, cos_tab, sin_tab, qk_rows)


def load_attn_weights(line, layer, wq_ref, wk_ref, wv_ref, wo_ref, wqkv_ref, woa_ref):
    rows, dim = wq_ref.shape[1:]
    here = pl.ds(pl.multiple_of(line.me * rows, rows), rows)
    for at, ref in enumerate((wq_ref, wk_ref, wv_ref)):
        wqkv_ref[here, at * dim:(at + 1) * dim] = ref[layer]
    o_rows = wo_ref.shape[1]
    woa_ref[pl.ds(pl.multiple_of(line.me * o_rows, o_rows), o_rows), :] = wo_ref[layer]
    return [(wqkv_ref, rows, 0, rows, None), (woa_ref, o_rows, 0, o_rows, None)]


def to_all(line, make):
    copies = []
    for step in range(1, line.n):
        peer = lax.rem(line.me + step, line.n)
        copies.append(make(step, peer))
    for c in copies:
        c.start()
    return copies


def others(line):
    return [lax.rem(line.me + step, line.n) for step in range(1, line.n)]


def start_kernel(n_model, hid_ref, sc_ref, wq_ref, wk_ref, wv_ref, wo_ref, wg_ref, wu_ref,
                 x_ref, h_ref, sca_ref, wqkv_ref, woa_ref, u0a_ref, u0b_ref, g1_ref, u1a_ref, u1b_ref,
                 xin, scin, stage, xs, xr, ss, sr, ls, hs, hr, es, er):
    torus, line = Torus(), Line(n_model)
    rows = x_ref.shape[0]
    part = wg_ref.shape[2] // 2
    shards = ((wu_ref, 0, (u0a_ref, u0b_ref)), (wg_ref, 1, (g1_ref,)), (wu_ref, 1, (u1a_ref, u1b_ref)))
    loads = [pltpu.make_async_copy(ref.at[layer], stage.at[k], ls.at[k]) for k, (ref, layer, _) in enumerate(shards)]
    stores = []
    for k, (_, _, dsts) in enumerate(shards):
        if len(dsts) == 1:
            stores.append([pltpu.make_async_copy(stage.at[k], dsts[0], ls.at[k])])
        else:
            stores.append([pltpu.make_async_copy(stage.at[k, :, pl.ds(i * part, part)], dst, ls.at[k + 3 * i]) for i, dst in enumerate(dsts)])
    for c in loads:
        c.start()
    meet(torus, others(line))
    xin[line.me] = hid_ref[line.me]
    scin[line.me] = sc_ref[...]
    xc = to_all(line, lambda step, peer: remote(hid_ref.at[peer], xin.at[line.me], xs.at[step], xr.at[step], {'model': peer}))
    sc = to_all(line, lambda step, peer: remote(sc_ref, scin.at[line.me], ss.at[step], sr.at[step], {'model': peer}))
    ex = Exchange(line, load_attn_weights(line, 0, wq_ref, wk_ref, wv_ref, wo_ref, wqkv_ref, woa_ref), es, er)
    ex.begin()
    for load, store in zip(loads, stores):
        load.wait()
        for c in store:
            c.start()
    for c in xc + sc:
        c.wait_recv()
    sca_ref[...] = jnp.concatenate([scin[m] for m in range(n_model)], axis=1)
    x = jnp.concatenate([xin[m] for m in range(n_model)], axis=1)
    x_ref[...] = x
    mine = torus.at(0, 0, 0)
    h_ref[pl.ds(pl.multiple_of(mine * rows, rows), rows), :] = norm(x.astype(jnp.float32), sca_ref[0:1]).astype(jnp.bfloat16)
    gather_blocks(torus, h_ref, hs, hr, ex.onward)
    ex.finish()
    for c in sum(stores, []):
        c.wait()
    for c in xc + sc:
        c.wait_send()


def attn_weight_shapes(wq, wo, n_model):
    _, rows, dim = wq.shape
    _, o_rows, o_cols = wo.shape
    return (jax.ShapeDtypeStruct((rows * n_model, 3 * dim), wq.dtype), jax.ShapeDtypeStruct((o_rows * n_model, o_cols), wo.dtype))


def start(hidden_mine, scales, wq, wk, wv, wo, wg, wu, cid):
    n_model, rows, width_loc = hidden_mine.shape
    width = n_model * width_loc
    peer_sems = [pltpu.SemaphoreType.DMA((n_model,))] * 4
    return pl.pallas_call(
        functools.partial(start_kernel, n_model),
        out_shape=(jax.ShapeDtypeStruct((rows, width), hidden_mine.dtype),
                   jax.ShapeDtypeStruct((rows * SIDE * SIDE, width), hidden_mine.dtype),
                   jax.ShapeDtypeStruct((scales.shape[0], width), scales.dtype)) + attn_weight_shapes(wq, wo, n_model)
        + tuple(jax.ShapeDtypeStruct((wg.shape[1], wg.shape[2] // cut), wg.dtype) for cut in (2, 2, 1, 2, 2)),
        in_specs=[VMEM] * 6 + [ANY] * 2, out_specs=(VMEM,) * 5 + (ANY,) * 5,
        scratch_shapes=[pltpu.VMEM(hidden_mine.shape, hidden_mine.dtype), pltpu.VMEM((n_model,) + scales.shape, scales.dtype),
                        pltpu.VMEM((3,) + wg.shape[1:], wg.dtype)]
        + peer_sems + [pltpu.SemaphoreType.DMA((6,))] + GATHER_SEMS + exchange_sems(2),
        compiler_params=params(cid), cost_estimate=cost(100_000_000), name='start',
    )(hidden_mine, scales, wq, wk, wv, wo, wg, wu)


def project_kernel(n_model, ffn, final, attn, down, a_ref, w_ref, res_ref, sa_ref, sb_ref, *rest):
    rest = list(rest)
    if ffn:
        wg_any, wu_lo, wu_hi = rest[:3]
        rest = rest[3:]
    fetch = attn or down is not None
    if attn:
        wq_ref, wk_ref, wv_ref, wo_ref = rest[:4]
        rest = rest[4:]
    if down is not None:
        wd_ref = rest.pop(0)
    if not final:
        x_ref = rest.pop(0)
    h_ref = rest.pop(0)
    if attn:
        wqkv_ref, woa_ref = rest[:2]
        rest = rest[2:]
    if down is not None:
        wda_ref = rest.pop(0)
    far, right, left, own, from_l1, from_r1, from_l, from_r, q_l1, q_r1, q_l, q_r, s1, r1, s2, r2, hs, hr = rest[:18]
    rest = rest[18:]
    if ffn:
        hp, mid, wg_ref, wu_ref, wd_ref2, fs = rest[:6]
        rest = rest[6:]
    torus, line = Torus(), Line(n_model)
    rows, width = res_ref.shape
    half = rows // 2
    cols = width // 2
    if ffn:
        span = wg_any.shape[1] // WIDE

        def wide_load(k, n):
            at = pl.ds(pl.multiple_of(n * span, span), span)
            dst = (wg_ref, wu_ref)[k]
            return pltpu.make_async_copy(wg_any.at[:, at], dst.at[:, at], fs.at[k, n])

        for n in range(WIDE):
            wide_load(0, n).start()
            part = wu_lo if n < WIDE // 2 else wu_hi
            pltpu.make_async_copy(part.at[:, pl.ds(n % (WIDE // 2) * span, span)], wu_ref.at[:, pl.ds(n * span, span)], fs.at[1, n]).start()
        down_load = pltpu.make_async_copy(w_ref, wd_ref2, fs.at[2, 0])
        down_load.start()
        w_ref = wd_ref2
    if final:
        meet(torus, others(line))
    elif fetch:
        meet(torus, (line.right, line.left, line.mate))
    else:
        meet(torus, ())
    order = (2, 1, -1, 0)

    def feed(group):
        these = slice(group * SIDE * rows, (group + 1) * SIDE * rows)

        def step(n, carry):
            if group == 0:
                wide_load(0, n).wait()
                wide_load(1, n).wait()
            at = pl.ds(pl.multiple_of(n * span, span), span)
            lhs = hp[these, :]
            g = jnp.dot(lhs, wg_ref[:, at], preferred_element_type=jnp.float32).astype(jnp.bfloat16)
            u = jnp.dot(lhs, wu_ref[:, at], preferred_element_type=jnp.float32).astype(jnp.bfloat16)
            act = jax.nn.gelu(g.astype(jnp.float32), approximate=True)
            mid[these, at] = (act * u.astype(jnp.float32)).astype(jnp.bfloat16)
            return carry

        lax.fori_loop(0, WIDE, step, 0)

    def operand(q, off, o):
        if ffn:
            at = NEED.index((off, o) if q == 0 else (o, off)) * rows
            return mid[at:at + rows, :]
        return a_ref[pl.ds(pl.multiple_of(torus.at(q, off, o) * rows, rows), rows), :]

    def product(q, off, dst):
        lhs = jnp.concatenate([operand(q, off, o) for o in order], axis=0)
        piece = w_ref.shape[2]
        per = cols // piece
        for p in range(0, per, 2):
            pair = jnp.concatenate([w_ref[q * per + p], w_ref[q * per + p + 1]], axis=1)
            res = jnp.dot(lhs, pair, preferred_element_type=jnp.float32)
            for n in range(SIDE):
                dst[q, n, :, p * piece:(p + 2) * piece] = res[n * rows:(n + 1) * rows]

    def ring1(q, n, k):
        src, dst, step = ((far.at[q, n, pl.ds(0, half)], from_l1.at[q, n], 1), (far.at[q, n, pl.ds(half, half)], from_r1.at[q, n], -1),
                          (right.at[q, n], from_l.at[q, n], 1), (left.at[q, n], from_r.at[q, n], -1))[k]
        return remote(src, dst, s1.at[q, n, k], r1.at[q, n, k], torus.peer(q, step))

    def ring2(q, k):
        src, dst, step = ((own.at[q, 0, pl.ds(0, half)], q_l1.at[q], 1), (own.at[q, 0, pl.ds(half, half)], q_r1.at[q], -1),
                          (own.at[q, 1], q_l.at[q], 1), (own.at[q, 2], q_r.at[q], -1))[k]
        return remote(src, dst, s2.at[q, k], r2.at[q, k], torus.peer(1 - q, step))

    if down is not None:
        mine, ls = rest[2:]
        load = pltpu.make_async_copy(wd_ref.at[down], mine, ls.at[0])
        load.start()
    if ffn:
        for k, (dy, dz) in enumerate(NEED):
            hp[k * rows:(k + 1) * rows, :] = a_ref[pl.ds(pl.multiple_of(torus.at(0, dy, dz) * rows, rows), rows), :]
    for q in (0, 1):
        if ffn:
            feed(q)
            if q == 0:
                down_load.wait()
        product(q, 2, far)
        for n in range(SIDE):
            ring1(q, n, 0).start()
            ring1(q, n, 1).start()
    if attn:
        ex = Exchange(line, load_attn_weights(line, 1, wq_ref, wk_ref, wv_ref, wo_ref, wqkv_ref, woa_ref), rest[0], rest[1])
        ex.begin()
    if down is not None:
        load.wait()
        stride = mine.shape[0]
        piece = stride // PIECES
        keep = pltpu.make_async_copy(mine, row_block(wda_ref, line.me * stride, stride, stride), ls.at[0])
        keep.start()
        ex = Exchange(line, [(wda_ref, stride, k * piece, piece, mine.at[pl.ds(k * piece, piece)]) for k in range(PIECES)], rest[0], rest[1])
        ex.begin()
    for q in (0, 1):
        if ffn and q == 0:
            feed(2)
        product(q, 1, right)
        for n in range(SIDE):
            ring1(q, n, 0).wait_recv()
            right[q, n, 0:half] += from_l1[q, n]
            ring1(q, n, 2).start()
        if ffn and q == 0:
            feed(3)
        product(q, -1, left)
        for n in range(SIDE):
            ring1(q, n, 1).wait_recv()
            left[q, n, half:rows] += from_r1[q, n]
            ring1(q, n, 3).start()
    for q in (0, 1):
        product(q, 0, own)
    if down is not None:
        ex.onward(0, 2)
    for n in range(SIDE):
        for q in (0, 1):
            ring1(q, n, 2).wait_recv()
            ring1(q, n, 3).wait_recv()
            own[q, n] += from_l[q, n] + from_r[q, n]
            if n == 0:
                ring2(q, 0).start()
                ring2(q, 1).start()
            if n == 1:
                ring2(q, 0).wait_recv()
                own[q, 1, 0:half] += q_l1[q]
                ring2(q, 2).start()
            if n == 2:
                ring2(q, 1).wait_recv()
                own[q, 2, half:rows] += q_r1[q]
                ring2(q, 3).start()
    total = []
    for q in (0, 1):
        ring2(q, 2).wait_recv()
        ring2(q, 3).wait_recv()
        total.append(own[q, 3] + q_l[q] + q_r[q])
    out = jnp.concatenate(total, axis=1).astype(jnp.bfloat16).astype(jnp.float32)
    x_new = (res_ref[...].astype(jnp.float32) + norm(out, sa_ref[...])).astype(jnp.bfloat16)
    here = pl.ds(pl.multiple_of(torus.at(0, 0, 0) * rows, rows), rows)
    if final:
        outgo, income, cs, cr = rest
        part = width // n_model
        for m in range(n_model):
            outgo[m] = x_new[:, m * part:(m + 1) * part]
        income[line.me] = outgo[line.me]
        copies = to_all(line, lambda step, peer: remote(outgo.at[peer], income.at[line.me], cs.at[step], cr.at[step], {'model': peer}))
        for c in copies:
            c.wait_recv()
        for m in range(n_model):
            h_ref[m, here, :] = income[m]
    else:
        x_ref[...] = x_new
        h_ref[here, :] = norm(x_new.astype(jnp.float32), sb_ref[...]).astype(jnp.bfloat16)
    if attn:
        gather_blocks(torus, h_ref, hs, hr, ex.onward)
        ex.finish()
    elif down is not None:
        gather_blocks(torus, h_ref, hs, hr, lambda: ex.onward(2))
        ex.finish()
        keep.wait()
    else:
        gather_blocks(torus, h_ref, hs, hr)
    if final:
        for c in copies:
            c.wait_send()
    for q in (0, 1):
        for k in range(4):
            ring2(q, k).wait_send()
            for n in range(SIDE):
                ring1(q, n, k).wait_send()


def project(a, w, resid, scale_a, scale_b, n_model, cid, wide=None, final=False, attn=None, down=None, layer=None):
    rows, width = resid.shape
    cols = width // 2
    half = rows // 2

    def f32(*shape):
        return pltpu.VMEM((2,) + shape + (cols,), jnp.float32)

    scratch = [f32(SIDE, rows)] * 4 + [f32(SIDE, half)] * 2 + [f32(SIDE, rows)] * 2 + [f32(half)] * 2 + [f32(rows)] * 2
    scratch += [pltpu.SemaphoreType.DMA((2, SIDE, 4))] * 2 + [pltpu.SemaphoreType.DMA((2, 4))] * 2 + GATHER_SEMS
    h_dims = (n_model, rows * SIDE * SIDE, width // n_model) if final else (rows * SIDE * SIDE, width)
    h_shape = jax.ShapeDtypeStruct(h_dims, jnp.bfloat16)
    out_shape = (h_shape,) if final else (jax.ShapeDtypeStruct((rows, width), jnp.bfloat16), h_shape)
    args = (a, w, resid, scale_a, scale_b)
    in_specs, out_specs = [VMEM] * 5, (VMEM,) * len(out_shape)
    if wide is not None:
        args += tuple(wide)
        in_specs[1] = ANY
        in_specs += [ANY] * 3
        gate = wide[0]
        scratch += [pltpu.VMEM(a.shape, a.dtype), pltpu.VMEM((a.shape[0], gate.shape[1]), a.dtype), pltpu.VMEM(gate.shape, gate.dtype),
                    pltpu.VMEM(gate.shape, gate.dtype), pltpu.VMEM(w.shape, w.dtype), pltpu.SemaphoreType.DMA((3, WIDE))]
    if attn is not None:
        args += tuple(attn)
        in_specs += [VMEM] * 4
        out_shape += attn_weight_shapes(attn[0], attn[3], n_model)
        out_specs += (VMEM,) * 2
        scratch += exchange_sems(2)
    if down is not None:
        args += (down,)
        in_specs += [ANY]
        _, d_rows, d_cols = down.shape
        out_shape += (jax.ShapeDtypeStruct((d_rows * n_model, d_cols), down.dtype),)
        out_specs += (ANY,)
        scratch += exchange_sems(PIECES) + [pltpu.VMEM((d_rows, d_cols), down.dtype), pltpu.SemaphoreType.DMA((1,))]
    if final:
        part = (n_model, rows, width // n_model)
        scratch += [pltpu.VMEM(part, jnp.bfloat16)] * 2 + [pltpu.SemaphoreType.DMA((n_model,))] * 2
    return pl.pallas_call(
        functools.partial(project_kernel, n_model, wide is not None, final, attn is not None, layer),
        out_shape=out_shape, in_specs=in_specs, out_specs=out_specs, scratch_shapes=scratch,
        compiler_params=params(cid), cost_estimate=cost(100_000_000), name='project_reduce',
    )(*args)


def solution(mesh):
    n_model = mesh.shape['model']
    n_heads = mesh.shape['heads']
    col_spec = P(None, 'model', 'heads')
    row_spec = P(None, 'heads', 'model')
    cache_spec = P(None, None, 'heads', None)

    def body(hidden_in, seg_ids, positions, w_query, w_key, w_value, w_out, w_gate, w_up, w_down, norm_scales, qk_scales):
        n_tok, width_loc = hidden_in.shape
        head_dim = qk_scales.shape[-1]
        tok_m = n_tok // n_model
        tok_own = tok_m // n_heads
        hd = lax.axis_index('heads')
        md = lax.axis_index('model')

        attn_shards = (w_query, w_key, w_value, w_out)
        mine = lax.dynamic_index_in_dim(hidden_in.reshape(n_model, n_heads, tok_own, width_loc), hd, 1, keepdims=False)
        gate_0 = lax.all_gather(w_gate[0], 'model', axis=0, tiled=True)
        resid, h, scales, wqkv, wo, *shards = start(mine, norm_scales.reshape(-1, width_loc), *attn_shards, w_gate, w_up, 0)
        wide = [gate_0] + [lax.all_gather(w, 'model', axis=0, tiled=True) for w in shards[:2]]

        pos_m = lax.dynamic_slice_in_dim(positions, md * tok_m, tok_m)
        seg_m = lax.dynamic_slice_in_dim(seg_ids, md * tok_m, tok_m)

        settings = ((GLOBAL_BASE, GLOBAL_FACTOR, n_tok), (LOCAL_BASE, 1.0, WINDOW))
        keys, values = [], []
        for l in range(2):
            rope_base, pos_factor, window = settings[l]
            cos_tab, sin_tab = rope_tables(pos_m, head_dim, rope_base, pos_factor)
            q, k_all, v_all = make_qkv(h, wqkv, cos_tab, sin_tab, qk_scales[l], n_model, 1 + 3 * l)
            if l == 1:
                k_all, up_last = lax.optimization_barrier((k_all, late[2]))
                wide_next.append(lax.all_gather(up_last, 'model', axis=0, tiled=True))
            keys.append(k_all[:, None, :])
            values.append(v_all[:, None, :])
            o = attend(q, k_all, v_all, seg_m, pos_m, seg_ids, positions, window)
            wo = wo.reshape(n_model, head_dim, width_loc)
            row = 4 * l
            resid, h, wd = project(o, wo, resid, scales[row + 1:row + 2], scales[row + 2:row + 3], n_model, 2 + 3 * l, down=w_down, layer=l)
            wd = wd.reshape(n_model, w_down.shape[1], width_loc)
            if l == 0:
                h, *late = lax.optimization_barrier((h, *shards[2:]))
                wide_next = [lax.all_gather(w, 'model', axis=0, tiled=True) for w in late[:2]]
                resid, h, wqkv, wo = project(h, wd, resid, scales[3:4], scales[4:5], n_model, 3, wide=wide, attn=attn_shards)
            else:
                out, = project(h, wd, resid, scales[7:8], scales[7:8], n_model, 6, wide=wide_next, final=True)
        out = out.reshape(n_tok, width_loc)
        return out, jnp.stack(keys), jnp.stack(values)

    return jax.shard_map(body, mesh=mesh,
                         in_specs=(P(None, 'model'), P(), P(), col_spec, col_spec, col_spec, row_spec, col_spec, col_spec, row_spec, P(None, None, 'model'), P()),
                         out_specs=(P(None, 'model'), cache_spec, cache_spec),
                         check_vma=False)
```
